32 devices in a mesh: member: 2 (over x), lat: 16 (over z, y, core).
Axes of the slice: x: 2, y: 2, z: 4, core: 2. Of those that a mesh axis runs over, the one named last changes fastest.
Arguments:
- height: float32 [128, 32, 1440], P(('member', 'lat')), parts along dimension 0, may hold values from -6 to 6
- zonal_courant: float32 [128, 32, 1440], P(('member', 'lat')), parts along dimension 0, may hold values from -1.5 to 1.5
- merid_courant: float32 [128, 32, 1440], P(('member', 'lat')), parts along dimension 0, may hold values from -1.5 to 1.5
- rates: float32 [64], P('member'), parts along dimension 0, may hold values from 0.05 to 0.5
- thresholds: float32 [64], P('member'), parts along dimension 0, may hold values from -3 to 3
- flags: int32 [64], replicated, may hold values from 0 to 1, as said below
- cutoffs: int32 [64], replicated, may hold values from 45 to 360
Outputs:
- filtered_height: float32 [128, 32, 1440], P(('member', 'lat')), parts along dimension 0
The draws below stay inside these ranges and needn't reach their ends.
There are 2 independent parts, one for each index of `member`. The reference program is written for one: setup_inputs(seed, part) draws one part's arguments, and reference() takes and returns one part's arrays. A program takes and returns all parts, laid end to end along the dimension named above; an argument that names none is the same for every part. Nothing has to cross between parts.
Inputs may be any that keep to these rules, and one draw needn't show every extreme that they name: flags is 1 on a southern band of rows that starts at row 0 and on a northern band that ends at row 63, each band 64 // 8 to 16 rows long, and 0 on all other rows.
All inputs are finite; a program needn't handle non-finite values.
Results may differ from the reference program's by a relative error of at most 0.00007.
Values sent between devices are 32-bit elements; how exact they have to be, the bound alone decides.
No kernel may reach another device: no remote copies, remote signals or barrier semaphores. Data moves between devices by JAX's collectives and lax.ppermute only.
A program may use at most 64 MiB of HBM per device.

```python
import math
import jax
import jax.numpy as jnp

NLON = 1440
LEV = 32
NLAT = 64


def draw_flags(key, part):
    south_key = jax.random.fold_in(key, 11)
    north_key = jax.random.fold_in(key, 23)
    south = jax.random.randint(south_key, (), NLAT // 8, NLAT // 4 + 1)
    north = jax.random.randint(north_key, (), NLAT // 8, NLAT // 4 + 1)
    rows = jnp.arange(NLAT, dtype=jnp.int32)
    return ((rows < south) | (rows >= NLAT - north)).astype(jnp.int32)


def with_ends(drawn, stream_key, low, high):
    spot = [jax.random.randint(jax.random.fold_in(stream_key, axis), (), 0, length) for axis, length in enumerate(drawn.shape)]
    widest = drawn.shape.index(max(drawn.shape))
    beside = spot[:widest] + [(spot[widest] + 1) % drawn.shape[widest]] + spot[widest + 1:]
    return drawn.at[tuple(spot)].set(low).at[tuple(beside)].set(high)


def block_levels(rng, shape, cuts, smallest, high):
    loudness = 1.0
    for axis_at, blocks in cuts:
        draws = jax.random.uniform(jax.random.fold_in(jax.random.fold_in(rng, 6), axis_at), (blocks,), jnp.float32, smallest / len(cuts), high / len(cuts))
        loudness = loudness * jnp.repeat(jnp.exp(draws), shape[axis_at] // blocks).reshape((-1,) + (1,) * (len(shape) - 1 - axis_at))
    return loudness


def normal_values(own_key, shape, scale, bound, pieces=(), kind=jnp.bfloat16):
    gain = block_levels(own_key, shape, pieces, -0.22, 0.18) if pieces else 1.0
    result = jax.random.normal(own_key, shape, jnp.float32) * scale * gain
    return jnp.minimum(jnp.maximum(result, -bound), bound).astype(kind)


def setup_inputs(seed: int = 0, part: int = 0) -> dict:
    splits = jax.random.split(jax.random.key(seed), 8)
    part_splits = jax.random.split(jax.random.fold_in(splits[7], part), 8)
    return {
        "height": normal_values(part_splits[0], (NLAT, LEV, NLON), 1.0, 6.0, ((0, 16),), jnp.float32),
        "zonal_courant": normal_values(part_splits[1], (NLAT, LEV, NLON), 0.3, 1.5, ((0, 16),), jnp.float32),
        "merid_courant": normal_values(part_splits[2], (NLAT, LEV, NLON), 0.3, 1.5, ((0, 16),), jnp.float32),
        "rates": jnp.clip(jnp.exp(jax.random.uniform(part_splits[3], (LEV,), jnp.float32, math.log(0.05), math.log(0.5))), 0.05, 0.5),
        "thresholds": normal_values(part_splits[4], (LEV,), 1.0, 3.0, (), jnp.float32),
        "flags": draw_flags(jax.random.fold_in(splits[7], 71), part),
        "cutoffs": with_ends(jax.random.randint(splits[6], (NLAT,), NLON // 32, NLON // 4 + 1), jax.random.fold_in(splits[6], 1), NLON // 32, (NLON // 4 + 1) - 1).astype(jnp.int32),
    }


def reference(height, zonal_courant, merid_courant, rates, thresholds, flags, cutoffs):
    rows = jnp.arange(NLAT, dtype=jnp.int32)
    cos_rows = jnp.sin(jnp.pi * (rows.astype(jnp.float32) + 0.5) / NLAT)
    faces = jnp.arange(NLAT + 1, dtype=jnp.int32)
    cos_faces = jnp.where((faces > 0) & (faces < NLAT), jnp.sin(jnp.pi * faces.astype(jnp.float32) / NLAT), jnp.float32(0.0))
    east = jnp.roll(height, -1, axis=2)
    west = jnp.roll(height, 1, axis=2)
    far_east = jnp.roll(height, -2, axis=2)
    face_height = (7.0 * (height + east) - (west + far_east)) / 12.0
    face_speed = 0.5 * (zonal_courant + jnp.roll(zonal_courant, -1, axis=2))
    zonal_flux = face_speed * face_height
    zonal_div = zonal_flux - jnp.roll(zonal_flux, 1, axis=2)
    padded_height = jnp.pad(height, ((2, 2), (0, 0), (0, 0)))
    padded_speed = jnp.pad(merid_courant, ((2, 2), (0, 0), (0, 0)))
    count = NLAT + 1
    merid_face = (7.0 * (padded_height[1:count + 1] + padded_height[2:count + 2]) - (padded_height[0:count] + padded_height[3:count + 3])) / 12.0
    merid_speed = 0.5 * (padded_speed[1:count + 1] + padded_speed[2:count + 2]) * cos_faces[:, None, None]
    merid_flux = merid_speed * merid_face
    merid_div = (merid_flux[1:] - merid_flux[:-1]) / cos_rows[:, None, None]
    source = -rates[None, :, None] * jax.nn.softplus(height - thresholds[None, :, None])
    level_mean = jnp.sum(jnp.sum(source, axis=2) * cos_rows[:, None], axis=0) / (NLON * jnp.sum(cos_rows))
    updated = height - zonal_div - merid_div + source - level_mean[None, :, None]
    waves = jnp.maximum(jnp.arange(NLON // 2 + 1), 1).astype(jnp.float32)
    ratio = cutoffs.astype(jnp.float32)[:, None] / waves[None, :]
    damp = jnp.where(flags[:, None] > 0, jnp.minimum(1.0, ratio * ratio), 1.0)
    spectrum = jnp.fft.rfft(updated, axis=2)
    filtered = jnp.fft.irfft(spectrum * damp[:, None, :], n=NLON, axis=2)
    return filtered.astype(jnp.float32)
```

```python
import functools

import jax
import jax.numpy as jnp
import ml_dtypes
import numpy as np
from jax import lax
from jax.experimental import pallas as pl
from jax.experimental.pallas import tpu as pltpu
from jax.sharding import PartitionSpec as P

LANES = 128


def round_up(value, step):
    return -(-value // step) * step


def split(table):
    high = table.astype(ml_dtypes.bfloat16)
    low = (table - high.astype(np.float64)).astype(ml_dtypes.bfloat16)
    return high, low


@functools.cache
def filter_tables(nlon):
    half = nlon // 2
    width = round_up(half // 2 + 1, LANES)
    depth = round_up(half, LANES)
    n = np.arange(depth)
    m = np.arange(width)
    tables = []
    for odd in (0, 1):
        waves = 2 * m + odd
        angle = 2.0 * np.pi / nlon * (n[:, None] * waves[None, :] % nlon)
        valid = (n[:, None] < half) & (waves[None, :] <= half)
        table = np.concatenate([np.cos(angle) * valid, np.sin(angle) * valid], axis=1)
        tables += [*split(table), *split(np.ascontiguousarray(table.T))]
    return tables


def softplus(s):
    return jnp.maximum(s, 0.0) + jnp.log(1.0 + jnp.exp(-jnp.abs(s)))


def wrapped(row, nlon, full):
    base = nlon // LANES * LANES
    rest = nlon - base
    body, tail = row[:, :base], row[:, base:]
    tail = jnp.concatenate([tail, jnp.zeros((row.shape[0], full - nlon), row.dtype)], axis=1)
    lane = lax.broadcasted_iota(jnp.int32, tail.shape, 1)
    head = pltpu.roll(row[:, : full - base], rest, 1)
    end = pltpu.roll(tail, full - base - rest, 1)
    tail = jnp.where(lane < rest, tail, jnp.where(lane < full - base - 8, head, end))
    return jnp.concatenate([body, tail], axis=1)


def local_kernel(cos_ref, rates_ref, thresholds_ref, h_ref, u_ref, out_ref, sum_ref):
    j = pl.program_id(0)
    rows = pl.num_programs(0)
    nlon = h_ref.shape[2]
    full = round_up(nlon, LANES)
    first = lax.axis_index("lat") * rows
    h0 = h_ref[0]
    s = softplus(h0 - thresholds_ref[...])
    area = s * cos_ref[first + j]
    base = nlon // LANES * LANES
    acc = area[:, 0:LANES]
    for t in range(1, nlon // LANES):
        acc = acc + area[:, t * LANES : (t + 1) * LANES]
    acc = acc + jnp.concatenate(
        [area[:, base:], jnp.zeros((acc.shape[0], full - nlon), jnp.float32)], axis=1
    )
    acc = acc * -rates_ref[...]

    @pl.when(j == 0)
    def _():
        sum_ref[...] = acc

    @pl.when(j > 0)
    def _():
        sum_ref[...] += acc

    h = wrapped(h0, nlon, full)
    u = wrapped(u_ref[0], nlon, full)
    east = pltpu.roll(h, full - 1, 1)
    far_east = pltpu.roll(h, full - 2, 1)
    west = pltpu.roll(h, 1, 1)
    face = (7.0 * (h + east) - (west + far_east)) * (1.0 / 12.0)
    flux = 0.5 * (u + pltpu.roll(u, full - 1, 1)) * face
    div = flux - pltpu.roll(flux, 1, 1)
    out_ref[0] = h0 - div[:, :nlon] - rates_ref[...] * s


def finish_kernel(
    cos_row_ref,
    cos_face_ref,
    flags_ref,
    cutoffs_ref,
    sums_ref,
    h_ref,
    v_ref,
    part_ref,
    a_ref,
    b_ref,
    *rest,
):
    tables, (out_ref, u_ref) = rest[:8], rest[8:]
    rows, levels, nlon = h_ref.shape
    full = round_up(nlon, LANES)
    half = nlon // 2
    depth, cols = tables[0].shape
    width = cols // 2
    position = lax.axis_index("lat")
    first = position * rows
    odd = position % 2 == 1
    area = nlon * float(np.sum(np.sin(np.pi * (np.arange(cos_row_ref.shape[0]) + 0.5) / cos_row_ref.shape[0])))
    mean = jnp.sum(sums_ref[...], axis=1, keepdims=True) * (1.0 / area)

    below = [jnp.where(odd, a_ref[i], b_ref[i]) for i in range(3)]
    above = [jnp.where(odd, b_ref[i], a_ref[i]) for i in range(3)]
    height = [below[0], below[1]] + [h_ref[j] for j in range(rows)] + [above[0], above[1]]
    speed = [below[2]] + [v_ref[j] for j in range(rows)] + [above[2]]
    flux = []
    for f in range(rows + 1):
        p = 7.0 * (height[f + 1] + height[f + 2]) - (height[f] + height[f + 3])
        c = cos_face_ref[first + f] * (0.5 / 12.0)
        flux.append((speed[f] + speed[f + 1]) * c * p)
    marked = flags_ref[first]
    for j in range(1, rows):
        marked = jnp.maximum(marked, flags_ref[first + j])

    def updated(j):
        return part_ref[j] - (flux[j + 1] - flux[j]) * (1.0 / cos_row_ref[first + j])

    @pl.when(marked == 0)
    def _():
        for j in range(rows):
            out_ref[j] = updated(j) - mean

    @pl.when(marked > 0)
    def _():
        u_ref[:, base_of(nlon):] = jnp.zeros((rows * levels, full - base_of(nlon)), jnp.float32)
        for j in range(rows):
            u_ref[j * levels : (j + 1) * levels, :nlon] = updated(j)
        x = u_ref[...]
        near = x[:, :depth]
        far = pltpu.roll(x, full - half, 1)[:, :depth]
        removed = []
        lane = lax.broadcasted_iota(jnp.int32, (1, width), 1)
        for parity in (0, 1):
            y = near + far if parity == 0 else near - far
            fwd_high, fwd_low, inv_high, inv_low = (t[...] for t in tables[4 * parity : 4 * parity + 4])
            spectrum = product(y, fwd_high, fwd_low)
            waves = 2 * lane + parity
            weight = jnp.where((waves > 0) & (waves < half), 2.0 / nlon, 1.0 / nlon)
            inverse = 1.0 / jnp.maximum(waves, 1).astype(jnp.float32)
            pieces = []
            for j in range(rows):
                ratio = cutoffs_ref[first + j].astype(jnp.float32) * inverse
                factor = (1.0 - jnp.minimum(1.0, ratio * ratio)) * weight
                factor = jnp.where(flags_ref[first + j] > 0, factor, 0.0)
                factor = jnp.concatenate([factor, factor], axis=1)
                pieces.append(spectrum[j * levels : (j + 1) * levels] * factor)
            removed.append(product(jnp.concatenate(pieces, axis=0), inv_high, inv_low))
        zeros = jnp.zeros((rows * levels, full - depth), jnp.float32)
        r1 = jnp.concatenate([removed[0] + removed[1], zeros], axis=1)
        r2 = jnp.concatenate([removed[0] - removed[1], zeros], axis=1)
        y = x - r1 - pltpu.roll(r2, half, 1)
        for j in range(rows):
            cut = cutoffs_ref[first + j].astype(jnp.float32)
            kept = jnp.where(flags_ref[first + j] > 0, jnp.minimum(1.0, cut * cut), 1.0)
            out_ref[j] = y[j * levels : (j + 1) * levels, :nlon] - mean * kept


def base_of(nlon):
    return nlon // LANES * LANES


def product(y, high, low):
    y_high = y.astype(jnp.bfloat16)
    y_low = (y - y_high.astype(jnp.float32)).astype(jnp.bfloat16)
    count = y.shape[0]
    both = jnp.dot(
        jnp.concatenate([y_high, y_low], axis=0), high, preferred_element_type=jnp.float32
    )
    return both[:count] + both[count:] + jnp.dot(y_high, low, preferred_element_type=jnp.float32)


def local(height, zonal_courant, merid_courant, rates, thresholds, flags, cutoffs):
    rows, levels, nlon = height.shape
    count = lax.axis_size("lat")
    nlat = rows * count
    odd = lax.axis_index("lat") % 2 == 1
    full = round_up(nlon, LANES)

    def edge(upper):
        two = jnp.where(upper, rows - 2, 0)
        one = jnp.where(upper, rows - 1, 0)
        return jnp.concatenate(
            [
                lax.dynamic_slice_in_dim(height, two, 2, 0),
                lax.dynamic_slice_in_dim(merid_courant, one, 1, 0),
            ]
        )

    between = [(i, i + 1) for i in range(1, count - 1, 2)]
    within = [(i, i + 1) for i in range(0, count - 1, 2)]
    between = between + [(j, i) for i, j in between]
    within = within + [(j, i) for i, j in within]
    b = lax.ppermute(edge(odd), "lat", between)
    a = lax.ppermute(edge(~odd), "lat", within)

    cos_row = jnp.asarray(np.sin(np.pi * (np.arange(nlat) + 0.5) / nlat).astype(np.float32))
    faces = np.sin(np.pi * np.arange(nlat + 1) / nlat)
    faces[0] = faces[nlat] = 0.0
    cos_face = jnp.asarray(faces.astype(np.float32))
    smem = pl.BlockSpec(memory_space=pltpu.SMEM)
    vmem = pl.BlockSpec(memory_space=pltpu.VMEM)
    row_block = pl.BlockSpec((1, levels, nlon), lambda j: (j, 0, 0))
    level_block = pl.BlockSpec((levels, 1), lambda j: (0, 0))
    part, sums = pl.pallas_call(
        local_kernel,
        grid=(rows,),
        in_specs=[smem, level_block, level_block, row_block, row_block],
        out_specs=[row_block, pl.BlockSpec((levels, LANES), lambda j: (0, 0))],
        out_shape=[
            jax.ShapeDtypeStruct(height.shape, jnp.float32),
            jax.ShapeDtypeStruct((levels, LANES), jnp.float32),
        ],
        name="local_part",
    )(cos_row, rates[:, None], thresholds[:, None], height, zonal_courant)

    bits = [1 << i for i in range((count - 1).bit_length())]
    if count == 1 << len(bits):
        for d in [1] + bits[2:] + bits[1:2]:
            sums = sums + lax.ppermute(sums, "lat", [(i, i ^ d) for i in range(count)])
    else:
        sums = lax.psum(sums, "lat")

    return pl.pallas_call(
        finish_kernel,
        in_specs=[smem] * 4 + [vmem] * 14,
        out_specs=vmem,
        out_shape=jax.ShapeDtypeStruct(height.shape, jnp.float32),
        scratch_shapes=[pltpu.VMEM((rows * levels, full), jnp.float32)],
        name="finish",
    )(
        cos_row,
        cos_face,
        flags,
        cutoffs,
        sums,
        height,
        merid_courant,
        part,
        a,
        b,
        *[jnp.asarray(t) for t in filter_tables(nlon)],
    )


def solution(mesh):
    split_rows = P(("member", "lat"), None, None)
    return jax.shard_map(
        local,
        mesh=mesh,
        in_specs=(split_rows, split_rows, split_rows, P("member"), P("member"), P(), P()),
        out_specs=split_rows,
        check_vma=False,
    )
```

```python
import functools

import jax
import jax.numpy as jnp
import numpy as np
from jax import lax
from jax.experimental import pallas as pl
from jax.experimental.pallas import tpu as pltpu
from jax.sharding import PartitionSpec as P

LANES = 128


def round_up(value, step):
    return -(-value // step) * step


@functools.cache
def phases(nlon):
    half = nlon // 2
    width = round_up(half // 2 + 1, LANES)
    depth = round_up(half, LANES)
    points = np.arange(depth)
    arrays = []
    for parity in (0, 1):
        waves = 2 * np.arange(width) + parity
        lanes = (waves <= half)[None, :]

        def both(steps, valid, axis):
            angle = 2.0 * np.pi / nlon * (steps % nlon)
            return np.concatenate([np.cos(angle) * valid, np.sin(angle) * valid], axis=axis)

        blocks = [
            both(points[::8, None] * waves[None, :], lanes & (points[::8, None] < half), 1),
            both(points[:8, None] * waves[None, :], True, 1),
            both(16 * np.arange(width // 8)[:, None] * points[None, :], (points < half)[None, :], 0),
            both(waves[:8, None] * points[None, :], True, 0),
        ]
        columns = max(x.shape[1] for x in blocks)
        arrays.append(
            np.concatenate([np.pad(x, ((0, 0), (0, columns - x.shape[1]))) for x in blocks]).astype(np.float32)
        )
    return arrays


def softplus(s):
    return jnp.maximum(s, 0.0) + jnp.log(1.0 + jnp.exp(-jnp.abs(s)))


def wrapped(row, nlon, full):
    base = nlon // LANES * LANES
    rest = nlon - base
    body, tail = row[:, :base], row[:, base:]
    tail = jnp.concatenate([tail, jnp.zeros((row.shape[0], full - nlon), row.dtype)], axis=1)
    lane = lax.broadcasted_iota(jnp.int32, tail.shape, 1)
    head = pltpu.roll(row[:, : full - base], rest, 1)
    end = pltpu.roll(tail, full - base - rest, 1)
    tail = jnp.where(lane < rest, tail, jnp.where(lane < full - base - 8, head, end))
    return jnp.concatenate([body, tail], axis=1)


def column(row):
    count = row.shape[1]
    same = lax.broadcasted_iota(jnp.int32, (count, count), 0) == lax.broadcasted_iota(
        jnp.int32, (count, count), 1
    )
    return jnp.sum(jnp.where(same, row, 0.0), axis=1, keepdims=True)


def dense_tiles(levels, nlon):
    rest = nlon % LANES
    shared = LANES // rest if rest else 1
    whole = levels // 8 * (nlon // LANES)
    return whole, shared, (-(-(levels // 8) // shared) if rest else 0)


def pack_row(row, out_ref, i):
    levels, nlon = row.shape
    whole, shared, extra = dense_tiles(levels, nlon)
    per = nlon // LANES
    rest = nlon % LANES
    for t in range(whole):
        g, k = divmod(t, per)
        out_ref[i, 8 * t : 8 * t + 8, :] = row[8 * g : 8 * g + 8, k * LANES : (k + 1) * LANES]
    for e in range(extra):
        parts = [
            row[8 * g : 8 * g + 8, per * LANES :]
            for g in range(e * shared, min((e + 1) * shared, levels // 8))
        ]
        parts.append(jnp.zeros((8, LANES - rest * len(parts)), row.dtype))
        t = whole + e
        out_ref[i, 8 * t : 8 * t + 8, :] = jnp.concatenate([p for p in parts if p.shape[1]], axis=1)


def unpack_row(ref, i, levels, nlon):
    whole, shared, _ = dense_tiles(levels, nlon)
    per = nlon // LANES
    rest = nlon % LANES
    groups = []
    for g in range(levels // 8):
        parts = [ref[i, 8 * t : 8 * t + 8, :] for t in range(g * per, (g + 1) * per)]
        if rest:
            t = whole + g // shared
            last = ref[i, 8 * t : 8 * t + 8, :]
            at = g % shared * rest
            parts.append((pltpu.roll(last, LANES - at, 1) if at else last)[:, :rest])
        groups.append(jnp.concatenate(parts, axis=1))
    return jnp.concatenate(groups, axis=0)


def pack_kernel(h_ref, v_ref, out_ref, edge_ref, sem):
    rows = h_ref.shape[0]
    odd = lax.axis_index("lat") % 2 == 1
    two = jnp.where(odd, rows - 2, 0)
    one = jnp.where(odd, rows - 1, 0)
    copies = [
        pltpu.make_async_copy(h_ref.at[pl.ds(two, 2)], edge_ref.at[pl.ds(0, 2)], sem.at[0]),
        pltpu.make_async_copy(v_ref.at[pl.ds(one, 1)], edge_ref.at[pl.ds(2, 1)], sem.at[1]),
    ]
    for c in copies:
        c.start()
    for c in copies:
        c.wait()
    for i in range(3):
        pack_row(edge_ref[i], out_ref, i)


def source_kernel(cos_ref, rates_ref, thresholds_ref, h_ref, v_ref, edge_ref, sum_ref, out_ref):
    rows, levels, nlon = h_ref.shape
    full = round_up(nlon, LANES)
    base = base_of(nlon)
    position = lax.axis_index("lat")
    first = position * rows
    rates = column(rates_ref[...])
    thresholds = column(thresholds_ref[...])
    total = jnp.zeros((levels, LANES), jnp.float32)
    for j in range(rows):
        s = softplus(h_ref[j] - thresholds) * -rates
        out_ref[j] = s
        acc = s[:, 0:LANES]
        for t in range(1, nlon // LANES):
            acc = acc + s[:, t * LANES : (t + 1) * LANES]
        if base < nlon:
            acc = acc + jnp.concatenate(
                [s[:, base:], jnp.zeros((levels, full - nlon), jnp.float32)], axis=1
            )
        total = total + acc * cos_ref[first + j]
    total = jnp.broadcast_to(jnp.sum(total, axis=1, keepdims=True), (levels, LANES))
    sum_ref[...] = total
    even = position % 2 == 0
    two = jnp.where(even, rows - 2, 0)
    one = jnp.where(even, rows - 1, 0)
    edge_ref[0, :, :nlon] = h_ref[two]
    edge_ref[1, :, :nlon] = h_ref[two + 1]
    edge_ref[2, :, :nlon] = v_ref[one]
    edge_ref[3, :, :LANES] = total


def zonal_kernel(h_ref, u_ref, s_ref, out_ref):
    rows, _, nlon = h_ref.shape
    full = round_up(nlon, LANES)
    for j in range(rows):
        h0 = h_ref[j]
        h = wrapped(h0, nlon, full)
        u = wrapped(u_ref[j], nlon, full)
        east = pltpu.roll(h, full - 1, 1)
        far_east = pltpu.roll(h, full - 2, 1)
        west = pltpu.roll(h, 1, 1)
        face = (7.0 * (h + east) - (west + far_east)) * (0.5 / 12.0)
        flux = (u + pltpu.roll(u, full - 1, 1)) * face
        div = flux - pltpu.roll(flux, 1, 1)
        out_ref[j] = h0 - div[:, :nlon] + s_ref[j]


def table_kernel(parity, half, source_ref, high_ref, low_ref, high_t_ref, low_t_ref):
    depth, cols = high_ref.shape
    width = cols // 2

    def put(high, low, at, cols, values):
        h = values.astype(jnp.bfloat16)
        high[at, cols] = h
        low[at, cols] = (values - h.astype(jnp.float32)).astype(jnp.bfloat16)

    def fill(coarse_cos, coarse_sin, fine_cos, fine_sin, count, store):
        for k in range(0, count, 2):
            pieces = []
            for q in (k, k + 1):
                cc, cs = coarse_cos(q), coarse_sin(q)
                pieces.append((cc * fine_cos - cs * fine_sin, cs * fine_cos + cc * fine_sin))
            store(k, *[jnp.concatenate(p, axis=0) for p in zip(*pieces)])

    def store(k, c, s):
        at = slice(8 * k, 8 * k + 16)
        put(high_ref, low_ref, at, slice(0, width), c)
        put(high_ref, low_ref, at, slice(width, cols), s)

    def store_t(k, c, s):
        if 2 * (8 * k + 15) + parity > half:
            waves = 2 * (8 * k + lax.broadcasted_iota(jnp.int32, c.shape, 0)) + parity
            c, s = jnp.where(waves <= half, c, 0.0), jnp.where(waves <= half, s, 0.0)
        put(high_t_ref, low_t_ref, slice(8 * k, 8 * k + 16), slice(None), c)
        put(high_t_ref, low_t_ref, slice(width + 8 * k, width + 8 * k + 16), slice(None), s)

    fine = depth // 8
    turned = fine + 8
    fine_t = turned + 2 * (width // 8)
    fill(
        lambda q: source_ref[q : q + 1, :width],
        lambda q: source_ref[q : q + 1, width:cols],
        source_ref[fine : fine + 8, :width],
        source_ref[fine : fine + 8, width:cols],
        depth // 8,
        store,
    )
    fill(
        lambda q: source_ref[turned + q : turned + q + 1, :depth],
        lambda q: source_ref[turned + width // 8 + q : turned + width // 8 + q + 1, :depth],
        source_ref[fine_t : fine_t + 8, :depth],
        source_ref[fine_t + 8 : fine_t + 16, :depth],
        width // 8,
        store_t,
    )


def finish_kernel(
    cos_row_ref,
    cos_face_ref,
    flags_ref,
    cutoffs_ref,
    sums_ref,
    h_ref,
    v_ref,
    part_ref,
    a_ref,
    b_ref,
    *rest,
):
    tables, (out_ref, u_ref) = rest[:8], rest[8:]
    rows, levels, nlon = h_ref.shape
    full = round_up(nlon, LANES)
    half = nlon // 2
    depth, cols = tables[0].shape
    width = cols // 2
    position = lax.axis_index("lat")
    first = position * rows
    odd = position % 2 == 1
    area = nlon * float(np.sum(np.sin(np.pi * (np.arange(cos_row_ref.shape[0]) + 0.5) / cos_row_ref.shape[0])))
    mean = sums_ref[:, :1] * (1.0 / area)

    b_rows = [unpack_row(b_ref, i, levels, nlon) for i in range(3)]
    below = [jnp.where(odd, a_ref[i], b_rows[i]) for i in range(3)]
    above = [jnp.where(odd, b_rows[i], a_ref[i]) for i in range(3)]
    height = [below[0], below[1]] + [h_ref[j] for j in range(rows)] + [above[0], above[1]]
    speed = [below[2]] + [v_ref[j] for j in range(rows)] + [above[2]]
    flux = []
    for f in range(rows + 1):
        p = 7.0 * (height[f + 1] + height[f + 2]) - (height[f] + height[f + 3])
        c = cos_face_ref[first + f] * (0.5 / 12.0)
        flux.append((speed[f] + speed[f + 1]) * c * p)
    marked = flags_ref[first]
    for j in range(1, rows):
        marked = jnp.maximum(marked, flags_ref[first + j])

    def updated(j):
        return part_ref[j] - (flux[j + 1] - flux[j]) * (1.0 / cos_row_ref[first + j])

    @pl.when(marked == 0)
    def _():
        for j in range(rows):
            out_ref[j] = updated(j) - mean

    @pl.when(marked > 0)
    def _():
        u_ref[:, base_of(nlon):] = jnp.zeros((rows * levels, full - base_of(nlon)), jnp.float32)
        for j in range(rows):
            u_ref[j * levels : (j + 1) * levels, :nlon] = updated(j)
        x = u_ref[...]
        near = x[:, :depth]
        far = pltpu.roll(x, full - half, 1)[:, :depth]
        removed = []
        lane = lax.broadcasted_iota(jnp.int32, (1, width), 1)
        for parity in (0, 1):
            y = near + far if parity == 0 else near - far
            fwd_high, fwd_low, inv_high, inv_low = (t[...] for t in tables[4 * parity : 4 * parity + 4])
            spectrum = product(y, fwd_high, fwd_low)
            waves = 2 * lane + parity
            weight = jnp.where((waves > 0) & (waves < half), 2.0 / nlon, 1.0 / nlon)
            inverse = 1.0 / jnp.maximum(waves, 1).astype(jnp.float32)
            pieces = []
            for j in range(rows):
                ratio = cutoffs_ref[first + j].astype(jnp.float32) * inverse
                factor = (1.0 - jnp.minimum(1.0, ratio * ratio)) * weight
                factor = jnp.where(flags_ref[first + j] > 0, factor, 0.0)
                factor = jnp.concatenate([factor, factor], axis=1)
                pieces.append(spectrum[j * levels : (j + 1) * levels] * factor)
            removed.append(product(jnp.concatenate(pieces, axis=0), inv_high, inv_low))
        zeros = jnp.zeros((rows * levels, full - depth), jnp.float32)
        r1 = jnp.concatenate([removed[0] + removed[1], zeros], axis=1)
        r2 = jnp.concatenate([removed[0] - removed[1], zeros], axis=1)
        y = x - r1 - pltpu.roll(r2, half, 1)
        for j in range(rows):
            cut = cutoffs_ref[first + j].astype(jnp.float32)
            kept = jnp.where(flags_ref[first + j] > 0, jnp.minimum(1.0, cut * cut), 1.0)
            out_ref[j] = y[j * levels : (j + 1) * levels, :nlon] - mean * kept


def base_of(nlon):
    return nlon // LANES * LANES


def product(y, high, low):
    y_high = y.astype(jnp.bfloat16)
    y_low = (y - y_high.astype(jnp.float32)).astype(jnp.bfloat16)
    count = y.shape[0]
    both = jnp.dot(
        jnp.concatenate([y_high, y_low], axis=0), high, preferred_element_type=jnp.float32
    )
    return both[:count] + both[count:] + jnp.dot(y_high, low, preferred_element_type=jnp.float32)


def call(kernel, ins, outs, megabytes, scratch=()):
    return pl.pallas_call(
        kernel,
        in_specs=[pl.BlockSpec(memory_space=space) for _, space in ins],
        out_specs=[pl.BlockSpec(memory_space=pltpu.VMEM) for _ in outs],
        out_shape=[jax.ShapeDtypeStruct(shape, dtype) for shape, dtype in outs],
        scratch_shapes=list(scratch),
        compiler_params=pltpu.CompilerParams(vmem_limit_bytes=megabytes << 20),
    )(*[x for x, _ in ins])


def permute(x, pairs):
    return lax.ppermute(x, "lat", pairs)


def step(height, zonal_courant, merid_courant, rates, thresholds, flags, cutoffs):
    rows, levels, nlon = height.shape
    count = lax.axis_size("lat")
    nlat = rows * count
    full = round_up(nlon, LANES)
    half = nlon // 2
    smem, vmem, hbm = pltpu.SMEM, pltpu.VMEM, pltpu.HBM
    f32 = jnp.float32

    between = [(i, i + 1) for i in range(1, count - 1, 2)]
    within = [(i, i + 1) for i in range(0, count - 1, 2)]
    between = between + [(j, i) for i, j in between]
    within = within + [(j, i) for i, j in within]
    whole, _, extra = dense_tiles(levels, nlon)
    (edge_b,) = call(
        pack_kernel,
        [(height, hbm), (merid_courant, hbm)],
        [((3, 8 * (whole + extra), LANES), f32)],
        4,
        [pltpu.VMEM((3, levels, nlon), f32), pltpu.SemaphoreType.DMA((2,))],
    )
    b = permute(edge_b, between)

    cos_row = jnp.asarray(np.sin(np.pi * (np.arange(nlat) + 0.5) / nlat).astype(np.float32))
    faces = np.sin(np.pi * np.arange(nlat + 1) / nlat)
    faces[0] = faces[nlat] = 0.0
    cos_face = jnp.asarray(faces.astype(np.float32))
    edge_a, sums, source = call(
        source_kernel,
        [(cos_row, smem), (rates[None], vmem), (thresholds[None], vmem), (height, vmem), (merid_courant, vmem)],
        [((4, levels, nlon), f32), ((levels, LANES), f32), (height.shape, f32)],
        8,
    )
    a = permute(edge_a, within)
    (part,) = call(zonal_kernel, [(height, vmem), (zonal_courant, vmem), (source, vmem)], [(height.shape, f32)], 8)
    depth = round_up(half, LANES)
    cols = 2 * round_up(half // 2 + 1, LANES)
    tables = []
    for parity in (0, 1):
        tables += call(
            functools.partial(table_kernel, parity, half),
            [(jnp.asarray(phases(nlon)[parity]), vmem)],
            [((depth, cols), jnp.bfloat16)] * 2 + [((cols, depth), jnp.bfloat16)] * 2,
            8,
        )

    bits = [1 << i for i in range((count - 1).bit_length())]
    if count == 1 << len(bits):
        sums = sums + a[3, :, :LANES]
        for d in bits[2:] + bits[1:2]:
            sums = sums + permute(sums, [(i, i ^ d) for i in range(count)])
    else:
        sums = lax.psum(sums, "lat")

    (out,) = call(
        finish_kernel,
        [(cos_row, smem), (cos_face, smem), (flags, smem), (cutoffs, smem)]
        + [(x, vmem) for x in (sums, height, merid_courant, part, a, b, *tables)],
        [(height.shape, f32)],
        24,
        [pltpu.VMEM((rows * levels, full), f32)],
    )
    return out


def solution(mesh):
    split_rows = P(("member", "lat"), None, None)
    return jax.shard_map(
        step,
        mesh=mesh,
        in_specs=(split_rows, split_rows, split_rows, P("member"), P("member"), P(), P()),
        out_specs=split_rows,
        check_vma=False,
    )
```

```python
import functools

import jax
import jax.numpy as jnp
import numpy as np
from jax import lax
from jax.experimental import pallas as pl
from jax.experimental.pallas import tpu as pltpu
from jax.sharding import PartitionSpec as P

LANES = 128


def round_up(value, step):
    return -(-value // step) * step


@functools.cache
def phases(nlon):
    half = nlon // 2
    width = round_up(half // 2 + 1, LANES)
    depth = round_up(half, LANES)
    points = np.arange(depth)
    arrays = []
    for parity in (0, 1):
        waves = 2 * np.arange(width) + parity
        lanes = (waves <= half)[None, :]

        def both(steps, valid, axis):
            angle = 2.0 * np.pi / nlon * (steps % nlon)
            return np.concatenate([np.cos(angle) * valid, np.sin(angle) * valid], axis=axis)

        blocks = [
            both(points[::8, None] * waves[None, :], lanes & (points[::8, None] < half), 1),
            both(points[:8, None] * waves[None, :], True, 1),
            both(16 * np.arange(width // 8)[:, None] * points[None, :], (points < half)[None, :], 0),
            both(waves[:8, None] * points[None, :], True, 0),
        ]
        columns = max(x.shape[1] for x in blocks)
        arrays.append(
            np.concatenate([np.pad(x, ((0, 0), (0, columns - x.shape[1]))) for x in blocks]).astype(np.float32)
        )
    return arrays


def softplus(s):
    return jnp.maximum(s, 0.0) + jnp.log(1.0 + jnp.exp(-jnp.abs(s)))


def wrapped(row, nlon, full):
    base = nlon // LANES * LANES
    rest = nlon - base
    body, tail = row[:, :base], row[:, base:]
    tail = jnp.concatenate([tail, jnp.zeros((row.shape[0], full - nlon), row.dtype)], axis=1)
    lane = lax.broadcasted_iota(jnp.int32, tail.shape, 1)
    head = pltpu.roll(row[:, : full - base], rest, 1)
    end = pltpu.roll(tail, full - base - rest, 1)
    tail = jnp.where(lane < rest, tail, jnp.where(lane < full - base - 8, head, end))
    return jnp.concatenate([body, tail], axis=1)


def column(row):
    count = row.shape[1]
    same = lax.broadcasted_iota(jnp.int32, (count, count), 0) == lax.broadcasted_iota(
        jnp.int32, (count, count), 1
    )
    return jnp.sum(jnp.where(same, row, 0.0), axis=1, keepdims=True)


def dense_tiles(levels, nlon):
    rest = nlon % LANES
    shared = LANES // rest if rest else 1
    whole = levels // 8 * (nlon // LANES)
    return whole, shared, (-(-(levels // 8) // shared) if rest else 0)


def pack_row(row, out_ref, i):
    levels, nlon = row.shape
    whole, shared, extra = dense_tiles(levels, nlon)
    per = nlon // LANES
    rest = nlon % LANES
    for t in range(whole):
        g, k = divmod(t, per)
        out_ref[i, 8 * t : 8 * t + 8, :] = row[8 * g : 8 * g + 8, k * LANES : (k + 1) * LANES]
    for e in range(extra):
        parts = [
            row[8 * g : 8 * g + 8, per * LANES :]
            for g in range(e * shared, min((e + 1) * shared, levels // 8))
        ]
        parts.append(jnp.zeros((8, LANES - rest * len(parts)), row.dtype))
        t = whole + e
        out_ref[i, 8 * t : 8 * t + 8, :] = jnp.concatenate([p for p in parts if p.shape[1]], axis=1)


def unpack_row(ref, i, levels, nlon):
    whole, shared, _ = dense_tiles(levels, nlon)
    per = nlon // LANES
    rest = nlon % LANES
    groups = []
    for g in range(levels // 8):
        parts = [ref[i, 8 * t : 8 * t + 8, :] for t in range(g * per, (g + 1) * per)]
        if rest:
            t = whole + g // shared
            last = ref[i, 8 * t : 8 * t + 8, :]
            at = g % shared * rest
            parts.append((pltpu.roll(last, LANES - at, 1) if at else last)[:, :rest])
        groups.append(jnp.concatenate(parts, axis=1))
    return jnp.concatenate(groups, axis=0)


def pack_kernel(h_ref, v_ref, out_ref, edge_ref, sem):
    rows = h_ref.shape[0]
    odd = lax.axis_index("lat") % 2 == 1
    two = jnp.where(odd, rows - 2, 0)
    one = jnp.where(odd, rows - 1, 0)
    copies = [
        pltpu.make_async_copy(h_ref.at[pl.ds(two, 2)], edge_ref.at[pl.ds(0, 2)], sem.at[0]),
        pltpu.make_async_copy(v_ref.at[pl.ds(one, 1)], edge_ref.at[pl.ds(2, 1)], sem.at[1]),
    ]
    for c in copies:
        c.start()
    for c in copies:
        c.wait()
    for i in range(3):
        pack_row(edge_ref[i], out_ref, i)


def source_kernel(cos_ref, rates_ref, thresholds_ref, h_ref, v_ref, edge_ref, sum_ref, out_ref):
    rows, levels, nlon = h_ref.shape
    full = round_up(nlon, LANES)
    base = base_of(nlon)
    position = lax.axis_index("lat")
    first = position * rows
    rates = column(rates_ref[...])
    thresholds = column(thresholds_ref[...])
    total = jnp.zeros((levels, LANES), jnp.float32)
    for j in range(rows):
        s = softplus(h_ref[j] - thresholds) * -rates
        out_ref[j] = s
        acc = s[:, 0:LANES]
        for t in range(1, nlon // LANES):
            acc = acc + s[:, t * LANES : (t + 1) * LANES]
        if base < nlon:
            acc = acc + jnp.concatenate(
                [s[:, base:], jnp.zeros((levels, full - nlon), jnp.float32)], axis=1
            )
        total = total + acc * cos_ref[first + j]
    total = jnp.broadcast_to(jnp.sum(total, axis=1, keepdims=True), (levels, LANES))
    sum_ref[...] = total
    even = position % 2 == 0
    two = jnp.where(even, rows - 2, 0)
    one = jnp.where(even, rows - 1, 0)
    edge_ref[0] = h_ref[two]
    edge_ref[1] = h_ref[two + 1]
    edge_ref[2] = v_ref[one]


def zonal_kernel(h_ref, u_ref, s_ref, out_ref):
    rows, _, nlon = h_ref.shape
    full = round_up(nlon, LANES)
    for j in range(rows):
        h0 = h_ref[j]
        h = wrapped(h0, nlon, full)
        u = wrapped(u_ref[j], nlon, full)
        east = pltpu.roll(h, full - 1, 1)
        far_east = pltpu.roll(h, full - 2, 1)
        west = pltpu.roll(h, 1, 1)
        face = (7.0 * (h + east) - (west + far_east)) * (0.5 / 12.0)
        flux = (u + pltpu.roll(u, full - 1, 1)) * face
        div = flux - pltpu.roll(flux, 1, 1)
        out_ref[j] = h0 - div[:, :nlon] + s_ref[j]


def table_kernel(parity, half, source_ref, high_ref, low_ref, high_t_ref, low_t_ref):
    depth, cols = high_ref.shape
    width = cols // 2

    def put(high, low, at, cols, values):
        h = values.astype(jnp.bfloat16)
        high[at, cols] = h
        low[at, cols] = (values - h.astype(jnp.float32)).astype(jnp.bfloat16)

    def fill(coarse_cos, coarse_sin, fine_cos, fine_sin, count, store):
        for k in range(0, count, 2):
            pieces = []
            for q in (k, k + 1):
                cc, cs = coarse_cos(q), coarse_sin(q)
                pieces.append((cc * fine_cos - cs * fine_sin, cs * fine_cos + cc * fine_sin))
            store(k, *[jnp.concatenate(p, axis=0) for p in zip(*pieces)])

    def store(k, c, s):
        at = slice(8 * k, 8 * k + 16)
        put(high_ref, low_ref, at, slice(0, width), c)
        put(high_ref, low_ref, at, slice(width, cols), s)

    def store_t(k, c, s):
        if 2 * (8 * k + 15) + parity > half:
            waves = 2 * (8 * k + lax.broadcasted_iota(jnp.int32, c.shape, 0)) + parity
            c, s = jnp.where(waves <= half, c, 0.0), jnp.where(waves <= half, s, 0.0)
        put(high_t_ref, low_t_ref, slice(8 * k, 8 * k + 16), slice(None), c)
        put(high_t_ref, low_t_ref, slice(width + 8 * k, width + 8 * k + 16), slice(None), s)

    fine = depth // 8
    turned = fine + 8
    fine_t = turned + 2 * (width // 8)
    fill(
        lambda q: source_ref[q : q + 1, :width],
        lambda q: source_ref[q : q + 1, width:cols],
        source_ref[fine : fine + 8, :width],
        source_ref[fine : fine + 8, width:cols],
        depth // 8,
        store,
    )
    fill(
        lambda q: source_ref[turned + q : turned + q + 1, :depth],
        lambda q: source_ref[turned + width // 8 + q : turned + width // 8 + q + 1, :depth],
        source_ref[fine_t : fine_t + 8, :depth],
        source_ref[fine_t + 8 : fine_t + 16, :depth],
        width // 8,
        store_t,
    )


def finish_kernel(
    cos_row_ref,
    cos_face_ref,
    flags_ref,
    cutoffs_ref,
    h_ref,
    v_ref,
    part_ref,
    a_ref,
    b_ref,
    *rest,
):
    tables, (out_ref, kept_ref, u_ref) = rest[:8], rest[8:]
    rows, levels, nlon = h_ref.shape
    full = round_up(nlon, LANES)
    half = nlon // 2
    depth, cols = tables[0].shape
    width = cols // 2
    position = lax.axis_index("lat")
    first = position * rows
    odd = position % 2 == 1
    b_rows = [unpack_row(b_ref, i, levels, nlon) for i in range(3)]
    below = [jnp.where(odd, a_ref[i], b_rows[i]) for i in range(3)]
    above = [jnp.where(odd, b_rows[i], a_ref[i]) for i in range(3)]
    height = [below[0], below[1]] + [h_ref[j] for j in range(rows)] + [above[0], above[1]]
    speed = [below[2]] + [v_ref[j] for j in range(rows)] + [above[2]]
    flux = []
    for f in range(rows + 1):
        p = 7.0 * (height[f + 1] + height[f + 2]) - (height[f] + height[f + 3])
        c = cos_face_ref[first + f] * (0.5 / 12.0)
        flux.append((speed[f] + speed[f + 1]) * c * p)
    marked = flags_ref[first]
    for j in range(1, rows):
        marked = jnp.maximum(marked, flags_ref[first + j])

    def updated(j):
        return part_ref[j] - (flux[j + 1] - flux[j]) * (1.0 / cos_row_ref[first + j])

    @pl.when(marked == 0)
    def _():
        for j in range(rows):
            out_ref[j] = updated(j)

    @pl.when(marked > 0)
    def _():
        u_ref[:, base_of(nlon):] = jnp.zeros((rows * levels, full - base_of(nlon)), jnp.float32)
        for j in range(rows):
            u_ref[j * levels : (j + 1) * levels, :nlon] = updated(j)
        x = u_ref[...]
        near = x[:, :depth]
        far = pltpu.roll(x, full - half, 1)[:, :depth]
        removed = []
        lane = lax.broadcasted_iota(jnp.int32, (1, width), 1)
        for parity in (0, 1):
            y = near + far if parity == 0 else near - far
            fwd_high, fwd_low, inv_high, inv_low = (t[...] for t in tables[4 * parity : 4 * parity + 4])
            spectrum = product(y, fwd_high, fwd_low)
            waves = 2 * lane + parity
            weight = jnp.where((waves > 0) & (waves < half), 2.0 / nlon, 1.0 / nlon)
            inverse = 1.0 / jnp.maximum(waves, 1).astype(jnp.float32)
            pieces = []
            for j in range(rows):
                ratio = cutoffs_ref[first + j].astype(jnp.float32) * inverse
                factor = (1.0 - jnp.minimum(1.0, ratio * ratio)) * weight
                factor = jnp.where(flags_ref[first + j] > 0, factor, 0.0)
                factor = jnp.concatenate([factor, factor], axis=1)
                pieces.append(spectrum[j * levels : (j + 1) * levels] * factor)
            removed.append(product(jnp.concatenate(pieces, axis=0), inv_high, inv_low))
        zeros = jnp.zeros((rows * levels, full - depth), jnp.float32)
        r1 = jnp.concatenate([removed[0] + removed[1], zeros], axis=1)
        r2 = jnp.concatenate([removed[0] - removed[1], zeros], axis=1)
        y = x - r1 - pltpu.roll(r2, half, 1)
        for j in range(rows):
            out_ref[j] = y[j * levels : (j + 1) * levels, :nlon]

    for j in range(rows):
        cut = jnp.full((8, LANES), cutoffs_ref[first + j].astype(jnp.float32))
        kept_ref[j] = jnp.where(flags_ref[first + j] > 0, jnp.minimum(1.0, cut * cut), 1.0)


def mean_kernel(area, sums_ref, kept_ref, part_ref, out_ref, row_ref, sem):
    rows = part_ref.shape[0]
    mean = sums_ref[:, :1] * (1.0 / area)
    copies = []
    for j in range(rows):
        row_ref[j] = part_ref[j] - mean * kept_ref[j, :1, :1]
        copies.append(pltpu.make_async_copy(row_ref.at[j], out_ref.at[j], sem.at[j]))
        copies[-1].start()
    for c in copies:
        c.wait()


def base_of(nlon):
    return nlon // LANES * LANES


def product(y, high, low):
    y_high = y.astype(jnp.bfloat16)
    y_low = (y - y_high.astype(jnp.float32)).astype(jnp.bfloat16)
    count = y.shape[0]
    both = jnp.dot(
        jnp.concatenate([y_high, y_low], axis=0), high, preferred_element_type=jnp.float32
    )
    return both[:count] + both[count:] + jnp.dot(y_high, low, preferred_element_type=jnp.float32)


def call(kernel, ins, outs, megabytes, scratch=(), out_space=pltpu.VMEM):
    return pl.pallas_call(
        kernel,
        in_specs=[pl.BlockSpec(memory_space=space) for _, space in ins],
        out_specs=[pl.BlockSpec(memory_space=out_space) for _ in outs],
        out_shape=[jax.ShapeDtypeStruct(shape, dtype) for shape, dtype in outs],
        scratch_shapes=list(scratch),
        compiler_params=pltpu.CompilerParams(vmem_limit_bytes=megabytes << 20),
    )(*[x for x, _ in ins])


def permute(x, pairs):
    return lax.ppermute(x, "lat", pairs)


def step(height, zonal_courant, merid_courant, rates, thresholds, flags, cutoffs):
    rows, levels, nlon = height.shape
    count = lax.axis_size("lat")
    nlat = rows * count
    full = round_up(nlon, LANES)
    half = nlon // 2
    smem, vmem, hbm = pltpu.SMEM, pltpu.VMEM, pltpu.HBM
    f32 = jnp.float32

    between = [(i, i + 1) for i in range(1, count - 1, 2)]
    within = [(i, i + 1) for i in range(0, count - 1, 2)]
    between = between + [(j, i) for i, j in between]
    within = within + [(j, i) for i, j in within]
    whole, _, extra = dense_tiles(levels, nlon)
    (edge_b,) = call(
        pack_kernel,
        [
            (pltpu.with_memory_space_constraint(height, hbm), hbm),
            (pltpu.with_memory_space_constraint(merid_courant, hbm), hbm),
        ],
        [((3, 8 * (whole + extra), LANES), f32)],
        4,
        [pltpu.VMEM((3, levels, nlon), f32), pltpu.SemaphoreType.DMA((2,))],
    )
    b = permute(edge_b, between)

    cos_row = jnp.asarray(np.sin(np.pi * (np.arange(nlat) + 0.5) / nlat).astype(np.float32))
    faces = np.sin(np.pi * np.arange(nlat + 1) / nlat)
    faces[0] = faces[nlat] = 0.0
    cos_face = jnp.asarray(faces.astype(np.float32))
    edge_a, sums, source = call(
        source_kernel,
        [(cos_row, smem), (rates[None], vmem), (thresholds[None], vmem), (height, vmem), (merid_courant, vmem)],
        [((3, levels, nlon), f32), ((levels, LANES), f32), (height.shape, f32)],
        8,
    )
    a = permute(edge_a, within)
    (part,) = call(zonal_kernel, [(height, vmem), (zonal_courant, vmem), (source, vmem)], [(height.shape, f32)], 8)
    depth = round_up(half, LANES)
    cols = 2 * round_up(half // 2 + 1, LANES)
    tables = []
    for parity in (0, 1):
        tables += call(
            functools.partial(table_kernel, parity, half),
            [(jnp.asarray(phases(nlon)[parity]), vmem)],
            [((depth, cols), jnp.bfloat16)] * 2 + [((cols, depth), jnp.bfloat16)] * 2,
            8,
        )

    bits = [1 << i for i in range((count - 1).bit_length())]
    if count == 1 << len(bits):
        for d in bits[:1] + bits[2:] + bits[1:2]:
            sums = sums + permute(sums, [(i, i ^ d) for i in range(count)])
    else:
        sums = lax.psum(sums, "lat")

    part, kept = call(
        finish_kernel,
        [(cos_row, smem), (cos_face, smem), (flags, smem), (cutoffs, smem)]
        + [(x, vmem) for x in (height, merid_courant, part, a, b, *tables)],
        [(height.shape, f32), ((rows, 8, LANES), f32)],
        24,
        [pltpu.VMEM((rows * levels, full), f32)],
    )
    area = nlon * float(np.sum(np.sin(np.pi * (np.arange(nlat) + 0.5) / nlat)))
    (out,) = call(
        functools.partial(mean_kernel, area),
        [(sums, vmem), (kept, vmem), (part, vmem)],
        [(height.shape, f32)],
        4,
        [pltpu.VMEM(height.shape, f32), pltpu.SemaphoreType.DMA((rows,))],
        hbm,
    )
    return out


def solution(mesh):
    split_rows = P(("member", "lat"), None, None)
    return jax.shard_map(
        step,
        mesh=mesh,
        in_specs=(split_rows, split_rows, split_rows, P("member"), P("member"), P(), P()),
        out_specs=split_rows,
        check_vma=False,
    )
```

```python
import functools

import jax
import jax.numpy as jnp
import numpy as np
from jax import lax
from jax.experimental import pallas as pl
from jax.experimental.pallas import tpu as pltpu
from jax.sharding import PartitionSpec as P

LANES = 128


def round_up(value, step):
    return -(-value // step) * step


@functools.cache
def phases(nlon):
    half = nlon // 2
    width = round_up(half // 2 + 1, LANES)
    depth = round_up(half, LANES)
    points = np.arange(depth)
    arrays = []
    for parity in (0, 1):
        waves = 2 * np.arange(width) + parity
        lanes = (waves <= half)[None, :]

        def both(steps, valid, axis):
            angle = 2.0 * np.pi / nlon * (steps % nlon)
            return np.concatenate([np.cos(angle) * valid, np.sin(angle) * valid], axis=axis)

        blocks = [
            both(points[::8, None] * waves[None, :], lanes & (points[::8, None] < half), 1),
            both(points[:8, None] * waves[None, :], True, 1),
            both(16 * np.arange(width // 8)[:, None] * points[None, :], (points < half)[None, :], 0),
            both(waves[:8, None] * points[None, :], True, 0),
        ]
        columns = max(x.shape[1] for x in blocks)
        arrays.append(
            np.concatenate([np.pad(x, ((0, 0), (0, columns - x.shape[1]))) for x in blocks]).astype(np.float32)
        )
    return arrays


def softplus(s):
    return jnp.maximum(s, 0.0) + jnp.log(1.0 + jnp.exp(-jnp.abs(s)))


def wrapped(row, nlon, full):
    base = nlon // LANES * LANES
    rest = nlon - base
    body, tail = row[:, :base], row[:, base:]
    tail = jnp.concatenate([tail, jnp.zeros((row.shape[0], full - nlon), row.dtype)], axis=1)
    lane = lax.broadcasted_iota(jnp.int32, tail.shape, 1)
    head = pltpu.roll(row[:, : full - base], rest, 1)
    end = pltpu.roll(tail, full - base - rest, 1)
    tail = jnp.where(lane < rest, tail, jnp.where(lane < full - base - 8, head, end))
    return jnp.concatenate([body, tail], axis=1)


def column(row):
    count = row.shape[1]
    same = lax.broadcasted_iota(jnp.int32, (count, count), 0) == lax.broadcasted_iota(
        jnp.int32, (count, count), 1
    )
    return jnp.sum(jnp.where(same, row, 0.0), axis=1, keepdims=True)


def dense_tiles(levels, nlon):
    rest = nlon % LANES
    shared = LANES // rest if rest else 1
    whole = levels // 8 * (nlon // LANES)
    return whole, shared, (-(-(levels // 8) // shared) if rest else 0)


def pack_row(row, out_ref, i):
    levels, nlon = row.shape
    whole, shared, extra = dense_tiles(levels, nlon)
    per = nlon // LANES
    rest = nlon % LANES
    for t in range(whole):
        g, k = divmod(t, per)
        out_ref[i, 8 * t : 8 * t + 8, :] = row[8 * g : 8 * g + 8, k * LANES : (k + 1) * LANES]
    for e in range(extra):
        parts = [
            row[8 * g : 8 * g + 8, per * LANES :]
            for g in range(e * shared, min((e + 1) * shared, levels // 8))
        ]
        parts.append(jnp.zeros((8, LANES - rest * len(parts)), row.dtype))
        t = whole + e
        out_ref[i, 8 * t : 8 * t + 8, :] = jnp.concatenate([p for p in parts if p.shape[1]], axis=1)


def unpack_row(ref, i, levels, nlon):
    whole, shared, _ = dense_tiles(levels, nlon)
    per = nlon // LANES
    rest = nlon % LANES
    groups = []
    for g in range(levels // 8):
        parts = [ref[i, 8 * t : 8 * t + 8, :] for t in range(g * per, (g + 1) * per)]
        if rest:
            t = whole + g // shared
            last = ref[i, 8 * t : 8 * t + 8, :]
            at = g % shared * rest
            parts.append((pltpu.roll(last, LANES - at, 1) if at else last)[:, :rest])
        groups.append(jnp.concatenate(parts, axis=1))
    return jnp.concatenate(groups, axis=0)


def pack_kernel(h_ref, v_ref, out_ref, edge_ref, sem):
    rows = h_ref.shape[0]
    odd = lax.axis_index("lat") % 2 == 1
    two = jnp.where(odd, rows - 2, 0)
    one = jnp.where(odd, rows - 1, 0)
    copies = [
        pltpu.make_async_copy(h_ref.at[pl.ds(two, 2)], edge_ref.at[pl.ds(0, 2)], sem.at[0]),
        pltpu.make_async_copy(v_ref.at[pl.ds(one, 1)], edge_ref.at[pl.ds(2, 1)], sem.at[1]),
    ]
    for c in copies:
        c.start()
    for c in copies:
        c.wait()
    for i in range(3):
        pack_row(edge_ref[i], out_ref, i)


def source_kernel(cos_ref, rates_ref, thresholds_ref, h_ref, v_ref, edge_ref, sum_ref, out_ref):
    rows, levels, nlon = h_ref.shape
    full = round_up(nlon, LANES)
    base = base_of(nlon)
    position = lax.axis_index("lat")
    first = position * rows
    rates = column(rates_ref[...])
    thresholds = column(thresholds_ref[...])
    total = jnp.zeros((levels, LANES), jnp.float32)
    for j in range(rows):
        s = softplus(h_ref[j] - thresholds) * -rates
        out_ref[j] = s
        acc = s[:, 0:LANES]
        for t in range(1, nlon // LANES):
            acc = acc + s[:, t * LANES : (t + 1) * LANES]
        if base < nlon:
            acc = acc + jnp.concatenate(
                [s[:, base:], jnp.zeros((levels, full - nlon), jnp.float32)], axis=1
            )
        total = total + acc * cos_ref[first + j]
    total = jnp.broadcast_to(jnp.sum(total, axis=1, keepdims=True), (levels, LANES))
    sum_ref[...] = total
    even = position % 2 == 0
    two = jnp.where(even, rows - 2, 0)
    one = jnp.where(even, rows - 1, 0)
    edge_ref[0] = h_ref[two]
    edge_ref[1] = h_ref[two + 1]
    edge_ref[2] = v_ref[one]


def zonal_kernel(h_ref, u_ref, s_ref, out_ref):
    rows, _, nlon = h_ref.shape
    full = round_up(nlon, LANES)
    for j in range(rows):
        h0 = h_ref[j]
        h = wrapped(h0, nlon, full)
        u = wrapped(u_ref[j], nlon, full)
        east = pltpu.roll(h, full - 1, 1)
        far_east = pltpu.roll(h, full - 2, 1)
        west = pltpu.roll(h, 1, 1)
        face = (7.0 * (h + east) - (west + far_east)) * (0.5 / 12.0)
        flux = (u + pltpu.roll(u, full - 1, 1)) * face
        div = flux - pltpu.roll(flux, 1, 1)
        out_ref[j] = h0 - div[:, :nlon] + s_ref[j]


def table_kernel(parity, half, source_ref, high_ref, low_ref, high_t_ref, low_t_ref):
    depth, cols = high_ref.shape
    width = cols // 2

    def put(high, low, at, cols, values):
        h = values.astype(jnp.bfloat16)
        high[at, cols] = h
        low[at, cols] = (values - h.astype(jnp.float32)).astype(jnp.bfloat16)

    def fill(coarse_cos, coarse_sin, fine_cos, fine_sin, count, store):
        for k in range(0, count, 2):
            pieces = []
            for q in (k, k + 1):
                cc, cs = coarse_cos(q), coarse_sin(q)
                pieces.append((cc * fine_cos - cs * fine_sin, cs * fine_cos + cc * fine_sin))
            store(k, *[jnp.concatenate(p, axis=0) for p in zip(*pieces)])

    def store(k, c, s):
        at = slice(8 * k, 8 * k + 16)
        put(high_ref, low_ref, at, slice(0, width), c)
        put(high_ref, low_ref, at, slice(width, cols), s)

    def store_t(k, c, s):
        if 2 * (8 * k + 15) + parity > half:
            waves = 2 * (8 * k + lax.broadcasted_iota(jnp.int32, c.shape, 0)) + parity
            c, s = jnp.where(waves <= half, c, 0.0), jnp.where(waves <= half, s, 0.0)
        put(high_t_ref, low_t_ref, slice(8 * k, 8 * k + 16), slice(None), c)
        put(high_t_ref, low_t_ref, slice(width + 8 * k, width + 8 * k + 16), slice(None), s)

    fine = depth // 8
    turned = fine + 8
    fine_t = turned + 2 * (width // 8)
    fill(
        lambda q: source_ref[q : q + 1, :width],
        lambda q: source_ref[q : q + 1, width:cols],
        source_ref[fine : fine + 8, :width],
        source_ref[fine : fine + 8, width:cols],
        depth // 8,
        store,
    )
    fill(
        lambda q: source_ref[turned + q : turned + q + 1, :depth],
        lambda q: source_ref[turned + width // 8 + q : turned + width // 8 + q + 1, :depth],
        source_ref[fine_t : fine_t + 8, :depth],
        source_ref[fine_t + 8 : fine_t + 16, :depth],
        width // 8,
        store_t,
    )


def finish_kernel(
    cos_row_ref,
    cos_face_ref,
    flags_ref,
    cutoffs_ref,
    h_ref,
    v_ref,
    part_ref,
    a_ref,
    b_ref,
    *rest,
):
    tables, (out_ref, kept_ref, u_ref) = rest[:8], rest[8:]
    rows, levels, nlon = h_ref.shape
    full = round_up(nlon, LANES)
    half = nlon // 2
    depth, cols = tables[0].shape
    width = cols // 2
    position = lax.axis_index("lat")
    first = position * rows
    odd = position % 2 == 1
    b_rows = [unpack_row(b_ref, i, levels, nlon) for i in range(3)]
    last = lax.axis_size("lat") - 1
    below = [jnp.where(odd, a_ref[i], jnp.where(position == 0, 0.0, b_rows[i])) for i in range(3)]
    above = [jnp.where(odd, jnp.where(position == last, 0.0, b_rows[i]), a_ref[i]) for i in range(3)]
    height = [below[0], below[1]] + [h_ref[j] for j in range(rows)] + [above[0], above[1]]
    speed = [below[2]] + [v_ref[j] for j in range(rows)] + [above[2]]
    flux = []
    for f in range(rows + 1):
        p = 7.0 * (height[f + 1] + height[f + 2]) - (height[f] + height[f + 3])
        c = cos_face_ref[first + f] * (0.5 / 12.0)
        flux.append((speed[f] + speed[f + 1]) * c * p)
    marked = flags_ref[first]
    for j in range(1, rows):
        marked = jnp.maximum(marked, flags_ref[first + j])

    def updated(j):
        return part_ref[j] - (flux[j + 1] - flux[j]) * (1.0 / cos_row_ref[first + j])

    @pl.when(marked == 0)
    def _():
        for j in range(rows):
            out_ref[j] = updated(j)

    @pl.when(marked > 0)
    def _():
        u_ref[:, base_of(nlon):] = jnp.zeros((rows * levels, full - base_of(nlon)), jnp.float32)
        for j in range(rows):
            u_ref[j * levels : (j + 1) * levels, :nlon] = updated(j)
        x = u_ref[...]
        near = x[:, :depth]
        far = pltpu.roll(x, full - half, 1)[:, :depth]
        removed = []
        lane = lax.broadcasted_iota(jnp.int32, (1, width), 1)
        for parity in (0, 1):
            y = near + far if parity == 0 else near - far
            fwd_high, fwd_low, inv_high, inv_low = (t[...] for t in tables[4 * parity : 4 * parity + 4])
            spectrum = product(y, fwd_high, fwd_low)
            waves = 2 * lane + parity
            weight = jnp.where((waves > 0) & (waves < half), 2.0 / nlon, 1.0 / nlon)
            inverse = 1.0 / jnp.maximum(waves, 1).astype(jnp.float32)
            pieces = []
            for j in range(rows):
                ratio = cutoffs_ref[first + j].astype(jnp.float32) * inverse
                factor = (1.0 - jnp.minimum(1.0, ratio * ratio)) * weight
                factor = jnp.where(flags_ref[first + j] > 0, factor, 0.0)
                factor = jnp.concatenate([factor, factor], axis=1)
                pieces.append(spectrum[j * levels : (j + 1) * levels] * factor)
            removed.append(product(jnp.concatenate(pieces, axis=0), inv_high, inv_low))
        zeros = jnp.zeros((rows * levels, full - depth), jnp.float32)
        r1 = jnp.concatenate([removed[0] + removed[1], zeros], axis=1)
        r2 = jnp.concatenate([removed[0] - removed[1], zeros], axis=1)
        y = x - r1 - pltpu.roll(r2, half, 1)
        for j in range(rows):
            out_ref[j] = y[j * levels : (j + 1) * levels, :nlon]

    for j in range(rows):
        cut = jnp.full((8, LANES), cutoffs_ref[first + j].astype(jnp.float32))
        kept_ref[j] = jnp.where(flags_ref[first + j] > 0, jnp.minimum(1.0, cut * cut), 1.0)


def mean_kernel(area, sums_ref, kept_ref, part_ref, out_ref, row_ref, sem):
    rows = part_ref.shape[0]
    mean = sums_ref[:, :1] * (1.0 / area)
    copies = []
    for j in range(rows):
        row_ref[j] = part_ref[j] - mean * kept_ref[j, :1, :1]
        copies.append(pltpu.make_async_copy(row_ref.at[j], out_ref.at[j], sem.at[j]))
        copies[-1].start()
    for c in copies:
        c.wait()


def base_of(nlon):
    return nlon // LANES * LANES


def product(y, high, low):
    y_high = y.astype(jnp.bfloat16)
    y_low = (y - y_high.astype(jnp.float32)).astype(jnp.bfloat16)
    count = y.shape[0]
    both = jnp.dot(
        jnp.concatenate([y_high, y_low], axis=0), high, preferred_element_type=jnp.float32
    )
    return both[:count] + both[count:] + jnp.dot(y_high, low, preferred_element_type=jnp.float32)


def call(kernel, ins, outs, megabytes, scratch=(), out_space=pltpu.VMEM):
    return pl.pallas_call(
        kernel,
        in_specs=[pl.BlockSpec(memory_space=space) for _, space in ins],
        out_specs=[pl.BlockSpec(memory_space=out_space) for _ in outs],
        out_shape=[jax.ShapeDtypeStruct(shape, dtype) for shape, dtype in outs],
        scratch_shapes=list(scratch),
        compiler_params=pltpu.CompilerParams(vmem_limit_bytes=megabytes << 20),
    )(*[x for x, _ in ins])


def permute(x, pairs, axes="lat"):
    return lax.ppermute(x, axes, pairs)


def step(height, zonal_courant, merid_courant, rates, thresholds, flags, cutoffs):
    rows, levels, nlon = height.shape
    count = lax.axis_size("lat")
    nlat = rows * count
    full = round_up(nlon, LANES)
    half = nlon // 2
    smem, vmem, hbm = pltpu.SMEM, pltpu.VMEM, pltpu.HBM
    f32 = jnp.float32

    between = [(i, i + 1) for i in range(1, count - 1, 2)]
    within = [(i, i + 1) for i in range(0, count - 1, 2)]
    between = between + [(j, i) for i, j in between]
    parts = lax.axis_size("member")
    between = [(p * count + i, p * count + j) for p in range(parts) for i, j in between]
    ends = [0, count - 1] if count % 2 == 0 else [0]
    if parts % 2 == 0:
        between += [(p * count + e, (p ^ 1) * count + e) for p in range(parts) for e in ends]
    within = within + [(j, i) for i, j in within]
    whole, _, extra = dense_tiles(levels, nlon)
    (edge_b,) = call(
        pack_kernel,
        [
            (pltpu.with_memory_space_constraint(height, hbm), hbm),
            (pltpu.with_memory_space_constraint(merid_courant, hbm), hbm),
        ],
        [((3, 8 * (whole + extra), LANES), f32)],
        4,
        [pltpu.VMEM((3, levels, nlon), f32), pltpu.SemaphoreType.DMA((2,))],
    )
    b = permute(edge_b, between, ("member", "lat"))

    cos_row = jnp.asarray(np.sin(np.pi * (np.arange(nlat) + 0.5) / nlat).astype(np.float32))
    faces = np.sin(np.pi * np.arange(nlat + 1) / nlat)
    faces[0] = faces[nlat] = 0.0
    cos_face = jnp.asarray(faces.astype(np.float32))
    edge_a, sums, source = call(
        source_kernel,
        [(cos_row, smem), (rates[None], vmem), (thresholds[None], vmem), (height, vmem), (merid_courant, vmem)],
        [((3, levels, nlon), f32), ((levels, LANES), f32), (height.shape, f32)],
        8,
    )
    a = permute(edge_a, within)
    (part,) = call(zonal_kernel, [(height, vmem), (zonal_courant, vmem), (source, vmem)], [(height.shape, f32)], 8)
    depth = round_up(half, LANES)
    cols = 2 * round_up(half // 2 + 1, LANES)
    tables = []
    for parity in (0, 1):
        tables += call(
            functools.partial(table_kernel, parity, half),
            [(jnp.asarray(phases(nlon)[parity]), vmem)],
            [((depth, cols), jnp.bfloat16)] * 2 + [((cols, depth), jnp.bfloat16)] * 2,
            8,
        )

    bits = [1 << i for i in range((count - 1).bit_length())]
    if count == 1 << len(bits):
        for d in bits[:1] + bits[2:] + bits[1:2]:
            sums = sums + permute(sums, [(i, i ^ d) for i in range(count)])
    else:
        sums = lax.psum(sums, "lat")

    part, kept = call(
        finish_kernel,
        [(cos_row, smem), (cos_face, smem), (flags, smem), (cutoffs, smem)]
        + [(x, vmem) for x in (height, merid_courant, part, a, b, *tables)],
        [(height.shape, f32), ((rows, 8, LANES), f32)],
        24,
        [pltpu.VMEM((rows * levels, full), f32)],
    )
    area = nlon * float(np.sum(np.sin(np.pi * (np.arange(nlat) + 0.5) / nlat)))
    (out,) = call(
        functools.partial(mean_kernel, area),
        [(sums, vmem), (kept, vmem), (part, vmem)],
        [(height.shape, f32)],
        4,
        [pltpu.VMEM(height.shape, f32), pltpu.SemaphoreType.DMA((rows,))],
        hbm,
    )
    return out


def solution(mesh):
    split_rows = P(("member", "lat"), None, None)
    return jax.shard_map(
        step,
        mesh=mesh,
        in_specs=(split_rows, split_rows, split_rows, P("member"), P("member"), P(), P()),
        out_specs=split_rows,
        check_vma=False,
    )
```

```python
import functools

import jax
import jax.numpy as jnp
import numpy as np
from jax import lax
from jax.experimental import pallas as pl
from jax.experimental.pallas import tpu as pltpu
from jax.sharding import PartitionSpec as P

LANES = 128


def round_up(value, step):
    return -(-value // step) * step


@functools.cache
def phases(nlon):
    half = nlon // 2
    width = round_up(half // 2 + 1, LANES)
    depth = round_up(half, LANES)
    points = np.arange(depth)
    arrays = []
    for parity in (0, 1):
        waves = 2 * np.arange(width) + parity
        lanes = (waves <= half)[None, :]

        def both(steps, valid, axis):
            angle = 2.0 * np.pi / nlon * (steps % nlon)
            return np.concatenate([np.cos(angle) * valid, np.sin(angle) * valid], axis=axis)

        blocks = [
            both(points[::8, None] * waves[None, :], lanes & (points[::8, None] < half), 1),
            both(points[:8, None] * waves[None, :], True, 1),
            both(16 * np.arange(width // 8)[:, None] * points[None, :], (points < half)[None, :], 0),
            both(waves[:8, None] * points[None, :], True, 0),
        ]
        columns = max(x.shape[1] for x in blocks)
        arrays.append(
            np.concatenate([np.pad(x, ((0, 0), (0, columns - x.shape[1]))) for x in blocks]).astype(np.float32)
        )
    return arrays


def softplus(s):
    return jnp.maximum(s, 0.0) + jnp.log(1.0 + jnp.exp(-jnp.abs(s)))


def wrapped(row, nlon, full):
    base = nlon // LANES * LANES
    rest = nlon - base
    body, tail = row[:, :base], row[:, base:]
    tail = jnp.concatenate([tail, jnp.zeros((row.shape[0], full - nlon), row.dtype)], axis=1)
    lane = lax.broadcasted_iota(jnp.int32, tail.shape, 1)
    head = pltpu.roll(row[:, : full - base], rest, 1)
    end = pltpu.roll(tail, full - base - rest, 1)
    tail = jnp.where(lane < rest, tail, jnp.where(lane < full - base - 8, head, end))
    return jnp.concatenate([body, tail], axis=1)


def column(row):
    count = row.shape[1]
    same = lax.broadcasted_iota(jnp.int32, (count, count), 0) == lax.broadcasted_iota(
        jnp.int32, (count, count), 1
    )
    return jnp.sum(jnp.where(same, row, 0.0), axis=1, keepdims=True)


def dense_tiles(levels, nlon):
    rest = nlon % LANES
    shared = LANES // rest if rest else 1
    whole = levels // 8 * (nlon // LANES)
    return whole, shared, (-(-(levels // 8) // shared) if rest else 0)


def pack_row(row, out_ref, i):
    levels, nlon = row.shape
    whole, shared, extra = dense_tiles(levels, nlon)
    per = nlon // LANES
    rest = nlon % LANES
    for t in range(whole):
        g, k = divmod(t, per)
        out_ref[i, 8 * t : 8 * t + 8, :] = row[8 * g : 8 * g + 8, k * LANES : (k + 1) * LANES]
    for e in range(extra):
        parts = [
            row[8 * g : 8 * g + 8, per * LANES :]
            for g in range(e * shared, min((e + 1) * shared, levels // 8))
        ]
        parts.append(jnp.zeros((8, LANES - rest * len(parts)), row.dtype))
        t = whole + e
        out_ref[i, 8 * t : 8 * t + 8, :] = jnp.concatenate([p for p in parts if p.shape[1]], axis=1)


def packed_tile(ref, i, g, k, levels, nlon):
    whole, shared, _ = dense_tiles(levels, nlon)
    per = nlon // LANES
    rest = nlon % LANES
    if k < per:
        t = g * per + k
        return ref[i, 8 * t : 8 * t + 8, :]
    t = whole + g // shared
    last = ref[i, 8 * t : 8 * t + 8, :]
    at = g % shared * rest
    return (pltpu.roll(last, LANES - at, 1) if at else last)[:, :rest]


def pack_kernel(h_ref, v_ref, out_ref, edge_ref, sem):
    rows = h_ref.shape[0]
    odd = lax.axis_index("lat") % 2 == 1
    two = jnp.where(odd, rows - 2, 0)
    one = jnp.where(odd, rows - 1, 0)
    copies = [
        pltpu.make_async_copy(h_ref.at[pl.ds(two, 2)], edge_ref.at[pl.ds(0, 2)], sem.at[0]),
        pltpu.make_async_copy(v_ref.at[pl.ds(one, 1)], edge_ref.at[pl.ds(2, 1)], sem.at[1]),
    ]
    for c in copies:
        c.start()
    for c in copies:
        c.wait()
    for i in range(3):
        pack_row(edge_ref[i], out_ref, i)


def source_kernel(cos_ref, rates_ref, thresholds_ref, h_ref, v_ref, edge_ref, sum_ref, out_ref):
    rows, levels, nlon = h_ref.shape
    full = round_up(nlon, LANES)
    base = base_of(nlon)
    position = lax.axis_index("lat")
    first = position * rows
    rates = column(rates_ref[...])
    thresholds = column(thresholds_ref[...])
    total = jnp.zeros((levels, LANES), jnp.float32)
    for j in range(rows):
        s = softplus(h_ref[j] - thresholds) * -rates
        out_ref[j] = s
        acc = s[:, 0:LANES]
        for t in range(1, nlon // LANES):
            acc = acc + s[:, t * LANES : (t + 1) * LANES]
        if base < nlon:
            acc = acc + jnp.concatenate(
                [s[:, base:], jnp.zeros((levels, full - nlon), jnp.float32)], axis=1
            )
        total = total + acc * cos_ref[first + j]
    total = jnp.broadcast_to(jnp.sum(total, axis=1, keepdims=True), (levels, LANES))
    sum_ref[...] = total
    even = position % 2 == 0
    two = jnp.where(even, rows - 2, 0)
    one = jnp.where(even, rows - 1, 0)
    edge_ref[0] = h_ref[two]
    edge_ref[1] = h_ref[two + 1]
    edge_ref[2] = v_ref[one]


def zonal_kernel(h_ref, u_ref, s_ref, out_ref):
    rows, levels, nlon = h_ref.shape
    full = round_up(nlon, LANES)
    for j in range(rows):
        for g in range(0, levels, 16):
            at = slice(g, g + 16)
            h0 = h_ref[j, at, :]
            h = wrapped(h0, nlon, full)
            u = wrapped(u_ref[j, at, :], nlon, full)
            face = 7.0 * (h + pltpu.roll(h, full - 1, 1))
            face = face - (pltpu.roll(h, 1, 1) + pltpu.roll(h, full - 2, 1))
            flux = (u + pltpu.roll(u, full - 1, 1)) * (face * (0.5 / 12.0))
            div = flux - pltpu.roll(flux, 1, 1)
            out_ref[j, at, :] = h0 - div[:, :nlon] + s_ref[j, at, :]


def table_kernel(parity, half, source_ref, high_ref, low_ref, high_t_ref, low_t_ref):
    depth, cols = high_ref.shape
    width = cols // 2

    def put(high, low, at, cols, values):
        h = values.astype(jnp.bfloat16)
        high[at, cols] = h
        low[at, cols] = (values - h.astype(jnp.float32)).astype(jnp.bfloat16)

    def fill(coarse_cos, coarse_sin, fine_cos, fine_sin, count, store):
        for k in range(0, count, 2):
            pieces = []
            for q in (k, k + 1):
                cc, cs = coarse_cos(q), coarse_sin(q)
                pieces.append((cc * fine_cos - cs * fine_sin, cs * fine_cos + cc * fine_sin))
            store(k, *[jnp.concatenate(p, axis=0) for p in zip(*pieces)])

    def store(k, c, s):
        at = slice(8 * k, 8 * k + 16)
        put(high_ref, low_ref, at, slice(0, width), c)
        put(high_ref, low_ref, at, slice(width, cols), s)

    def store_t(k, c, s):
        if 2 * (8 * k + 15) + parity > half:
            waves = 2 * (8 * k + lax.broadcasted_iota(jnp.int32, c.shape, 0)) + parity
            c, s = jnp.where(waves <= half, c, 0.0), jnp.where(waves <= half, s, 0.0)
        put(high_t_ref, low_t_ref, slice(8 * k, 8 * k + 16), slice(None), c)
        put(high_t_ref, low_t_ref, slice(width + 8 * k, width + 8 * k + 16), slice(None), s)

    fine = depth // 8
    turned = fine + 8
    fine_t = turned + 2 * (width // 8)
    fill(
        lambda q: source_ref[q : q + 1, :width],
        lambda q: source_ref[q : q + 1, width:cols],
        source_ref[fine : fine + 8, :width],
        source_ref[fine : fine + 8, width:cols],
        depth // 8,
        store,
    )
    fill(
        lambda q: source_ref[turned + q : turned + q + 1, :depth],
        lambda q: source_ref[turned + width // 8 + q : turned + width // 8 + q + 1, :depth],
        source_ref[fine_t : fine_t + 8, :depth],
        source_ref[fine_t + 8 : fine_t + 16, :depth],
        width // 8,
        store_t,
    )


def finish_kernel(
    cos_row_ref,
    cos_face_ref,
    flags_ref,
    cutoffs_ref,
    h_ref,
    v_ref,
    part_ref,
    a_ref,
    b_ref,
    *rest,
):
    tables, (out_ref, kept_ref, y_ref, s_ref, d_ref) = rest[:8], rest[8:]
    rows, levels, nlon = h_ref.shape
    full = round_up(nlon, LANES)
    half = nlon // 2
    depth, cols = tables[0].shape
    width = cols // 2
    units = rows * levels
    position = lax.axis_index("lat")
    last = lax.axis_size("lat") - 1
    first = position * rows
    odd = position % 2 == 1
    bottom, top = position == 0, position == last
    marked = flags_ref[first]
    for j in range(1, rows):
        marked = jnp.maximum(marked, flags_ref[first + j])
    inverse_cos = [1.0 / jnp.full((8, LANES), cos_row_ref[first + j]) for j in range(rows)]
    face_cos = [cos_face_ref[first + f] * (0.5 / 12.0) for f in range(rows + 1)]

    for g in range(levels // 8):
        at = slice(8 * g, 8 * g + 8)
        for k in range(full // LANES):
            lanes = slice(k * LANES, min((k + 1) * LANES, nlon))
            wide = lanes.stop - lanes.start
            near = [a_ref[i, at, lanes] for i in range(3)]
            far = [packed_tile(b_ref, i, g, k, levels, nlon) for i in range(3)]
            below = [jnp.where(odd, x, jnp.where(bottom, 0.0, y)) for x, y in zip(near, far)]
            above = [jnp.where(odd, jnp.where(top, 0.0, y), x) for x, y in zip(near, far)]
            height = [below[0], below[1], *(h_ref[j, at, lanes] for j in range(rows)), above[0], above[1]]
            speed = [below[2], *(v_ref[j, at, lanes] for j in range(rows)), above[2]]
            flux = []
            for f in range(rows + 1):
                p = 7.0 * (height[f + 1] + height[f + 2]) - (height[f] + height[f + 3])
                flux.append((speed[f] + speed[f + 1]) * face_cos[f] * p)
            for j in range(rows):
                div = (flux[j + 1] - flux[j]) * inverse_cos[j][:, :wide]
                out_ref[j, at, lanes] = part_ref[j, at, lanes] - div

    for j in range(rows):
        cut = jnp.full((8, LANES), cutoffs_ref[first + j].astype(jnp.float32))
        kept_ref[j] = jnp.where(flags_ref[first + j] > 0, jnp.minimum(1.0, cut * cut), 1.0)

    @pl.when(marked > 0)
    def _():
        for r in range(0, units, 16):
            j, q = divmod(r, levels)
            x = out_ref[j, q : q + 16, :]
            near = x[:, :depth]
            x = jnp.concatenate([x, jnp.zeros((16, full - nlon), jnp.float32)], axis=1)
            far = pltpu.roll(x, full - half, 1)[:, :depth]
            for parity, y in ((0, near + far), (1, near - far)):
                high = y.astype(jnp.bfloat16)
                y_ref[parity, r : r + 16, :] = high
                y_ref[parity, units + r : units + r + 16, :] = (y - high.astype(jnp.float32)).astype(jnp.bfloat16)
        lane = lax.broadcasted_iota(jnp.int32, (8, width), 1)
        chunk = 256 if cols % 256 == 0 and depth % 256 == 0 else LANES
        for parity in (0, 1):
            high_ref, low_ref = tables[4 * parity : 4 * parity + 2]
            waves = 2 * lane + parity
            weight = jnp.where((waves > 0) & (waves < half), 2.0 / nlon, 1.0 / nlon)
            inverse = 1.0 / jnp.maximum(waves, 1).astype(jnp.float32)
            factors = []
            for j in range(rows):
                ratio = cutoffs_ref[first + j].astype(jnp.float32) * inverse
                factor = (1.0 - jnp.minimum(1.0, ratio * ratio)) * weight
                factor = jnp.where(flags_ref[first + j] > 0, factor, 0.0)
                factors.append(jnp.concatenate([factor, factor], axis=1))
            for c in range(0, cols, chunk):
                spectrum = products(y_ref.at[parity], high_ref, low_ref, c, chunk, units)
                for r in range(0, units, 16):
                    f = factors[r // levels][:, c : c + chunk]
                    y = spectrum[r : r + 16] * jnp.concatenate([f, f], axis=0)
                    high = y.astype(jnp.bfloat16)
                    s_ref[parity, r : r + 16, c : c + chunk] = high
                    s_ref[parity, units + r : units + r + 16, c : c + chunk] = (
                        y - high.astype(jnp.float32)
                    ).astype(jnp.bfloat16)
        for c in range(0, depth, chunk):
            even = products(s_ref.at[0], tables[2], tables[3], c, chunk, units)
            uneven = products(s_ref.at[1], tables[6], tables[7], c, chunk, units)
            for r in range(0, units, 16):
                j, q = divmod(r, levels)
                x, y = even[r : r + 16], uneven[r : r + 16]
                out_ref[j, q : q + 16, c : c + chunk] -= x + y
                d_ref[r : r + 16, c : c + chunk] = x - y
        for r in range(0, units, 8):
            j, q = divmod(r, levels)
            d = jnp.concatenate([d_ref[r : r + 8, :], jnp.zeros((8, full - depth), jnp.float32)], axis=1)
            start = half // LANES * LANES
            out_ref[j, q : q + 8, start:] -= pltpu.roll(d, half, 1)[:, start:nlon]


def products(y_ref, high_ref, low_ref, c, chunk, units):
    both = jnp.dot(y_ref[...], high_ref[:, c : c + chunk], preferred_element_type=jnp.float32)
    third = jnp.dot(y_ref[:units, :], low_ref[:, c : c + chunk], preferred_element_type=jnp.float32)
    return both[:units] + both[units:] + third


def base_of(nlon):
    return nlon // LANES * LANES


def mean_kernel(area, sums_ref, kept_ref, part_ref, out_ref, row_ref, sem):
    rows = part_ref.shape[0]
    mean = sums_ref[:, :1] * (1.0 / area)
    copies = []
    for j in range(rows):
        row_ref[j] = part_ref[j] - mean * kept_ref[j, :1, :1]
        copies.append(pltpu.make_async_copy(row_ref.at[j], out_ref.at[j], sem.at[j]))
        copies[-1].start()
    for c in copies:
        c.wait()


def base_of(nlon):
    return nlon // LANES * LANES


def call(kernel, ins, outs, megabytes, scratch=(), out_space=pltpu.VMEM):
    return pl.pallas_call(
        kernel,
        in_specs=[pl.BlockSpec(memory_space=space) for _, space in ins],
        out_specs=[pl.BlockSpec(memory_space=out_space) for _ in outs],
        out_shape=[jax.ShapeDtypeStruct(shape, dtype) for shape, dtype in outs],
        scratch_shapes=list(scratch),
        compiler_params=pltpu.CompilerParams(vmem_limit_bytes=megabytes << 20),
    )(*[x for x, _ in ins])


def permute(x, pairs, axes="lat"):
    return lax.ppermute(x, axes, pairs)


def step(height, zonal_courant, merid_courant, rates, thresholds, flags, cutoffs):
    rows, levels, nlon = height.shape
    count = lax.axis_size("lat")
    nlat = rows * count
    half = nlon // 2
    smem, vmem, hbm = pltpu.SMEM, pltpu.VMEM, pltpu.HBM
    f32 = jnp.float32

    between = [(i, i + 1) for i in range(1, count - 1, 2)]
    within = [(i, i + 1) for i in range(0, count - 1, 2)]
    between = between + [(j, i) for i, j in between]
    parts = lax.axis_size("member")
    between = [(p * count + i, p * count + j) for p in range(parts) for i, j in between]
    ends = [0, count - 1] if count % 2 == 0 else [0]
    if parts % 2 == 0:
        between += [(p * count + e, (p ^ 1) * count + e) for p in range(parts) for e in ends]
    within = within + [(j, i) for i, j in within]
    whole, _, extra = dense_tiles(levels, nlon)
    (edge_b,) = call(
        pack_kernel,
        [
            (pltpu.with_memory_space_constraint(height, hbm), hbm),
            (pltpu.with_memory_space_constraint(merid_courant, hbm), hbm),
        ],
        [((3, 8 * (whole + extra), LANES), f32)],
        4,
        [pltpu.VMEM((3, levels, nlon), f32), pltpu.SemaphoreType.DMA((2,))],
    )
    b = permute(edge_b, between, ("member", "lat"))

    cos_row = jnp.asarray(np.sin(np.pi * (np.arange(nlat) + 0.5) / nlat).astype(np.float32))
    faces = np.sin(np.pi * np.arange(nlat + 1) / nlat)
    faces[0] = faces[nlat] = 0.0
    cos_face = jnp.asarray(faces.astype(np.float32))
    edge_a, sums, source = call(
        source_kernel,
        [(cos_row, smem), (rates[None], vmem), (thresholds[None], vmem), (height, vmem), (merid_courant, vmem)],
        [((3, levels, nlon), f32), ((levels, LANES), f32), (height.shape, f32)],
        8,
    )
    a = permute(edge_a, within)
    (part,) = call(zonal_kernel, [(height, vmem), (zonal_courant, vmem), (source, vmem)], [(height.shape, f32)], 8)
    depth = round_up(half, LANES)
    cols = 2 * round_up(half // 2 + 1, LANES)
    tables = []
    for parity in (0, 1):
        tables += call(
            functools.partial(table_kernel, parity, half),
            [(jnp.asarray(phases(nlon)[parity]), vmem)],
            [((depth, cols), jnp.bfloat16)] * 2 + [((cols, depth), jnp.bfloat16)] * 2,
            8,
        )

    bits = [1 << i for i in range((count - 1).bit_length())]
    if count == 1 << len(bits):
        for d in bits[:1] + bits[2:] + bits[1:2]:
            sums = sums + permute(sums, [(i, i ^ d) for i in range(count)])
    else:
        sums = lax.psum(sums, "lat")

    part, kept = call(
        finish_kernel,
        [(cos_row, smem), (cos_face, smem), (flags, smem), (cutoffs, smem)]
        + [(x, vmem) for x in (height, merid_courant, part, a, b, *tables)],
        [(height.shape, f32), ((rows, 8, LANES), f32)],
        24,
        [
            pltpu.VMEM((2, 2 * rows * levels, depth), jnp.bfloat16),
            pltpu.VMEM((2, 2 * rows * levels, cols), jnp.bfloat16),
            pltpu.VMEM((rows * levels, depth), f32),
        ],
    )
    area = nlon * float(np.sum(np.sin(np.pi * (np.arange(nlat) + 0.5) / nlat)))
    (out,) = call(
        functools.partial(mean_kernel, area),
        [(sums, vmem), (kept, vmem), (part, vmem)],
        [(height.shape, f32)],
        4,
        [pltpu.VMEM(height.shape, f32), pltpu.SemaphoreType.DMA((rows,))],
        hbm,
    )
    return out


def solution(mesh):
    split_rows = P(("member", "lat"), None, None)
    return jax.shard_map(
        step,
        mesh=mesh,
        in_specs=(split_rows, split_rows, split_rows, P("member"), P("member"), P(), P()),
        out_specs=split_rows,
        check_vma=False,
    )
```

```python
import functools

import jax
import jax.numpy as jnp
import numpy as np
from jax import lax
from jax.experimental import pallas as pl
from jax.experimental.pallas import tpu as pltpu
from jax.sharding import PartitionSpec as P

LANES = 128


def round_up(value, step):
    return -(-value // step) * step


@functools.cache
def phases(nlon):
    half = nlon // 2
    width = round_up(half // 2 + 1, LANES)
    depth = round_up(half, LANES)
    points = np.arange(depth)
    arrays = []
    for parity in (0, 1):
        waves = 2 * np.arange(width) + parity
        lanes = (waves <= half)[None, :]

        def both(steps, valid, axis):
            angle = 2.0 * np.pi / nlon * (steps % nlon)
            return np.concatenate([np.cos(angle) * valid, np.sin(angle) * valid], axis=axis)

        blocks = [
            both(points[::8, None] * waves[None, :], lanes & (points[::8, None] < half), 1),
            both(points[:8, None] * waves[None, :], True, 1),
            both(16 * np.arange(width // 8)[:, None] * points[None, :], (points < half)[None, :], 0),
            both(waves[:8, None] * points[None, :], True, 0),
        ]
        columns = max(x.shape[1] for x in blocks)
        arrays.append(
            np.concatenate([np.pad(x, ((0, 0), (0, columns - x.shape[1]))) for x in blocks]).astype(np.float32)
        )
    return arrays


def softplus(s):
    return jnp.maximum(s, 0.0) + jnp.log(1.0 + jnp.exp(-jnp.abs(s)))


def wrapped(row, nlon, full):
    base = nlon // LANES * LANES
    rest = nlon - base
    body, tail = row[:, :base], row[:, base:]
    tail = jnp.concatenate([tail, jnp.zeros((row.shape[0], full - nlon), row.dtype)], axis=1)
    lane = lax.broadcasted_iota(jnp.int32, tail.shape, 1)
    head = pltpu.roll(row[:, : full - base], rest, 1)
    end = pltpu.roll(tail, full - base - rest, 1)
    tail = jnp.where(lane < rest, tail, jnp.where(lane < full - base - 8, head, end))
    return jnp.concatenate([body, tail], axis=1)


def column(row):
    count = row.shape[1]
    same = lax.broadcasted_iota(jnp.int32, (count, count), 0) == lax.broadcasted_iota(
        jnp.int32, (count, count), 1
    )
    return jnp.sum(jnp.where(same, row, 0.0), axis=1, keepdims=True)


def dense_tiles(levels, nlon):
    rest = nlon % LANES
    shared = LANES // rest if rest else 1
    whole = levels // 8 * (nlon // LANES)
    return whole, shared, (-(-(levels // 8) // shared) if rest else 0)


def pack_row(row, out_ref, i):
    levels, nlon = row.shape
    whole, shared, extra = dense_tiles(levels, nlon)
    per = nlon // LANES
    rest = nlon % LANES
    for t in range(whole):
        g, k = divmod(t, per)
        out_ref[i, 8 * t : 8 * t + 8, :] = row[8 * g : 8 * g + 8, k * LANES : (k + 1) * LANES]
    for e in range(extra):
        parts = [
            row[8 * g : 8 * g + 8, per * LANES :]
            for g in range(e * shared, min((e + 1) * shared, levels // 8))
        ]
        parts.append(jnp.zeros((8, LANES - rest * len(parts)), row.dtype))
        t = whole + e
        out_ref[i, 8 * t : 8 * t + 8, :] = jnp.concatenate([p for p in parts if p.shape[1]], axis=1)


def packed_tile(ref, i, g, k, levels, nlon):
    whole, shared, _ = dense_tiles(levels, nlon)
    per = nlon // LANES
    rest = nlon % LANES
    if k < per:
        t = g * per + k
        return ref[i, 8 * t : 8 * t + 8, :]
    t = whole + g // shared
    last = ref[i, 8 * t : 8 * t + 8, :]
    at = g % shared * rest
    return (pltpu.roll(last, LANES - at, 1) if at else last)[:, :rest]


def pack_kernel(h_ref, v_ref, out_ref, edge_ref, sem):
    rows = h_ref.shape[0]
    odd = lax.axis_index("lat") % 2 == 1
    two = jnp.where(odd, rows - 2, 0)
    one = jnp.where(odd, rows - 1, 0)
    copies = [
        pltpu.make_async_copy(h_ref.at[pl.ds(two, 2)], edge_ref.at[pl.ds(0, 2)], sem.at[0]),
        pltpu.make_async_copy(v_ref.at[pl.ds(one, 1)], edge_ref.at[pl.ds(2, 1)], sem.at[1]),
    ]
    for c in copies:
        c.start()
    for c in copies:
        c.wait()
    for i in range(3):
        pack_row(edge_ref[i], out_ref, i)


def source_kernel(cos_ref, rates_ref, thresholds_ref, h_ref, v_ref, edge_ref, sum_ref, out_ref):
    rows, levels, nlon = h_ref.shape
    full = round_up(nlon, LANES)
    base = base_of(nlon)
    position = lax.axis_index("lat")
    first = position * rows
    rates = column(rates_ref[...])
    thresholds = column(thresholds_ref[...])
    total = jnp.zeros((levels, LANES), jnp.float32)
    for j in range(rows):
        s = softplus(h_ref[j] - thresholds) * -rates
        out_ref[j] = s
        acc = s[:, 0:LANES]
        for t in range(1, nlon // LANES):
            acc = acc + s[:, t * LANES : (t + 1) * LANES]
        if base < nlon:
            acc = acc + jnp.concatenate(
                [s[:, base:], jnp.zeros((levels, full - nlon), jnp.float32)], axis=1
            )
        total = total + acc * cos_ref[first + j]
    total = jnp.broadcast_to(jnp.sum(total, axis=1, keepdims=True), (levels, LANES))
    sum_ref[...] = total
    even = position % 2 == 0
    two = jnp.where(even, rows - 2, 0)
    one = jnp.where(even, rows - 1, 0)
    edge_ref[0] = h_ref[two]
    edge_ref[1] = h_ref[two + 1]
    edge_ref[2] = v_ref[one]


def zonal_kernel(h_ref, u_ref, s_ref, out_ref):
    rows, _, nlon = h_ref.shape
    full = round_up(nlon, LANES)
    for j in range(rows):
        h0 = h_ref[j]
        h = wrapped(h0, nlon, full)
        u = wrapped(u_ref[j], nlon, full)
        east = pltpu.roll(h, full - 1, 1)
        far_east = pltpu.roll(h, full - 2, 1)
        west = pltpu.roll(h, 1, 1)
        face = (7.0 * (h + east) - (west + far_east)) * (0.5 / 12.0)
        flux = (u + pltpu.roll(u, full - 1, 1)) * face
        div = flux - pltpu.roll(flux, 1, 1)
        out_ref[j] = h0 - div[:, :nlon] + s_ref[j]


def table_kernel(parity, half, source_ref, high_ref, low_ref, high_t_ref, low_t_ref):
    depth, cols = high_ref.shape
    width = cols // 2

    def put(high, low, at, cols, values):
        h = values.astype(jnp.bfloat16)
        high[at, cols] = h
        low[at, cols] = (values - h.astype(jnp.float32)).astype(jnp.bfloat16)

    def fill(coarse_cos, coarse_sin, fine_cos, fine_sin, count, store):
        for k in range(0, count, 2):
            pieces = []
            for q in (k, k + 1):
                cc, cs = coarse_cos(q), coarse_sin(q)
                pieces.append((cc * fine_cos - cs * fine_sin, cs * fine_cos + cc * fine_sin))
            store(k, *[jnp.concatenate(p, axis=0) for p in zip(*pieces)])

    def store(k, c, s):
        at = slice(8 * k, 8 * k + 16)
        put(high_ref, low_ref, at, slice(0, width), c)
        put(high_ref, low_ref, at, slice(width, cols), s)

    def store_t(k, c, s):
        if 2 * (8 * k + 15) + parity > half:
            waves = 2 * (8 * k + lax.broadcasted_iota(jnp.int32, c.shape, 0)) + parity
            c, s = jnp.where(waves <= half, c, 0.0), jnp.where(waves <= half, s, 0.0)
        put(high_t_ref, low_t_ref, slice(8 * k, 8 * k + 16), slice(None), c)
        put(high_t_ref, low_t_ref, slice(width + 8 * k, width + 8 * k + 16), slice(None), s)

    fine = depth // 8
    turned = fine + 8
    fine_t = turned + 2 * (width // 8)
    fill(
        lambda q: source_ref[q : q + 1, :width],
        lambda q: source_ref[q : q + 1, width:cols],
        source_ref[fine : fine + 8, :width],
        source_ref[fine : fine + 8, width:cols],
        depth // 8,
        store,
    )
    fill(
        lambda q: source_ref[turned + q : turned + q + 1, :depth],
        lambda q: source_ref[turned + width // 8 + q : turned + width // 8 + q + 1, :depth],
        source_ref[fine_t : fine_t + 8, :depth],
        source_ref[fine_t + 8 : fine_t + 16, :depth],
        width // 8,
        store_t,
    )


def finish_kernel(
    cos_row_ref,
    cos_face_ref,
    flags_ref,
    cutoffs_ref,
    sums_ref,
    h_ref,
    v_ref,
    part_ref,
    a_ref,
    b_ref,
    *rest,
):
    tables, (result_ref, out_ref, y_ref, s_ref, d_ref, sem) = rest[:8], rest[8:]
    rows, levels, nlon = h_ref.shape
    full = round_up(nlon, LANES)
    half = nlon // 2
    depth, cols = tables[0].shape
    width = cols // 2
    units = rows * levels
    position = lax.axis_index("lat")
    last = lax.axis_size("lat") - 1
    first = position * rows
    odd = position % 2 == 1
    bottom, top = position == 0, position == last
    marked = flags_ref[first]
    for j in range(1, rows):
        marked = jnp.maximum(marked, flags_ref[first + j])
    inverse_cos = [1.0 / jnp.full((8, LANES), cos_row_ref[first + j]) for j in range(rows)]
    face_cos = [cos_face_ref[first + f] * (0.5 / 12.0) for f in range(rows + 1)]

    nlat = cos_row_ref.shape[0]
    area = nlon * float(np.sum(np.sin(np.pi * (np.arange(nlat) + 0.5) / nlat)))
    mean = sums_ref[:, :LANES] * (1.0 / area)
    groups = levels // 8
    sends = [
        pltpu.make_async_copy(
            out_ref.at[:, pl.ds(8 * g, 8), :], result_ref.at[:, pl.ds(8 * g, 8), :], sem.at[g]
        )
        for g in range(groups)
    ]

    def update(g, shift):
        at = slice(8 * g, 8 * g + 8)
        for k in range(full // LANES):
            lanes = slice(k * LANES, min((k + 1) * LANES, nlon))
            wide = lanes.stop - lanes.start
            near = [a_ref[i, at, lanes] for i in range(3)]
            far = [packed_tile(b_ref, i, g, k, levels, nlon) for i in range(3)]
            below = [jnp.where(odd, x, jnp.where(bottom, 0.0, y)) for x, y in zip(near, far)]
            above = [jnp.where(odd, jnp.where(top, 0.0, y), x) for x, y in zip(near, far)]
            height = [below[0], below[1], *(h_ref[j, at, lanes] for j in range(rows)), above[0], above[1]]
            speed = [below[2], *(v_ref[j, at, lanes] for j in range(rows)), above[2]]
            flux = []
            for f in range(rows + 1):
                p = 7.0 * (height[f + 1] + height[f + 2]) - (height[f] + height[f + 3])
                flux.append((speed[f] + speed[f + 1]) * face_cos[f] * p)
            for j in range(rows):
                div = (flux[j + 1] - flux[j]) * inverse_cos[j][:, :wide]
                new = part_ref[j, at, lanes] - div
                out_ref[j, at, lanes] = new - mean[at, :wide] if shift else new

    @pl.when(marked == 0)
    def _():
        for g in range(groups):
            update(g, True)
            sends[g].start()

    @pl.when(marked > 0)
    def _():
        for g in range(groups):
            update(g, False)
        for r in range(0, units, 16):
            j, q = divmod(r, levels)
            x = out_ref[j, q : q + 16, :]
            near = x[:, :depth]
            x = jnp.concatenate([x, jnp.zeros((16, full - nlon), jnp.float32)], axis=1)
            far = pltpu.roll(x, full - half, 1)[:, :depth]
            for parity, y in ((0, near + far), (1, near - far)):
                high = y.astype(jnp.bfloat16)
                y_ref[parity, r : r + 16, :] = high
                y_ref[parity, units + r : units + r + 16, :] = (y - high.astype(jnp.float32)).astype(jnp.bfloat16)
        lane = lax.broadcasted_iota(jnp.int32, (8, width), 1)
        chunk = 256 if cols % 256 == 0 and depth % 256 == 0 else LANES
        for parity in (0, 1):
            high_ref, low_ref = tables[4 * parity : 4 * parity + 2]
            waves = 2 * lane + parity
            weight = jnp.where((waves > 0) & (waves < half), 2.0 / nlon, 1.0 / nlon)
            inverse = 1.0 / jnp.maximum(waves, 1).astype(jnp.float32)
            factors = []
            for j in range(rows):
                ratio = cutoffs_ref[first + j].astype(jnp.float32) * inverse
                factor = (1.0 - jnp.minimum(1.0, ratio * ratio)) * weight
                factor = jnp.where(flags_ref[first + j] > 0, factor, 0.0)
                factors.append(jnp.concatenate([factor, factor], axis=1))
            for c in range(0, cols, chunk):
                spectrum = products(y_ref.at[parity], high_ref, low_ref, c, chunk, units)
                for r in range(0, units, 16):
                    f = factors[r // levels][:, c : c + chunk]
                    y = spectrum[r : r + 16] * jnp.concatenate([f, f], axis=0)
                    high = y.astype(jnp.bfloat16)
                    s_ref[parity, r : r + 16, c : c + chunk] = high
                    s_ref[parity, units + r : units + r + 16, c : c + chunk] = (
                        y - high.astype(jnp.float32)
                    ).astype(jnp.bfloat16)
        for c in range(0, depth, chunk):
            even = products(s_ref.at[0], tables[2], tables[3], c, chunk, units)
            uneven = products(s_ref.at[1], tables[6], tables[7], c, chunk, units)
            for r in range(0, units, 16):
                j, q = divmod(r, levels)
                x, y = even[r : r + 16], uneven[r : r + 16]
                out_ref[j, q : q + 16, c : c + chunk] -= x + y
                d_ref[r : r + 16, c : c + chunk] = x - y
        kept = []
        for j in range(rows):
            cut = jnp.full((8, LANES), cutoffs_ref[first + j].astype(jnp.float32))
            kept.append(jnp.where(flags_ref[first + j] > 0, jnp.minimum(1.0, cut * cut), 1.0))
        start = half // LANES * LANES
        for g in range(groups):
            at = slice(8 * g, 8 * g + 8)
            for j in range(rows):
                r = j * levels + 8 * g
                d = jnp.concatenate([d_ref[r : r + 8, :], jnp.zeros((8, full - depth), jnp.float32)], axis=1)
                d = pltpu.roll(d, half, 1)
                shift = mean[at] * kept[j]
                for k in range(full // LANES):
                    lanes = slice(k * LANES, min((k + 1) * LANES, nlon))
                    less = shift[:, : lanes.stop - lanes.start]
                    if lanes.start >= start:
                        less = less + d[:, lanes]
                    out_ref[j, at, lanes] -= less
            sends[g].start()

    for send in sends:
        send.wait()


def products(y_ref, high_ref, low_ref, c, chunk, units):
    both = jnp.dot(y_ref[...], high_ref[:, c : c + chunk], preferred_element_type=jnp.float32)
    third = jnp.dot(y_ref[:units, :], low_ref[:, c : c + chunk], preferred_element_type=jnp.float32)
    return both[:units] + both[units:] + third


def base_of(nlon):
    return nlon // LANES * LANES


def call(kernel, ins, outs, megabytes, scratch=(), out_space=pltpu.VMEM):
    return pl.pallas_call(
        kernel,
        in_specs=[pl.BlockSpec(memory_space=space) for _, space in ins],
        out_specs=[pl.BlockSpec(memory_space=out_space) for _ in outs],
        out_shape=[jax.ShapeDtypeStruct(shape, dtype) for shape, dtype in outs],
        scratch_shapes=list(scratch),
        compiler_params=pltpu.CompilerParams(vmem_limit_bytes=megabytes << 20),
    )(*[x for x, _ in ins])


def permute(x, pairs, axes="lat"):
    return lax.ppermute(x, axes, pairs)


def step(height, zonal_courant, merid_courant, rates, thresholds, flags, cutoffs):
    rows, levels, nlon = height.shape
    count = lax.axis_size("lat")
    nlat = rows * count
    half = nlon // 2
    smem, vmem, hbm = pltpu.SMEM, pltpu.VMEM, pltpu.HBM
    f32 = jnp.float32

    between = [(i, i + 1) for i in range(1, count - 1, 2)]
    within = [(i, i + 1) for i in range(0, count - 1, 2)]
    between = between + [(j, i) for i, j in between]
    parts = lax.axis_size("member")
    between = [(p * count + i, p * count + j) for p in range(parts) for i, j in between]
    ends = [0, count - 1] if count % 2 == 0 else [0]
    if parts % 2 == 0:
        between += [(p * count + e, (p ^ 1) * count + e) for p in range(parts) for e in ends]
    within = within + [(j, i) for i, j in within]
    whole, _, extra = dense_tiles(levels, nlon)
    (edge_b,) = call(
        pack_kernel,
        [
            (pltpu.with_memory_space_constraint(height, hbm), hbm),
            (pltpu.with_memory_space_constraint(merid_courant, hbm), hbm),
        ],
        [((3, 8 * (whole + extra), LANES), f32)],
        4,
        [pltpu.VMEM((3, levels, nlon), f32), pltpu.SemaphoreType.DMA((2,))],
    )
    b = permute(edge_b, between, ("member", "lat"))

    cos_row = jnp.asarray(np.sin(np.pi * (np.arange(nlat) + 0.5) / nlat).astype(np.float32))
    faces = np.sin(np.pi * np.arange(nlat + 1) / nlat)
    faces[0] = faces[nlat] = 0.0
    cos_face = jnp.asarray(faces.astype(np.float32))
    edge_a, sums, source = call(
        source_kernel,
        [(cos_row, smem), (rates[None], vmem), (thresholds[None], vmem), (height, vmem), (merid_courant, vmem)],
        [((3, levels, nlon), f32), ((levels, LANES), f32), (height.shape, f32)],
        8,
    )
    a = permute(edge_a, within)
    (part,) = call(zonal_kernel, [(height, vmem), (zonal_courant, vmem), (source, vmem)], [(height.shape, f32)], 8)
    depth = round_up(half, LANES)
    cols = 2 * round_up(half // 2 + 1, LANES)
    tables = []
    for parity in (0, 1):
        tables += call(
            functools.partial(table_kernel, parity, half),
            [(jnp.asarray(phases(nlon)[parity]), vmem)],
            [((depth, cols), jnp.bfloat16)] * 2 + [((cols, depth), jnp.bfloat16)] * 2,
            8,
        )

    bits = [1 << i for i in range((count - 1).bit_length())]
    if count == 1 << len(bits):
        far = bits[2:]
        rounds = [bits[:1], *([*far[i : i + 2], sum(far[i : i + 2])] for i in range(0, len(far), 2)), bits[1:2]]
        for masks in rounds:
            sums = sums + sum(permute(sums, [(p, p ^ mask) for p in range(count)]) for mask in dict.fromkeys(masks))
    else:
        sums = lax.psum(sums, "lat")

    (out,) = call(
        finish_kernel,
        [(cos_row, smem), (cos_face, smem), (flags, smem), (cutoffs, smem)]
        + [(x, vmem) for x in (sums, height, merid_courant, part, a, b, *tables)],
        [(height.shape, f32)],
        24,
        [
            pltpu.VMEM(height.shape, f32),
            pltpu.VMEM((2, 2 * rows * levels, depth), jnp.bfloat16),
            pltpu.VMEM((2, 2 * rows * levels, cols), jnp.bfloat16),
            pltpu.VMEM((rows * levels, depth), f32),
            pltpu.SemaphoreType.DMA((levels // 8,)),
        ],
        hbm,
    )
    return out


def solution(mesh):
    split_rows = P(("member", "lat"), None, None)
    return jax.shard_map(
        step,
        mesh=mesh,
        in_specs=(split_rows, split_rows, split_rows, P("member"), P("member"), P(), P()),
        out_specs=split_rows,
        check_vma=False,
    )
```

```python
import functools

import jax
import jax.numpy as jnp
import numpy as np
from jax import lax
from jax.experimental import pallas as pl
from jax.experimental.pallas import tpu as pltpu
from jax.sharding import PartitionSpec as P

LANES = 128


def round_up(value, step):
    return -(-value // step) * step


@functools.cache
def phases(nlon):
    half = nlon // 2
    width = round_up(half // 2 + 1, LANES)
    depth = round_up(half, LANES)
    points = np.arange(depth)
    arrays = []
    for parity in (0, 1):
        waves = 2 * np.arange(width) + parity
        lanes = (waves <= half)[None, :]

        def both(steps, valid, axis):
            angle = 2.0 * np.pi / nlon * (steps % nlon)
            return np.concatenate([np.cos(angle) * valid, np.sin(angle) * valid], axis=axis)

        blocks = [
            both(points[::8, None] * waves[None, :], lanes & (points[::8, None] < half), 1),
            both(points[:8, None] * waves[None, :], True, 1),
            both(16 * np.arange(width // 8)[:, None] * points[None, :], (points < half)[None, :], 0),
            both(waves[:8, None] * points[None, :], True, 0),
        ]
        columns = max(x.shape[1] for x in blocks)
        arrays.append(
            np.concatenate([np.pad(x, ((0, 0), (0, columns - x.shape[1]))) for x in blocks]).astype(np.float32)
        )
    return arrays


def softplus(s):
    return jnp.maximum(s, 0.0) + jnp.log(1.0 + jnp.exp(-jnp.abs(s)))


def wrapped(row, nlon, full):
    base = nlon // LANES * LANES
    rest = nlon - base
    body, tail = row[:, :base], row[:, base:]
    tail = jnp.concatenate([tail, jnp.zeros((row.shape[0], full - nlon), row.dtype)], axis=1)
    lane = lax.broadcasted_iota(jnp.int32, tail.shape, 1)
    head = pltpu.roll(row[:, : full - base], rest, 1)
    end = pltpu.roll(tail, full - base - rest, 1)
    tail = jnp.where(lane < rest, tail, jnp.where(lane < full - base - 8, head, end))
    return jnp.concatenate([body, tail], axis=1)


def column(row):
    count = row.shape[1]
    same = lax.broadcasted_iota(jnp.int32, (count, count), 0) == lax.broadcasted_iota(
        jnp.int32, (count, count), 1
    )
    return jnp.sum(jnp.where(same, row, 0.0), axis=1, keepdims=True)


def dense_tiles(levels, nlon):
    rest = nlon % LANES
    shared = LANES // rest if rest else 1
    whole = levels // 8 * (nlon // LANES)
    return whole, shared, (-(-(levels // 8) // shared) if rest else 0)


def pack_row(row, out_ref, i):
    levels, nlon = row.shape
    whole, shared, extra = dense_tiles(levels, nlon)
    per = nlon // LANES
    rest = nlon % LANES
    for t in range(whole):
        g, k = divmod(t, per)
        out_ref[i, 8 * t : 8 * t + 8, :] = row[8 * g : 8 * g + 8, k * LANES : (k + 1) * LANES]
    for e in range(extra):
        parts = [
            row[8 * g : 8 * g + 8, per * LANES :]
            for g in range(e * shared, min((e + 1) * shared, levels // 8))
        ]
        parts.append(jnp.zeros((8, LANES - rest * len(parts)), row.dtype))
        t = whole + e
        out_ref[i, 8 * t : 8 * t + 8, :] = jnp.concatenate([p for p in parts if p.shape[1]], axis=1)


def packed_tile(ref, i, g, k, levels, nlon):
    whole, shared, _ = dense_tiles(levels, nlon)
    per = nlon // LANES
    rest = nlon % LANES
    if k < per:
        t = g * per + k
        return ref[i, 8 * t : 8 * t + 8, :]
    t = whole + g // shared
    last = ref[i, 8 * t : 8 * t + 8, :]
    at = g % shared * rest
    return (pltpu.roll(last, LANES - at, 1) if at else last)[:, :rest]


def pack_kernel(h_ref, v_ref, out_ref, edge_ref, sem):
    rows = h_ref.shape[0]
    odd = lax.axis_index("lat") % 2 == 1
    two = jnp.where(odd, rows - 2, 0)
    one = jnp.where(odd, rows - 1, 0)
    copies = [
        pltpu.make_async_copy(h_ref.at[pl.ds(two, 2)], edge_ref.at[pl.ds(0, 2)], sem.at[0]),
        pltpu.make_async_copy(v_ref.at[pl.ds(one, 1)], edge_ref.at[pl.ds(2, 1)], sem.at[1]),
    ]
    for c in copies:
        c.start()
    for c in copies:
        c.wait()
    for i in range(3):
        pack_row(edge_ref[i], out_ref, i)


def source_kernel(cos_ref, rates_ref, thresholds_ref, h_ref, v_ref, edge_ref, sum_ref, out_ref):
    rows, levels, nlon = h_ref.shape
    full = round_up(nlon, LANES)
    base = base_of(nlon)
    position = lax.axis_index("lat")
    first = position * rows
    rates = column(rates_ref[...])
    thresholds = column(thresholds_ref[...])
    total = jnp.zeros((levels, LANES), jnp.float32)
    for j in range(rows):
        s = softplus(h_ref[j] - thresholds) * -rates
        out_ref[j] = s
        acc = s[:, 0:LANES]
        for t in range(1, nlon // LANES):
            acc = acc + s[:, t * LANES : (t + 1) * LANES]
        if base < nlon:
            acc = acc + jnp.concatenate(
                [s[:, base:], jnp.zeros((levels, full - nlon), jnp.float32)], axis=1
            )
        total = total + acc * cos_ref[first + j]
    total = jnp.broadcast_to(jnp.sum(total, axis=1, keepdims=True), (levels, LANES))
    sum_ref[...] = total
    even = position % 2 == 0
    two = jnp.where(even, rows - 2, 0)
    one = jnp.where(even, rows - 1, 0)
    edge_ref[0] = h_ref[two]
    edge_ref[1] = h_ref[two + 1]
    edge_ref[2] = v_ref[one]


def zonal_kernel(h_ref, u_ref, s_ref, out_ref):
    rows, _, nlon = h_ref.shape
    full = round_up(nlon, LANES)
    for j in range(rows):
        h0 = h_ref[j]
        h = wrapped(h0, nlon, full)
        u = wrapped(u_ref[j], nlon, full)
        east = pltpu.roll(h, full - 1, 1)
        far_east = pltpu.roll(h, full - 2, 1)
        west = pltpu.roll(h, 1, 1)
        face = (7.0 * (h + east) - (west + far_east)) * (0.5 / 12.0)
        flux = (u + pltpu.roll(u, full - 1, 1)) * face
        div = flux - pltpu.roll(flux, 1, 1)
        out_ref[j] = h0 - div[:, :nlon] + s_ref[j]


def table_kernel(parity, half, source_ref, high_ref, low_ref, high_t_ref, low_t_ref):
    depth, cols = high_ref.shape
    width = cols // 2

    def put(high, low, at, cols, values):
        h = values.astype(jnp.bfloat16)
        high[at, cols] = h
        low[at, cols] = (values - h.astype(jnp.float32)).astype(jnp.bfloat16)

    def fill(coarse_cos, coarse_sin, fine_cos, fine_sin, count, store):
        for k in range(0, count, 2):
            pieces = []
            for q in (k, k + 1):
                cc, cs = coarse_cos(q), coarse_sin(q)
                pieces.append((cc * fine_cos - cs * fine_sin, cs * fine_cos + cc * fine_sin))
            store(k, *[jnp.concatenate(p, axis=0) for p in zip(*pieces)])

    def store(k, c, s):
        at = slice(8 * k, 8 * k + 16)
        put(high_ref, low_ref, at, slice(0, width), c)
        put(high_ref, low_ref, at, slice(width, cols), s)

    def store_t(k, c, s):
        if 2 * (8 * k + 15) + parity > half:
            waves = 2 * (8 * k + lax.broadcasted_iota(jnp.int32, c.shape, 0)) + parity
            c, s = jnp.where(waves <= half, c, 0.0), jnp.where(waves <= half, s, 0.0)
        put(high_t_ref, low_t_ref, slice(8 * k, 8 * k + 16), slice(None), c)
        put(high_t_ref, low_t_ref, slice(width + 8 * k, width + 8 * k + 16), slice(None), s)

    fine = depth // 8
    turned = fine + 8
    fine_t = turned + 2 * (width // 8)
    fill(
        lambda q: source_ref[q : q + 1, :width],
        lambda q: source_ref[q : q + 1, width:cols],
        source_ref[fine : fine + 8, :width],
        source_ref[fine : fine + 8, width:cols],
        depth // 8,
        store,
    )
    fill(
        lambda q: source_ref[turned + q : turned + q + 1, :depth],
        lambda q: source_ref[turned + width // 8 + q : turned + width // 8 + q + 1, :depth],
        source_ref[fine_t : fine_t + 8, :depth],
        source_ref[fine_t + 8 : fine_t + 16, :depth],
        width // 8,
        store_t,
    )


def zoned(position, count):
    edge = -(-count // 4)
    return (position < edge) | (position >= count - edge)


def early(position, count):
    odd = position % 2 == 1
    upper = odd * (position + 1) + (1 - odd) * position
    both = zoned(upper - 1, count) | zoned(upper, count)
    return zoned(position, count) | (((upper & 3) == 0) & (both == False))


class Rows:
    def __init__(self, cos_row_ref, cos_face_ref, h_ref, v_ref, part_ref, a_ref):
        self.refs = h_ref, v_ref, part_ref, a_ref
        self.rows, self.levels, self.nlon = h_ref.shape
        self.full = round_up(self.nlon, LANES)
        self.position = lax.axis_index("lat")
        self.last = lax.axis_size("lat") - 1
        self.first = self.position * self.rows
        self.inverse_cos = [
            1.0 / jnp.full((8, LANES), cos_row_ref[self.first + j]) for j in range(self.rows)
        ]
        self.face_cos = [cos_face_ref[self.first + f] * (0.5 / 12.0) for f in range(self.rows + 1)]

    def tiles(self, g):
        for k in range(self.full // LANES):
            yield k, slice(8 * g, 8 * g + 8), slice(k * LANES, min((k + 1) * LANES, self.nlon))

    def update(self, g, far_tile, store):
        h_ref, v_ref, part_ref, a_ref = self.refs
        rows = self.rows
        odd = self.position % 2 == 1
        bottom, top = self.position == 0, self.position == self.last
        for k, at, lanes in self.tiles(g):
            wide = lanes.stop - lanes.start
            near = [a_ref[i, at, lanes] for i in range(3)]
            far = [far_tile(i, g, k) for i in range(3)]
            below = [jnp.where(odd, x, jnp.where(bottom, 0.0, y)) for x, y in zip(near, far)]
            above = [jnp.where(odd, jnp.where(top, 0.0, y), x) for x, y in zip(near, far)]
            height = [below[0], below[1], *(h_ref[j, at, lanes] for j in range(rows)), above[0], above[1]]
            speed = [below[2], *(v_ref[j, at, lanes] for j in range(rows)), above[2]]
            flux = []
            for f in range(rows + 1):
                p = 7.0 * (height[f + 1] + height[f + 2]) - (height[f] + height[f + 3])
                flux.append((speed[f] + speed[f + 1]) * self.face_cos[f] * p)
            for j in range(rows):
                div = (flux[j + 1] - flux[j]) * self.inverse_cos[j][:, :wide]
                store(j, at, lanes, part_ref[j, at, lanes] - div)


def any_marked(flags_ref, first, rows):
    marked = flags_ref[first]
    for j in range(1, rows):
        marked = jnp.maximum(marked, flags_ref[first + j])
    return marked


def filter_kernel(cos_row_ref, cos_face_ref, flags_ref, cutoffs_ref, h_ref, v_ref, part_ref, a_ref, b_ref, *rest):
    tables, (out_ref, y_ref, s_ref, d_ref) = rest[:8], rest[8:]
    rows, levels, nlon = h_ref.shape
    full = round_up(nlon, LANES)
    half = nlon // 2
    depth, cols = tables[0].shape
    width = cols // 2
    units = rows * levels
    first = lax.axis_index("lat") * rows

    def store(j, at, lanes, value):
        out_ref[j, at, lanes] = value

    @pl.when(any_marked(flags_ref, first, rows) > 0)
    def _():
        state = Rows(cos_row_ref, cos_face_ref, h_ref, v_ref, part_ref, a_ref)
        for g in range(levels // 8):
            state.update(g, lambda i, g, k: packed_tile(b_ref, i, g, k, levels, nlon), store)
        for r in range(0, units, 16):
            j, q = divmod(r, levels)
            x = out_ref[j, q : q + 16, :]
            near = x[:, :depth]
            x = jnp.concatenate([x, jnp.zeros((16, full - nlon), jnp.float32)], axis=1)
            far = pltpu.roll(x, full - half, 1)[:, :depth]
            for parity, y in ((0, near + far), (1, near - far)):
                high = y.astype(jnp.bfloat16)
                y_ref[parity, r : r + 16, :] = high
                y_ref[parity, units + r : units + r + 16, :] = (y - high.astype(jnp.float32)).astype(jnp.bfloat16)
        lane = lax.broadcasted_iota(jnp.int32, (8, width), 1)
        chunk = 256 if cols % 256 == 0 and depth % 256 == 0 else LANES
        for parity in (0, 1):
            high_ref, low_ref = tables[4 * parity : 4 * parity + 2]
            waves = 2 * lane + parity
            weight = jnp.where((waves > 0) & (waves < half), 2.0 / nlon, 1.0 / nlon)
            inverse = 1.0 / jnp.maximum(waves, 1).astype(jnp.float32)
            factors = []
            for j in range(rows):
                ratio = cutoffs_ref[first + j].astype(jnp.float32) * inverse
                factor = (1.0 - jnp.minimum(1.0, ratio * ratio)) * weight
                factor = jnp.where(flags_ref[first + j] > 0, factor, 0.0)
                factors.append(jnp.concatenate([factor, factor], axis=1))
            for c in range(0, cols, chunk):
                spectrum = products(y_ref.at[parity], high_ref, low_ref, c, chunk, units)
                for r in range(0, units, 16):
                    f = factors[r // levels][:, c : c + chunk]
                    y = spectrum[r : r + 16] * jnp.concatenate([f, f], axis=0)
                    high = y.astype(jnp.bfloat16)
                    s_ref[parity, r : r + 16, c : c + chunk] = high
                    s_ref[parity, units + r : units + r + 16, c : c + chunk] = (
                        y - high.astype(jnp.float32)
                    ).astype(jnp.bfloat16)
        for c in range(0, depth, chunk):
            even = products(s_ref.at[0], tables[2], tables[3], c, chunk, units)
            uneven = products(s_ref.at[1], tables[6], tables[7], c, chunk, units)
            for r in range(0, units, 16):
                j, q = divmod(r, levels)
                x, y = even[r : r + 16], uneven[r : r + 16]
                out_ref[j, q : q + 16, c : c + chunk] -= x + y
                d_ref[r : r + 16, c : c + chunk] = x - y
        start = half // LANES * LANES
        for r in range(0, units, 8):
            j, q = divmod(r, levels)
            d = jnp.concatenate([d_ref[r : r + 8, :], jnp.zeros((8, full - depth), jnp.float32)], axis=1)
            out_ref[j, q : q + 8, start:] -= pltpu.roll(d, half, 1)[:, start:nlon]


def finish_kernel(
    cos_row_ref,
    cos_face_ref,
    flags_ref,
    cutoffs_ref,
    sums_ref,
    h_ref,
    v_ref,
    part_ref,
    a_ref,
    b_ref,
    c_ref,
    filtered_ref,
    result_ref,
    out_ref,
    sem,
):
    rows, levels, nlon = h_ref.shape
    first = lax.axis_index("lat") * rows
    nlat = cos_row_ref.shape[0]
    area = nlon * float(np.sum(np.sin(np.pi * (np.arange(nlat) + 0.5) / nlat)))
    mean = sums_ref[:, :LANES] * (1.0 / area)
    groups = levels // 8
    sends = [
        pltpu.make_async_copy(
            out_ref.at[:, pl.ds(8 * g, 8), :], result_ref.at[:, pl.ds(8 * g, 8), :], sem.at[g]
        )
        for g in range(groups)
    ]
    marked = any_marked(flags_ref, first, rows)
    state = Rows(cos_row_ref, cos_face_ref, h_ref, v_ref, part_ref, a_ref)

    @pl.when(marked == 0)
    def _():
        soon = early(state.position, state.last + 1)

        def far_tile(i, g, k):
            x = packed_tile(b_ref, i, g, k, levels, nlon)
            return jnp.where(soon, x, packed_tile(c_ref, i, g, k, levels, nlon))

        def store(j, at, lanes, value):
            out_ref[j, at, lanes] = value - mean[at, : lanes.stop - lanes.start]

        for g in range(groups):
            state.update(g, far_tile, store)
            sends[g].start()

    @pl.when(marked > 0)
    def _():
        kept = []
        for j in range(rows):
            cut = jnp.full((8, LANES), cutoffs_ref[first + j].astype(jnp.float32))
            kept.append(jnp.where(flags_ref[first + j] > 0, jnp.minimum(1.0, cut * cut), 1.0))
        for g in range(groups):
            for k, at, lanes in state.tiles(g):
                for j in range(rows):
                    shift = (mean[at] * kept[j])[:, : lanes.stop - lanes.start]
                    out_ref[j, at, lanes] = filtered_ref[j, at, lanes] - shift
            sends[g].start()

    for send in sends:
        send.wait()


def products(y_ref, high_ref, low_ref, c, chunk, units):
    both = jnp.dot(y_ref[...], high_ref[:, c : c + chunk], preferred_element_type=jnp.float32)
    third = jnp.dot(y_ref[:units, :], low_ref[:, c : c + chunk], preferred_element_type=jnp.float32)
    return both[:units] + both[units:] + third


def base_of(nlon):
    return nlon // LANES * LANES


def call(kernel, ins, outs, megabytes, scratch=(), out_space=pltpu.VMEM):
    return pl.pallas_call(
        kernel,
        in_specs=[pl.BlockSpec(memory_space=space) for _, space in ins],
        out_specs=[pl.BlockSpec(memory_space=out_space) for _ in outs],
        out_shape=[jax.ShapeDtypeStruct(shape, dtype) for shape, dtype in outs],
        scratch_shapes=list(scratch),
        compiler_params=pltpu.CompilerParams(vmem_limit_bytes=megabytes << 20),
    )(*[x for x, _ in ins])


def permute(x, pairs, axes="lat"):
    return lax.ppermute(x, axes, pairs)


def exchanges(parts, count):
    flows = [(i, i + 1) for i in range(1, count - 1, 2)]
    flows += [(j, i) for i, j in flows]
    groups = []
    for first in (True, False):
        real = [(i, j) for i, j in flows if bool(early(j, count)) == first]
        senders = set(range(count)) - {i for i, _ in real}
        receivers = set(range(count)) - {j for _, j in real}
        pairs = [(p * count + i, p * count + j) for p in range(parts) for i, j in real]
        if parts % 2 == 0 and len(senders) == len(receivers):
            spare = senders & receivers
            local = {i for i in spare if i ^ 1 in spare}
            away = [(i, i) for i in sorted(spare - local)]
            away += zip(sorted(senders - spare), sorted(receivers - spare, reverse=True))
            for p in range(parts):
                pairs += [(p * count + i, p * count + (i ^ 1)) for i in sorted(local)]
                pairs += [(p * count + i, (p ^ 1) * count + j) for i, j in away]
        groups.append(pairs)
    return groups


def step(height, zonal_courant, merid_courant, rates, thresholds, flags, cutoffs):
    rows, levels, nlon = height.shape
    count = lax.axis_size("lat")
    nlat = rows * count
    half = nlon // 2
    smem, vmem, hbm = pltpu.SMEM, pltpu.VMEM, pltpu.HBM
    f32 = jnp.float32

    within = [(i, i + 1) for i in range(0, count - 1, 2)]
    within = within + [(j, i) for i, j in within]
    whole, _, extra = dense_tiles(levels, nlon)
    (edge_b,) = call(
        pack_kernel,
        [
            (pltpu.with_memory_space_constraint(height, hbm), hbm),
            (pltpu.with_memory_space_constraint(merid_courant, hbm), hbm),
        ],
        [((3, 8 * (whole + extra), LANES), f32)],
        4,
        [pltpu.VMEM((3, levels, nlon), f32), pltpu.SemaphoreType.DMA((2,))],
    )
    parts = lax.axis_size("member")
    b, c = (
        permute(edge_b, pairs, ("member", "lat"))
        for pairs in exchanges(parts, count)
    )

    cos_row = jnp.asarray(np.sin(np.pi * (np.arange(nlat) + 0.5) / nlat).astype(np.float32))
    faces = np.sin(np.pi * np.arange(nlat + 1) / nlat)
    faces[0] = faces[nlat] = 0.0
    cos_face = jnp.asarray(faces.astype(np.float32))
    edge_a, sums, source = call(
        source_kernel,
        [(cos_row, smem), (rates[None], vmem), (thresholds[None], vmem), (height, vmem), (merid_courant, vmem)],
        [((3, levels, nlon), f32), ((levels, LANES), f32), (height.shape, f32)],
        8,
    )
    a = permute(edge_a, within)
    (part,) = call(zonal_kernel, [(height, vmem), (zonal_courant, vmem), (source, vmem)], [(height.shape, f32)], 8)
    depth = round_up(half, LANES)
    cols = 2 * round_up(half // 2 + 1, LANES)
    tables = []
    for parity in (0, 1):
        tables += call(
            functools.partial(table_kernel, parity, half),
            [(jnp.asarray(phases(nlon)[parity]), vmem)],
            [((depth, cols), jnp.bfloat16)] * 2 + [((cols, depth), jnp.bfloat16)] * 2,
            8,
        )

    bits = [1 << i for i in range((count - 1).bit_length())]
    if count == 1 << len(bits):
        far = bits[2:]
        rounds = [bits[:1], *([*far[i : i + 2], sum(far[i : i + 2])] for i in range(0, len(far), 2)), bits[1:2]]
        for masks in rounds:
            sums = sums + sum(permute(sums, [(p, p ^ mask) for p in range(count)]) for mask in dict.fromkeys(masks))
    else:
        sums = lax.psum(sums, "lat")

    scalars = [(x, smem) for x in (cos_row, cos_face, flags, cutoffs)]
    rows_and_edges = [(x, vmem) for x in (height, merid_courant, part, a, b)]
    (filtered,) = call(
        filter_kernel,
        scalars + rows_and_edges + [(x, vmem) for x in tables],
        [(height.shape, f32)],
        24,
        [
            pltpu.VMEM((2, 2 * rows * levels, depth), jnp.bfloat16),
            pltpu.VMEM((2, 2 * rows * levels, cols), jnp.bfloat16),
            pltpu.VMEM((rows * levels, depth), f32),
        ],
    )
    (out,) = call(
        finish_kernel,
        [*scalars, (sums, vmem), *rows_and_edges, (c, vmem), (filtered, vmem)],
        [(height.shape, f32)],
        8,
        [pltpu.VMEM(height.shape, f32), pltpu.SemaphoreType.DMA((levels // 8,))],
        hbm,
    )
    return out


def solution(mesh):
    split_rows = P(("member", "lat"), None, None)
    return jax.shard_map(
        step,
        mesh=mesh,
        in_specs=(split_rows, split_rows, split_rows, P("member"), P("member"), P(), P()),
        out_specs=split_rows,
        check_vma=False,
    )
```

```python
import functools

import jax
import jax.numpy as jnp
import numpy as np
from jax import lax
from jax.experimental import pallas as pl
from jax.experimental.pallas import tpu as pltpu
from jax.sharding import PartitionSpec as P

LANES = 128


def round_up(value, step):
    return -(-value // step) * step


@functools.cache
def phases(nlon):
    half = nlon // 2
    width = round_up(half // 2 + 1, LANES)
    depth = round_up(half, LANES)
    points = np.arange(depth)
    arrays = []
    for parity in (0, 1):
        waves = 2 * np.arange(width) + parity
        lanes = (waves <= half)[None, :]

        def both(steps, valid, axis):
            angle = 2.0 * np.pi / nlon * (steps % nlon)
            return np.concatenate([np.cos(angle) * valid, np.sin(angle) * valid], axis=axis)

        blocks = [
            both(points[::8, None] * waves[None, :], lanes & (points[::8, None] < half), 1),
            both(points[:8, None] * waves[None, :], True, 1),
            both(16 * np.arange(width // 8)[:, None] * points[None, :], (points < half)[None, :], 0),
            both(waves[:8, None] * points[None, :], True, 0),
        ]
        columns = max(x.shape[1] for x in blocks)
        arrays.append(
            np.concatenate([np.pad(x, ((0, 0), (0, columns - x.shape[1]))) for x in blocks]).astype(np.float32)
        )
    return arrays


def softplus(s):
    return jnp.maximum(s, 0.0) + jnp.log(1.0 + jnp.exp(-jnp.abs(s)))


def wrapped(row, nlon, full):
    base = nlon // LANES * LANES
    rest = nlon - base
    body, tail = row[:, :base], row[:, base:]
    tail = jnp.concatenate([tail, jnp.zeros((row.shape[0], full - nlon), row.dtype)], axis=1)
    lane = lax.broadcasted_iota(jnp.int32, tail.shape, 1)
    head = pltpu.roll(row[:, : full - base], rest, 1)
    end = pltpu.roll(tail, full - base - rest, 1)
    tail = jnp.where(lane < rest, tail, jnp.where(lane < full - base - 8, head, end))
    return jnp.concatenate([body, tail], axis=1)


def column(row):
    count = row.shape[1]
    same = lax.broadcasted_iota(jnp.int32, (count, count), 0) == lax.broadcasted_iota(
        jnp.int32, (count, count), 1
    )
    return jnp.sum(jnp.where(same, row, 0.0), axis=1, keepdims=True)


def dense_tiles(levels, nlon):
    rest = nlon % LANES
    shared = LANES // rest if rest else 1
    whole = levels // 8 * (nlon // LANES)
    return whole, shared, (-(-(levels // 8) // shared) if rest else 0)


def pack_row(row, out_ref, i):
    levels, nlon = row.shape
    whole, shared, extra = dense_tiles(levels, nlon)
    per = nlon // LANES
    rest = nlon % LANES
    for t in range(whole):
        g, k = divmod(t, per)
        out_ref[i, 8 * t : 8 * t + 8, :] = row[8 * g : 8 * g + 8, k * LANES : (k + 1) * LANES]
    for e in range(extra):
        parts = [
            row[8 * g : 8 * g + 8, per * LANES :]
            for g in range(e * shared, min((e + 1) * shared, levels // 8))
        ]
        parts.append(jnp.zeros((8, LANES - rest * len(parts)), row.dtype))
        t = whole + e
        out_ref[i, 8 * t : 8 * t + 8, :] = jnp.concatenate([p for p in parts if p.shape[1]], axis=1)


def packed_tile(ref, i, g, k, levels, nlon):
    whole, shared, _ = dense_tiles(levels, nlon)
    per = nlon // LANES
    rest = nlon % LANES
    if k < per:
        t = g * per + k
        return ref[i, 8 * t : 8 * t + 8, :]
    t = whole + g // shared
    last = ref[i, 8 * t : 8 * t + 8, :]
    at = g % shared * rest
    return (pltpu.roll(last, LANES - at, 1) if at else last)[:, :rest]


def edge_rows(upper, rows):
    return jnp.where(upper, rows - 2, 1), jnp.where(upper, rows - 1, 0)


def pack_kernel(h_ref, v_ref, out_ref, edge_ref, sem):
    far, near = edge_rows(lax.axis_index("lat") % 2 == 1, h_ref.shape[0])
    copies = [
        pltpu.make_async_copy(ref.at[row], edge_ref.at[i], sem.at[i])
        for i, (ref, row) in enumerate([(h_ref, far), (h_ref, near), (v_ref, near)])
    ]
    for c in copies:
        c.start()
    for c in copies:
        c.wait()
    for i in range(3):
        pack_row(edge_ref[i], out_ref, i)


def source_kernel(cos_ref, rates_ref, thresholds_ref, h_ref, v_ref, edge_ref, sum_ref, out_ref):
    rows, levels, nlon = h_ref.shape
    full = round_up(nlon, LANES)
    base = base_of(nlon)
    position = lax.axis_index("lat")
    first = position * rows
    rates = column(rates_ref[...])
    thresholds = column(thresholds_ref[...])
    total = jnp.zeros((levels, LANES), jnp.float32)
    for j in range(rows):
        s = softplus(h_ref[j] - thresholds) * -rates
        out_ref[j] = s
        acc = s[:, 0:LANES]
        for t in range(1, nlon // LANES):
            acc = acc + s[:, t * LANES : (t + 1) * LANES]
        if base < nlon:
            acc = acc + jnp.concatenate(
                [s[:, base:], jnp.zeros((levels, full - nlon), jnp.float32)], axis=1
            )
        total = total + acc * cos_ref[first + j]
    total = jnp.broadcast_to(jnp.sum(total, axis=1, keepdims=True), (levels, LANES))
    sum_ref[...] = total
    far, near = edge_rows(position % 2 == 0, rows)
    edge_ref[0] = h_ref[far]
    edge_ref[1] = h_ref[near]
    edge_ref[2] = v_ref[near]


def zonal_kernel(h_ref, u_ref, s_ref, out_ref):
    rows, _, nlon = h_ref.shape
    full = round_up(nlon, LANES)
    for j in range(rows):
        h0 = h_ref[j]
        h = wrapped(h0, nlon, full)
        u = wrapped(u_ref[j], nlon, full)
        east = pltpu.roll(h, full - 1, 1)
        far_east = pltpu.roll(h, full - 2, 1)
        west = pltpu.roll(h, 1, 1)
        face = (7.0 * (h + east) - (west + far_east)) * (0.5 / 12.0)
        flux = (u + pltpu.roll(u, full - 1, 1)) * face
        div = flux - pltpu.roll(flux, 1, 1)
        out_ref[j] = h0 - div[:, :nlon] + s_ref[j]


def table_kernel(parity, half, source_ref, high_ref, low_ref, high_t_ref, low_t_ref):
    depth, cols = high_ref.shape
    width = cols // 2

    def put(high, low, at, cols, values):
        h = values.astype(jnp.bfloat16)
        high[at, cols] = h
        low[at, cols] = (values - h.astype(jnp.float32)).astype(jnp.bfloat16)

    def fill(coarse_cos, coarse_sin, fine_cos, fine_sin, count, store):
        for k in range(0, count, 2):
            pieces = []
            for q in (k, k + 1):
                cc, cs = coarse_cos(q), coarse_sin(q)
                pieces.append((cc * fine_cos - cs * fine_sin, cs * fine_cos + cc * fine_sin))
            store(k, *[jnp.concatenate(p, axis=0) for p in zip(*pieces)])

    def store(k, c, s):
        at = slice(8 * k, 8 * k + 16)
        put(high_ref, low_ref, at, slice(0, width), c)
        put(high_ref, low_ref, at, slice(width, cols), s)

    def store_t(k, c, s):
        if 2 * (8 * k + 15) + parity > half:
            waves = 2 * (8 * k + lax.broadcasted_iota(jnp.int32, c.shape, 0)) + parity
            c, s = jnp.where(waves <= half, c, 0.0), jnp.where(waves <= half, s, 0.0)
        put(high_t_ref, low_t_ref, slice(8 * k, 8 * k + 16), slice(None), c)
        put(high_t_ref, low_t_ref, slice(width + 8 * k, width + 8 * k + 16), slice(None), s)

    fine = depth // 8
    turned = fine + 8
    fine_t = turned + 2 * (width // 8)
    fill(
        lambda q: source_ref[q : q + 1, :width],
        lambda q: source_ref[q : q + 1, width:cols],
        source_ref[fine : fine + 8, :width],
        source_ref[fine : fine + 8, width:cols],
        depth // 8,
        store,
    )
    fill(
        lambda q: source_ref[turned + q : turned + q + 1, :depth],
        lambda q: source_ref[turned + width // 8 + q : turned + width // 8 + q + 1, :depth],
        source_ref[fine_t : fine_t + 8, :depth],
        source_ref[fine_t + 8 : fine_t + 16, :depth],
        width // 8,
        store_t,
    )


class Side:
    def __init__(self, lower, scalars, arrays):
        self.cos_row_ref, self.cos_face_ref, self.flags_ref, self.cutoffs_ref = scalars
        self.h_ref, self.v_ref, self.part_ref = arrays
        self.rows, self.levels, self.nlon = self.h_ref.shape
        self.full = round_up(self.nlon, LANES)
        self.lower = lower
        position = lax.axis_index("lat")
        self.first = position * self.rows
        self.outermost = position == jnp.where(lower, 0, lax.axis_size("lat") - 1)

    def row(self, i):
        return jnp.where(self.lower, i, self.rows - 1 - i)

    def tiles(self, g):
        for k in range(self.full // LANES):
            yield k, slice(8 * g, 8 * g + 8), slice(k * LANES, min((k + 1) * LANES, self.nlon))

    def any_marked(self):
        marked = self.flags_ref[self.first]
        for j in range(1, self.rows):
            marked = jnp.maximum(marked, self.flags_ref[self.first + j])
        return marked > 0

    def kept(self, i):
        row = self.first + self.row(i)
        cut = jnp.full((8, LANES), self.cutoffs_ref[row].astype(jnp.float32))
        return jnp.where(self.flags_ref[row] > 0, jnp.minimum(1.0, cut * cut), 1.0)

    def update(self, count, halo_tile, out_ref):
        sign = jnp.where(self.lower, 1.0, -1.0)
        scale = [sign / jnp.full((8, LANES), self.cos_row_ref[self.first + self.row(i)]) for i in range(count)]
        face_cos = [
            self.cos_face_ref[self.first + jnp.where(self.lower, i, self.rows - i)] * (0.5 / 12.0)
            for i in range(count + 1)
        ]
        for g in range(self.levels // 8):
            for k, at, lanes in self.tiles(g):
                wide = lanes.stop - lanes.start
                far, near, beyond = (jnp.where(self.outermost, 0.0, halo_tile(i, g, k)) for i in range(3))
                height = [far, near, *(self.h_ref[self.row(i), at, lanes] for i in range(count + 2))]
                speed = [beyond, *(self.v_ref[self.row(i), at, lanes] for i in range(count + 1))]
                flux = []
                for f in range(count + 1):
                    p = 7.0 * (height[f + 1] + height[f + 2]) - (height[f] + height[f + 3])
                    flux.append((speed[f] + speed[f + 1]) * face_cos[f] * p)
                for i in range(count):
                    div = (flux[i + 1] - flux[i]) * scale[i][:, :wide]
                    out_ref[i, at, lanes] = self.part_ref[self.row(i), at, lanes] - div

    def filter(self, count, tables, y_ref, s_ref, d_ref, out_ref):
        levels, nlon, full = self.levels, self.nlon, self.full
        half = nlon // 2
        depth, cols = tables[0].shape
        width = cols // 2
        units = count * levels
        for r in range(0, units, 16):
            j, q = divmod(r, levels)
            x = out_ref[j, q : q + 16, :]
            near = x[:, :depth]
            x = jnp.concatenate([x, jnp.zeros((16, full - nlon), jnp.float32)], axis=1)
            far = pltpu.roll(x, full - half, 1)[:, :depth]
            for parity, y in ((0, near + far), (1, near - far)):
                put_parts(y_ref, parity, r, units, slice(None), y)
        lane = lax.broadcasted_iota(jnp.int32, (8, width), 1)
        chunk = 256 if cols % 256 == 0 and depth % 256 == 0 else LANES
        for parity in (0, 1):
            high_ref, low_ref = tables[4 * parity : 4 * parity + 2]
            waves = 2 * lane + parity
            weight = jnp.where((waves > 0) & (waves < half), 2.0 / nlon, 1.0 / nlon)
            inverse = 1.0 / jnp.maximum(waves, 1).astype(jnp.float32)
            factors = []
            for j in range(count):
                row = self.first + self.row(j)
                ratio = self.cutoffs_ref[row].astype(jnp.float32) * inverse
                factor = (1.0 - jnp.minimum(1.0, ratio * ratio)) * weight
                factor = jnp.where(self.flags_ref[row] > 0, factor, 0.0)
                factors.append(jnp.concatenate([factor, factor], axis=1))
            for c in range(0, cols, chunk):
                spectrum = products(y_ref.at[parity], high_ref, low_ref, c, chunk, units)
                for r in range(0, units, 16):
                    f = factors[r // levels][:, c : c + chunk]
                    y = spectrum[r : r + 16] * jnp.concatenate([f, f], axis=0)
                    put_parts(s_ref, parity, r, units, slice(c, c + chunk), y)
        for c in range(0, depth, chunk):
            even = products(s_ref.at[0], tables[2], tables[3], c, chunk, units)
            uneven = products(s_ref.at[1], tables[6], tables[7], c, chunk, units)
            for r in range(0, units, 16):
                j, q = divmod(r, levels)
                x, y = even[r : r + 16], uneven[r : r + 16]
                out_ref[j, q : q + 16, c : c + chunk] -= x + y
                d_ref[r : r + 16, c : c + chunk] = x - y


def put_parts(ref, parity, r, units, lanes, y):
    high = y.astype(jnp.bfloat16)
    ref[parity, r : r + 16, lanes] = high
    ref[parity, units + r : units + r + 16, lanes] = (y - high.astype(jnp.float32)).astype(jnp.bfloat16)


def near_kernel(*refs):
    scalars, arrays, a_ref, tables = refs[:4], refs[4:7], refs[7], refs[8:16]
    out_ref, y_ref, s_ref, d_ref = refs[16:]
    side = Side(lax.axis_index("lat") % 2 == 1, scalars, arrays)
    count = out_ref.shape[0]

    def halo_tile(i, g, k):
        return a_ref[i, 8 * g : 8 * g + 8, k * LANES : min((k + 1) * LANES, side.nlon)]

    side.update(count, halo_tile, out_ref)

    @pl.when(side.any_marked())
    def _():
        side.filter(count, tables, y_ref, s_ref, d_ref, out_ref)
        start = side.nlon // 2 // LANES * LANES
        for r in range(0, count * side.levels, 8):
            j, q = divmod(r, side.levels)
            out_ref[j, q : q + 8, start:] -= shifted(d_ref, r, side)[:, start:]


def shifted(d_ref, r, side):
    depth = d_ref.shape[1]
    d = jnp.concatenate([d_ref[r : r + 8, :], jnp.zeros((8, side.full - depth), jnp.float32)], axis=1)
    return pltpu.roll(d, side.nlon // 2, 1)[:, : side.nlon]


def finish_kernel(*refs):
    scalars, sums_ref, arrays, b_ref, done_ref, tables = refs[:4], refs[4], refs[5:8], refs[8], refs[9], refs[10:18]
    result_ref, out_ref, y_ref, s_ref, d_ref, sem = refs[18:]
    odd = lax.axis_index("lat") % 2 == 1
    side, other = Side(odd == False, scalars, arrays), Side(odd, scalars, arrays)
    levels, nlon = side.levels, side.nlon
    done = done_ref.shape[0]
    count = side.rows - done
    nlat = scalars[0].shape[0]
    area = nlon * float(np.sum(np.sin(np.pi * (np.arange(nlat) + 0.5) / nlat)))
    mean = sums_ref[:, :LANES] * (1.0 / area)
    sends = []

    def send(view, i):
        n = len(sends)
        sends.append(pltpu.make_async_copy(out_ref.at[n], result_ref.at[view.row(i)], sem.at[n]))
        sends[-1].start()

    for i in range(done):
        kept = other.kept(i)
        for g in range(levels // 8):
            for _, at, lanes in side.tiles(g):
                shift = (mean[at] * kept)[:, : lanes.stop - lanes.start]
                out_ref[i, at, lanes] = done_ref[i, at, lanes] - shift
        send(other, i)

    new_ref = out_ref.at[pl.ds(done, count)]
    side.update(count, lambda i, g, k: packed_tile(b_ref, i, g, k, levels, nlon), new_ref)
    marked = side.any_marked()

    @pl.when(marked)
    def _():
        side.filter(count, tables, y_ref, s_ref, d_ref, new_ref)

    @pl.when(marked == False)
    def _():
        d_ref[...] = jnp.zeros_like(d_ref)

    start = nlon // 2 // LANES * LANES
    for i in range(count):
        kept = side.kept(i)
        for g in range(levels // 8):
            d = shifted(d_ref, i * levels + 8 * g, side)
            for _, at, lanes in side.tiles(g):
                less = (mean[at] * kept)[:, : lanes.stop - lanes.start]
                if lanes.start >= start:
                    less = less + d[:, lanes]
                new_ref[i, at, lanes] -= less
        send(side, i)
    for copy in sends:
        copy.wait()


def products(y_ref, high_ref, low_ref, c, chunk, units):
    both = jnp.dot(y_ref[...], high_ref[:, c : c + chunk], preferred_element_type=jnp.float32)
    third = jnp.dot(y_ref[:units, :], low_ref[:, c : c + chunk], preferred_element_type=jnp.float32)
    return both[:units] + both[units:] + third


def base_of(nlon):
    return nlon // LANES * LANES


def call(kernel, ins, outs, megabytes, scratch=(), out_space=pltpu.VMEM):
    return pl.pallas_call(
        kernel,
        in_specs=[pl.BlockSpec(memory_space=space) for _, space in ins],
        out_specs=[pl.BlockSpec(memory_space=out_space) for _ in outs],
        out_shape=[jax.ShapeDtypeStruct(shape, dtype) for shape, dtype in outs],
        scratch_shapes=list(scratch),
        compiler_params=pltpu.CompilerParams(vmem_limit_bytes=megabytes << 20),
    )(*[x for x, _ in ins])


def permute(x, pairs, axes="lat"):
    return lax.ppermute(x, axes, pairs)


def step(height, zonal_courant, merid_courant, rates, thresholds, flags, cutoffs):
    rows, levels, nlon = height.shape
    count = lax.axis_size("lat")
    nlat = rows * count
    half = nlon // 2
    smem, vmem, hbm = pltpu.SMEM, pltpu.VMEM, pltpu.HBM
    f32 = jnp.float32

    between = [(i, i + 1) for i in range(1, count - 1, 2)]
    within = [(i, i + 1) for i in range(0, count - 1, 2)]
    between = between + [(j, i) for i, j in between]
    parts = lax.axis_size("member")
    between = [(p * count + i, p * count + j) for p in range(parts) for i, j in between]
    ends = [0, count - 1] if count % 2 == 0 else [0]
    if parts % 2 == 0:
        between += [(p * count + e, (p ^ 1) * count + e) for p in range(parts) for e in ends]
    within = within + [(j, i) for i, j in within]
    whole, _, extra = dense_tiles(levels, nlon)
    (edge_b,) = call(
        pack_kernel,
        [
            (pltpu.with_memory_space_constraint(height, hbm), hbm),
            (pltpu.with_memory_space_constraint(merid_courant, hbm), hbm),
        ],
        [((3, 8 * (whole + extra), LANES), f32)],
        4,
        [pltpu.VMEM((3, levels, nlon), f32), pltpu.SemaphoreType.DMA((3,))],
    )
    b = permute(edge_b, between, ("member", "lat"))

    cos_row = jnp.asarray(np.sin(np.pi * (np.arange(nlat) + 0.5) / nlat).astype(np.float32))
    faces = np.sin(np.pi * np.arange(nlat + 1) / nlat)
    faces[0] = faces[nlat] = 0.0
    cos_face = jnp.asarray(faces.astype(np.float32))
    edge_a, sums, source = call(
        source_kernel,
        [(cos_row, smem), (rates[None], vmem), (thresholds[None], vmem), (height, vmem), (merid_courant, vmem)],
        [((3, levels, nlon), f32), ((levels, LANES), f32), (height.shape, f32)],
        8,
    )
    a = permute(edge_a, within)
    (part,) = call(zonal_kernel, [(height, vmem), (zonal_courant, vmem), (source, vmem)], [(height.shape, f32)], 8)
    depth = round_up(half, LANES)
    cols = 2 * round_up(half // 2 + 1, LANES)
    tables = []
    for parity in (0, 1):
        tables += call(
            functools.partial(table_kernel, parity, half),
            [(jnp.asarray(phases(nlon)[parity]), vmem)],
            [((depth, cols), jnp.bfloat16)] * 2 + [((cols, depth), jnp.bfloat16)] * 2,
            8,
        )

    bits = [1 << i for i in range((count - 1).bit_length())]
    if count == 1 << len(bits):
        far = bits[2:]
        rounds = [bits[:1], *([*far[i : i + 2], sum(far[i : i + 2])] for i in range(0, len(far), 2)), bits[1:2]]
        for masks in rounds:
            sums = sums + sum(permute(sums, [(p, p ^ mask) for p in range(count)]) for mask in dict.fromkeys(masks))
    else:
        sums = lax.psum(sums, "lat")

    scalars = [(x, smem) for x in (cos_row, cos_face, flags, cutoffs)]
    arrays = [(x, vmem) for x in (height, merid_courant, part)]
    held = [(x, vmem) for x in tables]

    def scratch(rows):
        return [
            pltpu.VMEM((2, 2 * rows * levels, depth), jnp.bfloat16),
            pltpu.VMEM((2, 2 * rows * levels, cols), jnp.bfloat16),
            pltpu.VMEM((rows * levels, depth), f32),
        ]

    done = rows - 2
    (near,) = call(near_kernel, [*scalars, *arrays, (a, vmem), *held], [((done, levels, nlon), f32)], 16, scratch(done))
    (out,) = call(
        finish_kernel,
        [*scalars, (sums, vmem), *arrays, (b, vmem), (near, vmem), *held],
        [(height.shape, f32)],
        16,
        [pltpu.VMEM(height.shape, f32), *scratch(2), pltpu.SemaphoreType.DMA((rows,))],
        hbm,
    )
    return out


def solution(mesh):
    split_rows = P(("member", "lat"), None, None)
    return jax.shard_map(
        step,
        mesh=mesh,
        in_specs=(split_rows, split_rows, split_rows, P("member"), P("member"), P(), P()),
        out_specs=split_rows,
        check_vma=False,
    )
```

```python
import functools

import jax
import jax.numpy as jnp
import numpy as np
from jax import lax
from jax.experimental import pallas as pl
from jax.experimental.pallas import tpu as pltpu
from jax.sharding import PartitionSpec as P

LANES = 128


def round_up(value, step):
    return -(-value // step) * step


@functools.cache
def phases(nlon):
    half = nlon // 2
    width = round_up(half // 2 + 1, LANES)
    depth = round_up(half, LANES)
    points = np.arange(depth)
    arrays = []
    for parity in (0, 1):
        waves = 2 * np.arange(width) + parity
        lanes = (waves <= half)[None, :]

        def both(steps, valid, axis):
            angle = 2.0 * np.pi / nlon * (steps % nlon)
            return np.concatenate([np.cos(angle) * valid, np.sin(angle) * valid], axis=axis)

        blocks = [
            both(points[::8, None] * waves[None, :], lanes & (points[::8, None] < half), 1),
            both(points[:8, None] * waves[None, :], True, 1),
            both(16 * np.arange(width // 8)[:, None] * points[None, :], (points < half)[None, :], 0),
            both(waves[:8, None] * points[None, :], True, 0),
        ]
        columns = max(x.shape[1] for x in blocks)
        arrays.append(
            np.concatenate([np.pad(x, ((0, 0), (0, columns - x.shape[1]))) for x in blocks]).astype(np.float32)
        )
    return arrays


def softplus(s):
    return jnp.maximum(s, 0.0) + jnp.log(1.0 + jnp.exp(-jnp.abs(s)))


def wrapped(row, nlon, full):
    base = nlon // LANES * LANES
    rest = nlon - base
    body, tail = row[:, :base], row[:, base:]
    tail = jnp.concatenate([tail, jnp.zeros((row.shape[0], full - nlon), row.dtype)], axis=1)
    lane = lax.broadcasted_iota(jnp.int32, tail.shape, 1)
    head = pltpu.roll(row[:, : full - base], rest, 1)
    end = pltpu.roll(tail, full - base - rest, 1)
    tail = jnp.where(lane < rest, tail, jnp.where(lane < full - base - 8, head, end))
    return jnp.concatenate([body, tail], axis=1)


def column(row):
    count = row.shape[1]
    same = lax.broadcasted_iota(jnp.int32, (count, count), 0) == lax.broadcasted_iota(
        jnp.int32, (count, count), 1
    )
    return jnp.sum(jnp.where(same, row, 0.0), axis=1, keepdims=True)


def dense_tiles(levels, nlon):
    rest = nlon % LANES
    shared = LANES // rest if rest else 1
    whole = levels // 8 * (nlon // LANES)
    return whole, shared, (-(-(levels // 8) // shared) if rest else 0)


def pack_row(row, out_ref, i):
    levels, nlon = row.shape
    whole, shared, extra = dense_tiles(levels, nlon)
    per = nlon // LANES
    rest = nlon % LANES
    for t in range(whole):
        g, k = divmod(t, per)
        out_ref[i, 8 * t : 8 * t + 8, :] = row[8 * g : 8 * g + 8, k * LANES : (k + 1) * LANES]
    for e in range(extra):
        parts = [
            row[8 * g : 8 * g + 8, per * LANES :]
            for g in range(e * shared, min((e + 1) * shared, levels // 8))
        ]
        parts.append(jnp.zeros((8, LANES - rest * len(parts)), row.dtype))
        t = whole + e
        out_ref[i, 8 * t : 8 * t + 8, :] = jnp.concatenate([p for p in parts if p.shape[1]], axis=1)


def packed_tile(ref, i, g, k, levels, nlon):
    whole, shared, _ = dense_tiles(levels, nlon)
    per = nlon // LANES
    rest = nlon % LANES
    if k < per:
        t = g * per + k
        return ref[i, 8 * t : 8 * t + 8, :]
    t = whole + g // shared
    last = ref[i, 8 * t : 8 * t + 8, :]
    at = g % shared * rest
    return (pltpu.roll(last, LANES - at, 1) if at else last)[:, :rest]


def edge_rows(upper, rows):
    return jnp.where(upper, rows - 2, 1), jnp.where(upper, rows - 1, 0)


def pack_kernel(
    h_ref, v_ref, cos_ref, flags_ref, cutoffs_ref, out_ref, about_ref, edge_ref, cos, flags, cutoffs, sem
):
    rows = h_ref.shape[0]
    nlat = flags_ref.shape[0]
    position = lax.axis_index("lat")
    first = position * rows
    far, near = edge_rows(position % 2 == 1, rows)
    moves = [(h_ref.at[far], edge_ref.at[0]), (h_ref.at[near], edge_ref.at[1]), (v_ref.at[near], edge_ref.at[2])]
    moves += [(cos_ref, cos), (flags_ref, flags), (cutoffs_ref, cutoffs)]
    copies = [pltpu.make_async_copy(source, target, sem.at[i]) for i, (source, target) in enumerate(moves)]
    for c in copies:
        c.start()
    for c in copies[3:]:
        c.wait()
    flat = (8, LANES)
    for j in range(rows):
        about_ref[j] = 1.0 / jnp.full(flat, cos[first + j])
        about_ref[rows + j] = jnp.full(flat, flags[first + j].astype(jnp.float32))
        about_ref[2 * rows + j] = jnp.full(flat, cutoffs[first + j].astype(jnp.float32))
        about_ref[3 * rows + j] = jnp.full(flat, cos[first + j])
    for f in range(rows + 1):
        about_ref[4 * rows + f] = jnp.full(flat, cos[nlat + first + f] * (0.5 / 12.0))
    for c in copies[:3]:
        c.wait()
    for i in range(3):
        pack_row(edge_ref[i], out_ref, i)


def source_kernel(about_ref, rates_ref, thresholds_ref, h_ref, v_ref, edge_ref, sum_ref, out_ref):
    rows, levels, nlon = h_ref.shape
    full = round_up(nlon, LANES)
    base = base_of(nlon)
    position = lax.axis_index("lat")
    rates = column(rates_ref[...])
    thresholds = column(thresholds_ref[...])
    total = jnp.zeros((levels, LANES), jnp.float32)
    for j in range(rows):
        s = softplus(h_ref[j] - thresholds) * -rates
        out_ref[j] = s
        acc = s[:, 0:LANES]
        for t in range(1, nlon // LANES):
            acc = acc + s[:, t * LANES : (t + 1) * LANES]
        if base < nlon:
            acc = acc + jnp.concatenate(
                [s[:, base:], jnp.zeros((levels, full - nlon), jnp.float32)], axis=1
            )
        weight = about_ref[3 * rows + j]
        total = total + acc * jnp.concatenate([weight] * (levels // 8), axis=0)
    total = jnp.broadcast_to(jnp.sum(total, axis=1, keepdims=True), (levels, LANES))
    sum_ref[...] = total
    far, near = edge_rows(position % 2 == 0, rows)
    edge_ref[0] = h_ref[far]
    edge_ref[1] = h_ref[near]
    edge_ref[2] = v_ref[near]


def zonal_kernel(h_ref, u_ref, s_ref, out_ref):
    rows, _, nlon = h_ref.shape
    full = round_up(nlon, LANES)
    for j in range(rows):
        h0 = h_ref[j]
        h = wrapped(h0, nlon, full)
        u = wrapped(u_ref[j], nlon, full)
        east = pltpu.roll(h, full - 1, 1)
        far_east = pltpu.roll(h, full - 2, 1)
        west = pltpu.roll(h, 1, 1)
        face = (7.0 * (h + east) - (west + far_east)) * (0.5 / 12.0)
        flux = (u + pltpu.roll(u, full - 1, 1)) * face
        div = flux - pltpu.roll(flux, 1, 1)
        out_ref[j] = h0 - div[:, :nlon] + s_ref[j]


def table_kernel(parity, half, source_ref, high_ref, low_ref, high_t_ref, low_t_ref):
    depth, cols = high_ref.shape
    width = cols // 2

    def put(high, low, at, cols, values):
        h = values.astype(jnp.bfloat16)
        high[at, cols] = h
        low[at, cols] = (values - h.astype(jnp.float32)).astype(jnp.bfloat16)

    def fill(coarse_cos, coarse_sin, fine_cos, fine_sin, count, store):
        for k in range(0, count, 2):
            pieces = []
            for q in (k, k + 1):
                cc, cs = coarse_cos(q), coarse_sin(q)
                pieces.append((cc * fine_cos - cs * fine_sin, cs * fine_cos + cc * fine_sin))
            store(k, *[jnp.concatenate(p, axis=0) for p in zip(*pieces)])

    def store(k, c, s):
        at = slice(8 * k, 8 * k + 16)
        put(high_ref, low_ref, at, slice(0, width), c)
        put(high_ref, low_ref, at, slice(width, cols), s)

    def store_t(k, c, s):
        if 2 * (8 * k + 15) + parity > half:
            waves = 2 * (8 * k + lax.broadcasted_iota(jnp.int32, c.shape, 0)) + parity
            c, s = jnp.where(waves <= half, c, 0.0), jnp.where(waves <= half, s, 0.0)
        put(high_t_ref, low_t_ref, slice(8 * k, 8 * k + 16), slice(None), c)
        put(high_t_ref, low_t_ref, slice(width + 8 * k, width + 8 * k + 16), slice(None), s)

    fine = depth // 8
    turned = fine + 8
    fine_t = turned + 2 * (width // 8)
    fill(
        lambda q: source_ref[q : q + 1, :width],
        lambda q: source_ref[q : q + 1, width:cols],
        source_ref[fine : fine + 8, :width],
        source_ref[fine : fine + 8, width:cols],
        depth // 8,
        store,
    )
    fill(
        lambda q: source_ref[turned + q : turned + q + 1, :depth],
        lambda q: source_ref[turned + width // 8 + q : turned + width // 8 + q + 1, :depth],
        source_ref[fine_t : fine_t + 8, :depth],
        source_ref[fine_t + 8 : fine_t + 16, :depth],
        width // 8,
        store_t,
    )


class Side:
    def __init__(self, lower, about_ref, arrays):
        self.about_ref = about_ref
        self.h_ref, self.v_ref, self.part_ref = arrays
        self.rows, self.levels, self.nlon = self.h_ref.shape
        self.full = round_up(self.nlon, LANES)
        self.lower = lower
        self.outermost = lax.axis_index("lat") == jnp.where(lower, 0, lax.axis_size("lat") - 1)

    def row(self, i):
        return jnp.where(self.lower, i, self.rows - 1 - i)

    def tiles(self, g):
        for k in range(self.full // LANES):
            yield k, slice(8 * g, 8 * g + 8), slice(k * LANES, min((k + 1) * LANES, self.nlon))

    def any_marked(self):
        marked = self.about_ref[self.rows]
        for j in range(1, self.rows):
            marked = jnp.maximum(marked, self.about_ref[self.rows + j])
        return marked[0, 0] > 0

    def update(self, count, halo_tile, out_ref):
        sign = jnp.where(self.lower, 1.0, -1.0)
        scale = [self.about_ref[self.row(i)] * sign for i in range(count)]
        face_cos = [
            self.about_ref[4 * self.rows + jnp.where(self.lower, i, self.rows - i)] for i in range(count + 1)
        ]
        for g in range(self.levels // 8):
            for k, at, lanes in self.tiles(g):
                wide = lanes.stop - lanes.start
                far, near, beyond = (jnp.where(self.outermost, 0.0, halo_tile(i, g, k)) for i in range(3))
                height = [far, near, *(self.h_ref[self.row(i), at, lanes] for i in range(count + 2))]
                speed = [beyond, *(self.v_ref[self.row(i), at, lanes] for i in range(count + 1))]
                flux = []
                for f in range(count + 1):
                    p = 7.0 * (height[f + 1] + height[f + 2]) - (height[f] + height[f + 3])
                    flux.append((speed[f] + speed[f + 1]) * face_cos[f][:, :wide] * p)
                for i in range(count):
                    div = (flux[i + 1] - flux[i]) * scale[i][:, :wide]
                    out_ref[i, at, lanes] = self.part_ref[self.row(i), at, lanes] - div

    def filter(self, count, tables, y_ref, s_ref, d_ref, out_ref):
        levels, nlon, full = self.levels, self.nlon, self.full
        half = nlon // 2
        depth, cols = tables[0].shape
        width = cols // 2
        units = count * levels
        for r in range(0, units, 16):
            j, q = divmod(r, levels)
            x = out_ref[j, q : q + 16, :]
            near = x[:, :depth]
            x = jnp.concatenate([x, jnp.zeros((16, full - nlon), jnp.float32)], axis=1)
            far = pltpu.roll(x, full - half, 1)[:, :depth]
            for parity, y in ((0, near + far), (1, near - far)):
                put_parts(y_ref, parity, r, units, slice(None), y)
        lane = lax.broadcasted_iota(jnp.int32, (8, width), 1)
        chunk = 256 if cols % 256 == 0 and depth % 256 == 0 else LANES
        for parity in (0, 1):
            high_ref, low_ref = tables[4 * parity : 4 * parity + 2]
            waves = 2 * lane + parity
            weight = jnp.where((waves > 0) & (waves < half), 2.0 / nlon, 1.0 / nlon)
            inverse = 1.0 / jnp.maximum(waves, 1).astype(jnp.float32)
            factors = []
            for j in range(count):
                row = self.rows + self.row(j)
                ratio = self.about_ref[self.rows + row][:, :1] * inverse
                factor = (1.0 - jnp.minimum(1.0, ratio * ratio)) * weight
                factor = jnp.where(self.about_ref[row][:, :1] > 0, factor, 0.0)
                factors.append(jnp.concatenate([factor, factor], axis=1))
            for c in range(0, cols, chunk):
                spectrum = products(y_ref.at[parity], high_ref, low_ref, c, chunk, units)
                for r in range(0, units, 16):
                    f = factors[r // levels][:, c : c + chunk]
                    y = spectrum[r : r + 16] * jnp.concatenate([f, f], axis=0)
                    put_parts(s_ref, parity, r, units, slice(c, c + chunk), y)
        for c in range(0, depth, chunk):
            even = products(s_ref.at[0], tables[2], tables[3], c, chunk, units)
            uneven = products(s_ref.at[1], tables[6], tables[7], c, chunk, units)
            for r in range(0, units, 16):
                j, q = divmod(r, levels)
                x, y = even[r : r + 16], uneven[r : r + 16]
                out_ref[j, q : q + 16, c : c + chunk] -= x + y
                d_ref[r : r + 16, c : c + chunk] = x - y
        start = half // LANES * LANES
        for r in range(0, units, 8):
            j, q = divmod(r, levels)
            d = jnp.concatenate([d_ref[r : r + 8, :], jnp.zeros((8, full - depth), jnp.float32)], axis=1)
            out_ref[j, q : q + 8, start:] -= pltpu.roll(d, half, 1)[:, start:nlon]


def put_parts(ref, parity, r, units, lanes, y):
    high = y.astype(jnp.bfloat16)
    ref[parity, r : r + 16, lanes] = high
    ref[parity, units + r : units + r + 16, lanes] = (y - high.astype(jnp.float32)).astype(jnp.bfloat16)


def near_kernel(about_ref, h_ref, v_ref, part_ref, a_ref, *refs):
    tables, out_ref, scratch = refs[:8], refs[8], refs[9:]
    side = Side(lax.axis_index("lat") % 2 == 1, about_ref, (h_ref, v_ref, part_ref))
    count = out_ref.shape[0]

    def halo_tile(i, g, k):
        return a_ref[i, 8 * g : 8 * g + 8, k * LANES : min((k + 1) * LANES, side.nlon)]

    side.update(count, halo_tile, out_ref)
    pl.when(side.any_marked())(lambda: side.filter(count, tables, *scratch, out_ref))


def far_kernel(about_ref, h_ref, v_ref, part_ref, b_ref, *refs):
    tables, out_ref, scratch = refs[:8], refs[8], refs[9:]
    side = Side(lax.axis_index("lat") % 2 == 0, about_ref, (h_ref, v_ref, part_ref))
    count = out_ref.shape[0]
    side.update(count, lambda i, g, k: packed_tile(b_ref, i, g, k, side.levels, side.nlon), out_ref)
    pl.when(side.any_marked())(lambda: side.filter(count, tables, *scratch, out_ref))


def mean_kernel(nlat, about_ref, sums_ref, near_ref, far_ref, out_ref, row_ref, sem):
    rows, levels, nlon = row_ref.shape
    odd = lax.axis_index("lat") % 2 == 1
    area = nlon * float(np.sum(np.sin(np.pi * (np.arange(nlat) + 0.5) / nlat)))
    mean = sums_ref[...] * (1.0 / area)
    done = near_ref.shape[0]
    copies = []
    for i in range(rows):
        ref, k, lower = (near_ref, i, odd) if i < done else (far_ref, i - done, odd == False)
        row = jnp.where(lower, k, rows - 1 - k)
        cut = about_ref[2 * rows + row]
        kept = jnp.where(about_ref[rows + row] > 0, jnp.minimum(1.0, cut * cut), 1.0)
        for g in range(levels // 8):
            at = slice(8 * g, 8 * g + 8)
            shift = mean[at] * kept
            for t in range(0, nlon, LANES):
                lanes = slice(t, min(t + LANES, nlon))
                row_ref[i, at, lanes] = ref[k, at, lanes] - shift[:, : lanes.stop - lanes.start]
        copies.append(pltpu.make_async_copy(row_ref.at[i], out_ref.at[row], sem.at[i]))
        copies[-1].start()
    for c in copies:
        c.wait()


def products(y_ref, high_ref, low_ref, c, chunk, units):
    both = jnp.dot(y_ref[...], high_ref[:, c : c + chunk], preferred_element_type=jnp.float32)
    third = jnp.dot(y_ref[:units, :], low_ref[:, c : c + chunk], preferred_element_type=jnp.float32)
    return both[:units] + both[units:] + third


def base_of(nlon):
    return nlon // LANES * LANES


def call(kernel, ins, outs, megabytes, scratch=(), out_space=pltpu.VMEM):
    return pl.pallas_call(
        kernel,
        in_specs=[pl.BlockSpec(memory_space=space) for _, space in ins],
        out_specs=[pl.BlockSpec(memory_space=out_space) for _ in outs],
        out_shape=[jax.ShapeDtypeStruct(shape, dtype) for shape, dtype in outs],
        scratch_shapes=list(scratch),
        compiler_params=pltpu.CompilerParams(vmem_limit_bytes=megabytes << 20),
    )(*[x for x, _ in ins])


def permute(x, pairs, axes="lat"):
    return lax.ppermute(x, axes, pairs)


def step(height, zonal_courant, merid_courant, rates, thresholds, flags, cutoffs):
    rows, levels, nlon = height.shape
    count = lax.axis_size("lat")
    nlat = rows * count
    half = nlon // 2
    vmem, hbm = pltpu.VMEM, pltpu.HBM
    f32 = jnp.float32

    between = [(i, i + 1) for i in range(1, count - 1, 2)]
    within = [(i, i + 1) for i in range(0, count - 1, 2)]
    between = between + [(j, i) for i, j in between]
    parts = lax.axis_size("member")
    between = [(p * count + i, p * count + j) for p in range(parts) for i, j in between]
    ends = [0, count - 1] if count % 2 == 0 else [0]
    if parts % 2 == 0:
        between += [(p * count + e, (p ^ 1) * count + e) for p in range(parts) for e in ends]
    within = within + [(j, i) for i, j in within]
    whole, _, extra = dense_tiles(levels, nlon)
    faces = np.sin(np.pi * np.arange(nlat + 1) / nlat)
    faces[0] = faces[nlat] = 0.0
    cosines = np.concatenate([np.sin(np.pi * (np.arange(nlat) + 0.5) / nlat), faces])
    cosines = jnp.asarray(cosines.astype(np.float32))
    edge_b, about = call(
        pack_kernel,
        [
            (pltpu.with_memory_space_constraint(x, hbm), hbm)
            for x in (height, merid_courant, cosines, flags, cutoffs)
        ],
        [((3, 8 * (whole + extra), LANES), f32), ((5 * rows + 1, 8, LANES), f32)],
        4,
        [
            pltpu.VMEM((3, levels, nlon), f32),
            pltpu.SMEM(cosines.shape, f32),
            pltpu.SMEM(flags.shape, jnp.int32),
            pltpu.SMEM(cutoffs.shape, jnp.int32),
            pltpu.SemaphoreType.DMA((6,)),
        ],
    )
    b = permute(edge_b, between, ("member", "lat"))

    edge_a, sums, source = call(
        source_kernel,
        [(x, vmem) for x in (about, rates[None], thresholds[None], height, merid_courant)],
        [((3, levels, nlon), f32), ((levels, LANES), f32), (height.shape, f32)],
        8,
    )
    a = permute(edge_a, within)
    (part,) = call(zonal_kernel, [(height, vmem), (zonal_courant, vmem), (source, vmem)], [(height.shape, f32)], 8)
    depth = round_up(half, LANES)
    cols = 2 * round_up(half // 2 + 1, LANES)
    tables = []
    for parity in (0, 1):
        tables += call(
            functools.partial(table_kernel, parity, half),
            [(jnp.asarray(phases(nlon)[parity]), vmem)],
            [((depth, cols), jnp.bfloat16)] * 2 + [((cols, depth), jnp.bfloat16)] * 2,
            8,
        )

    bits = [1 << i for i in range((count - 1).bit_length())]
    if count == 1 << len(bits):
        far = bits[2:]
        rounds = [bits[:1], *([*far[i : i + 2], sum(far[i : i + 2])] for i in range(0, len(far), 2)), bits[1:2]]
        for masks in rounds:
            sums = sums + sum(permute(sums, [(p, p ^ mask) for p in range(count)]) for mask in dict.fromkeys(masks))
    else:
        sums = lax.psum(sums, "lat")

    def rows_of(kernel, edge, rows):
        return call(
            kernel,
            [(x, vmem) for x in (about, height, merid_courant, part, edge, *tables)],
            [((rows, levels, nlon), f32)],
            16,
            [
                pltpu.VMEM((2, 2 * rows * levels, depth), jnp.bfloat16),
                pltpu.VMEM((2, 2 * rows * levels, cols), jnp.bfloat16),
                pltpu.VMEM((rows * levels, depth), f32),
            ],
        )[0]

    near = rows_of(near_kernel, a, rows - 2)
    far = rows_of(far_kernel, b, 2)
    (out,) = call(
        functools.partial(mean_kernel, nlat),
        [(x, vmem) for x in (about, sums, near, far)],
        [(height.shape, f32)],
        4,
        [pltpu.VMEM(height.shape, f32), pltpu.SemaphoreType.DMA((rows,))],
        hbm,
    )
    return out


def solution(mesh):
    split_rows = P(("member", "lat"), None, None)
    return jax.shard_map(
        step,
        mesh=mesh,
        in_specs=(split_rows, split_rows, split_rows, P("member"), P("member"), P(), P()),
        out_specs=split_rows,
        check_vma=False,
    )
```

```python
import functools

import jax
import jax.numpy as jnp
import numpy as np
from jax import lax
from jax.experimental import pallas as pl
from jax.experimental.pallas import tpu as pltpu
from jax.sharding import PartitionSpec as P

LANES = 128


def round_up(value, step):
    return -(-value // step) * step


@functools.cache
def phases(nlon):
    half = nlon // 2
    width = round_up(half // 2 + 1, LANES)
    depth = round_up(half, LANES)
    points = np.arange(depth)
    arrays = []
    for parity in (0, 1):
        waves = 2 * np.arange(width) + parity
        lanes = (waves <= half)[None, :]

        def both(steps, valid, axis):
            angle = 2.0 * np.pi / nlon * (steps % nlon)
            return np.concatenate([np.cos(angle) * valid, np.sin(angle) * valid], axis=axis)

        blocks = [
            both(points[::8, None] * waves[None, :], lanes & (points[::8, None] < half), 1),
            both(points[:8, None] * waves[None, :], True, 1),
            both(16 * np.arange(width // 8)[:, None] * points[None, :], (points < half)[None, :], 0),
            both(waves[:8, None] * points[None, :], True, 0),
        ]
        columns = max(x.shape[1] for x in blocks)
        arrays.append(
            np.concatenate([np.pad(x, ((0, 0), (0, columns - x.shape[1]))) for x in blocks]).astype(np.float32)
        )
    return arrays


def softplus(s):
    return jnp.maximum(s, 0.0) + jnp.log(1.0 + jnp.exp(-jnp.abs(s)))


def wrapped(row, nlon, full):
    base = nlon // LANES * LANES
    rest = nlon - base
    body, tail = row[:, :base], row[:, base:]
    tail = jnp.concatenate([tail, jnp.zeros((row.shape[0], full - nlon), row.dtype)], axis=1)
    lane = lax.broadcasted_iota(jnp.int32, tail.shape, 1)
    head = pltpu.roll(row[:, : full - base], rest, 1)
    end = pltpu.roll(tail, full - base - rest, 1)
    tail = jnp.where(lane < rest, tail, jnp.where(lane < full - base - 8, head, end))
    return jnp.concatenate([body, tail], axis=1)


def diagonal(shape):
    return lax.broadcasted_iota(jnp.int32, shape, 0) == lax.broadcasted_iota(jnp.int32, shape, 1)


def column(row):
    count = row.shape[1]
    same = lax.broadcasted_iota(jnp.int32, (count, count), 0) == lax.broadcasted_iota(
        jnp.int32, (count, count), 1
    )
    return jnp.sum(jnp.where(same, row, 0.0), axis=1, keepdims=True)


def dense_tiles(levels, nlon):
    rest = nlon % LANES
    shared = LANES // rest if rest else 1
    whole = levels // 8 * (nlon // LANES)
    return whole, shared, (-(-(levels // 8) // shared) if rest else 0)


def pack_row(row, out_ref, i):
    levels, nlon = row.shape
    whole, shared, extra = dense_tiles(levels, nlon)
    per = nlon // LANES
    rest = nlon % LANES
    for t in range(whole):
        g, k = divmod(t, per)
        out_ref[i, 8 * t : 8 * t + 8, :] = row[8 * g : 8 * g + 8, k * LANES : (k + 1) * LANES]
    for e in range(extra):
        parts = [
            row[8 * g : 8 * g + 8, per * LANES :]
            for g in range(e * shared, min((e + 1) * shared, levels // 8))
        ]
        parts.append(jnp.zeros((8, LANES - rest * len(parts)), row.dtype))
        t = whole + e
        out_ref[i, 8 * t : 8 * t + 8, :] = jnp.concatenate([p for p in parts if p.shape[1]], axis=1)


def packed_tile(ref, i, g, k, levels, nlon):
    whole, shared, _ = dense_tiles(levels, nlon)
    per = nlon // LANES
    rest = nlon % LANES
    if k < per:
        t = g * per + k
        return ref[i, 8 * t : 8 * t + 8, :]
    t = whole + g // shared
    last = ref[i, 8 * t : 8 * t + 8, :]
    at = g % shared * rest
    return (pltpu.roll(last, LANES - at, 1) if at else last)[:, :rest]


def edge_rows(upper, rows):
    return jnp.where(upper, rows - 2, 1), jnp.where(upper, rows - 1, 0)


def pack_kernel(
    h_ref, v_ref, cos_ref, flags_ref, cutoffs_ref, out_ref, about_ref, edge_ref, cos, flags, cutoffs, sem
):
    rows = h_ref.shape[0]
    nlat = flags_ref.shape[0]
    position = lax.axis_index("lat")
    first = position * rows
    far, near = edge_rows(position % 2 == 1, rows)
    moves = [(h_ref.at[far], edge_ref.at[0]), (h_ref.at[near], edge_ref.at[1]), (v_ref.at[near], edge_ref.at[2])]
    moves += [(cos_ref, cos), (flags_ref, flags), (cutoffs_ref, cutoffs)]
    copies = [pltpu.make_async_copy(source, target, sem.at[i]) for i, (source, target) in enumerate(moves)]
    for c in copies:
        c.start()
    for c in copies[3:]:
        c.wait()
    flat = (8, LANES)
    for j in range(rows):
        about_ref[j] = 1.0 / jnp.full(flat, cos[first + j])
        about_ref[rows + j] = jnp.full(flat, flags[first + j].astype(jnp.float32))
        about_ref[2 * rows + j] = jnp.full(flat, cutoffs[first + j].astype(jnp.float32))
        about_ref[3 * rows + j] = jnp.full(flat, cos[first + j])
    for f in range(rows + 1):
        about_ref[4 * rows + f] = jnp.full(flat, cos[nlat + first + f] * (0.5 / 12.0))
    for c in copies[:3]:
        c.wait()
    for i in range(3):
        pack_row(edge_ref[i], out_ref, i)


def source_kernel(about_ref, rates_ref, thresholds_ref, h_ref, v_ref, edge_ref, sum_ref, out_ref):
    rows, levels, nlon = h_ref.shape
    full = round_up(nlon, LANES)
    base = base_of(nlon)
    position = lax.axis_index("lat")
    rates = column(rates_ref[...])
    thresholds = column(thresholds_ref[...])
    total = jnp.zeros((levels, LANES), jnp.float32)
    for j in range(rows):
        s = softplus(h_ref[j] - thresholds) * -rates
        out_ref[j] = s
        acc = s[:, 0:LANES]
        for t in range(1, nlon // LANES):
            acc = acc + s[:, t * LANES : (t + 1) * LANES]
        if base < nlon:
            acc = acc + jnp.concatenate(
                [s[:, base:], jnp.zeros((levels, full - nlon), jnp.float32)], axis=1
            )
        weight = about_ref[3 * rows + j]
        total = total + acc * jnp.concatenate([weight] * (levels // 8), axis=0)
    total = jnp.broadcast_to(jnp.sum(total, axis=1, keepdims=True), (levels, sum_ref.shape[1]))
    sum_ref[...] = jnp.sum(jnp.where(diagonal(total.shape), total, 0.0), axis=0, keepdims=True)
    far, near = edge_rows(position % 2 == 0, rows)
    edge_ref[0] = h_ref[far]
    edge_ref[1] = h_ref[near]
    edge_ref[2] = v_ref[near]


def zonal_kernel(h_ref, u_ref, s_ref, out_ref):
    rows, _, nlon = h_ref.shape
    full = round_up(nlon, LANES)
    for j in range(rows):
        h0 = h_ref[j]
        h = wrapped(h0, nlon, full)
        u = wrapped(u_ref[j], nlon, full)
        east = pltpu.roll(h, full - 1, 1)
        far_east = pltpu.roll(h, full - 2, 1)
        west = pltpu.roll(h, 1, 1)
        face = (7.0 * (h + east) - (west + far_east)) * (0.5 / 12.0)
        flux = (u + pltpu.roll(u, full - 1, 1)) * face
        div = flux - pltpu.roll(flux, 1, 1)
        out_ref[j] = h0 - div[:, :nlon] + s_ref[j]


def table_kernel(parity, half, source_ref, high_ref, low_ref, high_t_ref, low_t_ref):
    depth, cols = high_ref.shape
    width = cols // 2

    def put(high, low, at, cols, values):
        h = values.astype(jnp.bfloat16)
        high[at, cols] = h
        low[at, cols] = (values - h.astype(jnp.float32)).astype(jnp.bfloat16)

    def fill(coarse_cos, coarse_sin, fine_cos, fine_sin, count, store):
        for k in range(0, count, 2):
            pieces = []
            for q in (k, k + 1):
                cc, cs = coarse_cos(q), coarse_sin(q)
                pieces.append((cc * fine_cos - cs * fine_sin, cs * fine_cos + cc * fine_sin))
            store(k, *[jnp.concatenate(p, axis=0) for p in zip(*pieces)])

    def store(k, c, s):
        at = slice(8 * k, 8 * k + 16)
        put(high_ref, low_ref, at, slice(0, width), c)
        put(high_ref, low_ref, at, slice(width, cols), s)

    def store_t(k, c, s):
        if 2 * (8 * k + 15) + parity > half:
            waves = 2 * (8 * k + lax.broadcasted_iota(jnp.int32, c.shape, 0)) + parity
            c, s = jnp.where(waves <= half, c, 0.0), jnp.where(waves <= half, s, 0.0)
        put(high_t_ref, low_t_ref, slice(8 * k, 8 * k + 16), slice(None), c)
        put(high_t_ref, low_t_ref, slice(width + 8 * k, width + 8 * k + 16), slice(None), s)

    fine = depth // 8
    turned = fine + 8
    fine_t = turned + 2 * (width // 8)
    fill(
        lambda q: source_ref[q : q + 1, :width],
        lambda q: source_ref[q : q + 1, width:cols],
        source_ref[fine : fine + 8, :width],
        source_ref[fine : fine + 8, width:cols],
        depth // 8,
        store,
    )
    fill(
        lambda q: source_ref[turned + q : turned + q + 1, :depth],
        lambda q: source_ref[turned + width // 8 + q : turned + width // 8 + q + 1, :depth],
        source_ref[fine_t : fine_t + 8, :depth],
        source_ref[fine_t + 8 : fine_t + 16, :depth],
        width // 8,
        store_t,
    )


class Side:
    def __init__(self, lower, about_ref, arrays):
        self.about_ref = about_ref
        self.h_ref, self.v_ref, self.part_ref = arrays
        self.rows, self.levels, self.nlon = self.h_ref.shape
        self.full = round_up(self.nlon, LANES)
        self.lower = lower
        self.outermost = lax.axis_index("lat") == jnp.where(lower, 0, lax.axis_size("lat") - 1)

    def row(self, i):
        return jnp.where(self.lower, i, self.rows - 1 - i)

    def tiles(self, g):
        for k in range(self.full // LANES):
            yield k, slice(8 * g, 8 * g + 8), slice(k * LANES, min((k + 1) * LANES, self.nlon))

    def any_marked(self):
        marked = self.about_ref[self.rows]
        for j in range(1, self.rows):
            marked = jnp.maximum(marked, self.about_ref[self.rows + j])
        return marked[0, 0] > 0

    def update(self, count, halo_tile, out_ref):
        sign = jnp.where(self.lower, 1.0, -1.0)
        scale = [self.about_ref[self.row(i)] * sign for i in range(count)]
        face_cos = [
            self.about_ref[4 * self.rows + jnp.where(self.lower, i, self.rows - i)] for i in range(count + 1)
        ]
        for g in range(self.levels // 8):
            for k, at, lanes in self.tiles(g):
                wide = lanes.stop - lanes.start
                far, near, beyond = (jnp.where(self.outermost, 0.0, halo_tile(i, g, k)) for i in range(3))
                height = [far, near, *(self.h_ref[self.row(i), at, lanes] for i in range(count + 2))]
                speed = [beyond, *(self.v_ref[self.row(i), at, lanes] for i in range(count + 1))]
                flux = []
                for f in range(count + 1):
                    p = 7.0 * (height[f + 1] + height[f + 2]) - (height[f] + height[f + 3])
                    flux.append((speed[f] + speed[f + 1]) * face_cos[f][:, :wide] * p)
                for i in range(count):
                    div = (flux[i + 1] - flux[i]) * scale[i][:, :wide]
                    out_ref[i, at, lanes] = self.part_ref[self.row(i), at, lanes] - div

    def filter(self, count, tables, y_ref, s_ref, d_ref, out_ref):
        levels, nlon, full = self.levels, self.nlon, self.full
        half = nlon // 2
        depth, cols = tables[0].shape
        width = cols // 2
        units = count * levels
        for r in range(0, units, 16):
            j, q = divmod(r, levels)
            x = out_ref[j, q : q + 16, :]
            near = x[:, :depth]
            x = jnp.concatenate([x, jnp.zeros((16, full - nlon), jnp.float32)], axis=1)
            far = pltpu.roll(x, full - half, 1)[:, :depth]
            for parity, y in ((0, near + far), (1, near - far)):
                put_parts(y_ref, parity, r, units, slice(None), y)
        lane = lax.broadcasted_iota(jnp.int32, (8, width), 1)
        chunk = 256 if cols % 256 == 0 and depth % 256 == 0 else LANES
        for parity in (0, 1):
            high_ref, low_ref = tables[4 * parity : 4 * parity + 2]
            waves = 2 * lane + parity
            weight = jnp.where((waves > 0) & (waves < half), 2.0 / nlon, 1.0 / nlon)
            inverse = 1.0 / jnp.maximum(waves, 1).astype(jnp.float32)
            factors = []
            for j in range(count):
                row = self.rows + self.row(j)
                ratio = self.about_ref[self.rows + row][:, :1] * inverse
                factor = (1.0 - jnp.minimum(1.0, ratio * ratio)) * weight
                factor = jnp.where(self.about_ref[row][:, :1] > 0, factor, 0.0)
                factors.append(jnp.concatenate([factor, factor], axis=1))
            for c in range(0, cols, chunk):
                spectrum = products(y_ref.at[parity], high_ref, low_ref, c, chunk, units)
                for r in range(0, units, 16):
                    f = factors[r // levels][:, c : c + chunk]
                    y = spectrum[r : r + 16] * jnp.concatenate([f, f], axis=0)
                    put_parts(s_ref, parity, r, units, slice(c, c + chunk), y)
        for c in range(0, depth, chunk):
            even = products(s_ref.at[0], tables[2], tables[3], c, chunk, units)
            uneven = products(s_ref.at[1], tables[6], tables[7], c, chunk, units)
            for r in range(0, units, 16):
                j, q = divmod(r, levels)
                x, y = even[r : r + 16], uneven[r : r + 16]
                out_ref[j, q : q + 16, c : c + chunk] -= x + y
                d_ref[r : r + 16, c : c + chunk] = x - y
        start = half // LANES * LANES
        for r in range(0, units, 8):
            j, q = divmod(r, levels)
            d = jnp.concatenate([d_ref[r : r + 8, :], jnp.zeros((8, full - depth), jnp.float32)], axis=1)
            out_ref[j, q : q + 8, start:] -= pltpu.roll(d, half, 1)[:, start:nlon]


def put_parts(ref, parity, r, units, lanes, y):
    high = y.astype(jnp.bfloat16)
    ref[parity, r : r + 16, lanes] = high
    ref[parity, units + r : units + r + 16, lanes] = (y - high.astype(jnp.float32)).astype(jnp.bfloat16)


def near_kernel(about_ref, h_ref, v_ref, part_ref, a_ref, *refs):
    tables, out_ref, scratch = refs[:8], refs[8], refs[9:]
    side = Side(lax.axis_index("lat") % 2 == 1, about_ref, (h_ref, v_ref, part_ref))
    count = out_ref.shape[0]

    def halo_tile(i, g, k):
        return a_ref[i, 8 * g : 8 * g + 8, k * LANES : min((k + 1) * LANES, side.nlon)]

    side.update(count, halo_tile, out_ref)
    pl.when(side.any_marked())(lambda: side.filter(count, tables, *scratch, out_ref))


def far_kernel(about_ref, h_ref, v_ref, part_ref, b_ref, *refs):
    tables, out_ref, scratch = refs[:8], refs[8], refs[9:]
    side = Side(lax.axis_index("lat") % 2 == 0, about_ref, (h_ref, v_ref, part_ref))
    count = out_ref.shape[0]
    side.update(count, lambda i, g, k: packed_tile(b_ref, i, g, k, side.levels, side.nlon), out_ref)
    pl.when(side.any_marked())(lambda: side.filter(count, tables, *scratch, out_ref))


def mean_kernel(nlat, about_ref, sums_ref, near_ref, far_ref, out_ref, row_ref, sem):
    rows, levels, nlon = row_ref.shape
    odd = lax.axis_index("lat") % 2 == 1
    area = nlon * float(np.sum(np.sin(np.pi * (np.arange(nlat) + 0.5) / nlat)))
    width = sums_ref.shape[1]
    mean = jnp.where(diagonal((levels, width)), sums_ref[...] * (1.0 / area), 0.0)
    mean = jnp.broadcast_to(jnp.sum(mean, axis=1, keepdims=True), (levels, LANES))
    done = near_ref.shape[0]
    copies = []
    for i in range(rows):
        ref, k, lower = (near_ref, i, odd) if i < done else (far_ref, i - done, odd == False)
        row = jnp.where(lower, k, rows - 1 - k)
        cut = about_ref[2 * rows + row]
        kept = jnp.where(about_ref[rows + row] > 0, jnp.minimum(1.0, cut * cut), 1.0)
        for g in range(levels // 8):
            at = slice(8 * g, 8 * g + 8)
            shift = mean[at] * kept
            for t in range(0, nlon, LANES):
                lanes = slice(t, min(t + LANES, nlon))
                row_ref[i, at, lanes] = ref[k, at, lanes] - shift[:, : lanes.stop - lanes.start]
        copies.append(pltpu.make_async_copy(row_ref.at[i], out_ref.at[row], sem.at[i]))
        copies[-1].start()
    for c in copies:
        c.wait()


def products(y_ref, high_ref, low_ref, c, chunk, units):
    both = jnp.dot(y_ref[...], high_ref[:, c : c + chunk], preferred_element_type=jnp.float32)
    third = jnp.dot(y_ref[:units, :], low_ref[:, c : c + chunk], preferred_element_type=jnp.float32)
    return both[:units] + both[units:] + third


def base_of(nlon):
    return nlon // LANES * LANES


def call(kernel, ins, outs, megabytes, scratch=(), out_space=pltpu.VMEM):
    return pl.pallas_call(
        kernel,
        in_specs=[pl.BlockSpec(memory_space=space) for _, space in ins],
        out_specs=[pl.BlockSpec(memory_space=out_space) for _ in outs],
        out_shape=[jax.ShapeDtypeStruct(shape, dtype) for shape, dtype in outs],
        scratch_shapes=list(scratch),
        compiler_params=pltpu.CompilerParams(vmem_limit_bytes=megabytes << 20),
    )(*[x for x, _ in ins])


def permute(x, pairs, axes="lat"):
    return lax.ppermute(x, axes, pairs)


def step(height, zonal_courant, merid_courant, rates, thresholds, flags, cutoffs):
    rows, levels, nlon = height.shape
    count = lax.axis_size("lat")
    nlat = rows * count
    half = nlon // 2
    vmem, hbm = pltpu.VMEM, pltpu.HBM
    f32 = jnp.float32

    between = [(i, i + 1) for i in range(1, count - 1, 2)]
    within = [(i, i + 1) for i in range(0, count - 1, 2)]
    between = between + [(j, i) for i, j in between]
    parts = lax.axis_size("member")
    between = [(p * count + i, p * count + j) for p in range(parts) for i, j in between]
    ends = [0, count - 1] if count % 2 == 0 else [0]
    if parts % 2 == 0:
        between += [(p * count + e, (p ^ 1) * count + e) for p in range(parts) for e in ends]
    within = within + [(j, i) for i, j in within]
    whole, _, extra = dense_tiles(levels, nlon)
    faces = np.sin(np.pi * np.arange(nlat + 1) / nlat)
    faces[0] = faces[nlat] = 0.0
    cosines = np.concatenate([np.sin(np.pi * (np.arange(nlat) + 0.5) / nlat), faces])
    cosines = jnp.asarray(cosines.astype(np.float32))
    edge_b, about = call(
        pack_kernel,
        [
            (pltpu.with_memory_space_constraint(x, hbm), hbm)
            for x in (height, merid_courant, cosines, flags, cutoffs)
        ],
        [((3, 8 * (whole + extra), LANES), f32), ((5 * rows + 1, 8, LANES), f32)],
        4,
        [
            pltpu.VMEM((3, levels, nlon), f32),
            pltpu.SMEM(cosines.shape, f32),
            pltpu.SMEM(flags.shape, jnp.int32),
            pltpu.SMEM(cutoffs.shape, jnp.int32),
            pltpu.SemaphoreType.DMA((6,)),
        ],
    )
    b = permute(edge_b, between, ("member", "lat"))

    edge_a, sums, source = call(
        source_kernel,
        [(x, vmem) for x in (about, rates[None], thresholds[None], height, merid_courant)],
        [((3, levels, nlon), f32), ((1, round_up(levels, LANES)), f32), (height.shape, f32)],
        8,
    )
    a = permute(edge_a, within)
    (part,) = call(zonal_kernel, [(height, vmem), (zonal_courant, vmem), (source, vmem)], [(height.shape, f32)], 8)
    depth = round_up(half, LANES)
    cols = 2 * round_up(half // 2 + 1, LANES)
    tables = []
    for parity in (0, 1):
        tables += call(
            functools.partial(table_kernel, parity, half),
            [(jnp.asarray(phases(nlon)[parity]), vmem)],
            [((depth, cols), jnp.bfloat16)] * 2 + [((cols, depth), jnp.bfloat16)] * 2,
            8,
        )

    bits = [1 << i for i in range((count - 1).bit_length())]
    if count == 1 << len(bits):
        far = bits[2:]
        rounds = [bits[:1], *([mask | 1 for mask in (*far[i : i + 2], sum(far[i : i + 2]))] for i in range(0, len(far), 2)), [mask | 1 for mask in bits[1:2]]]
        for masks in rounds:
            sums = sums + sum(permute(sums, [(p, p ^ mask) for p in range(count)]) for mask in dict.fromkeys(masks))
    else:
        sums = lax.psum(sums, "lat")

    def rows_of(kernel, edge, rows):
        return call(
            kernel,
            [(x, vmem) for x in (about, height, merid_courant, part, edge, *tables)],
            [((rows, levels, nlon), f32)],
            16,
            [
                pltpu.VMEM((2, 2 * rows * levels, depth), jnp.bfloat16),
                pltpu.VMEM((2, 2 * rows * levels, cols), jnp.bfloat16),
                pltpu.VMEM((rows * levels, depth), f32),
            ],
        )[0]

    near = rows_of(near_kernel, a, rows - 2)
    far = rows_of(far_kernel, b, 2)
    (out,) = call(
        functools.partial(mean_kernel, nlat),
        [(x, vmem) for x in (about, sums, near, far)],
        [(height.shape, f32)],
        4,
        [pltpu.VMEM(height.shape, f32), pltpu.SemaphoreType.DMA((rows,))],
        hbm,
    )
    return out


def solution(mesh):
    split_rows = P(("member", "lat"), None, None)
    return jax.shard_map(
        step,
        mesh=mesh,
        in_specs=(split_rows, split_rows, split_rows, P("member"), P("member"), P(), P()),
        out_specs=split_rows,
        check_vma=False,
    )
```

```python
import functools

import jax
import jax.numpy as jnp
import numpy as np
from jax import lax
from jax.experimental import pallas as pl
from jax.experimental.pallas import tpu as pltpu
from jax.sharding import PartitionSpec as P

LANES = 128


def round_up(value, step):
    return -(-value // step) * step


@functools.cache
def phases(nlon):
    half = nlon // 2
    width = round_up(half // 2 + 1, LANES)
    depth = round_up(half, LANES)
    points = np.arange(depth)
    arrays = []
    for parity in (0, 1):
        waves = 2 * np.arange(width) + parity
        lanes = (waves <= half)[None, :]

        def both(steps, valid, axis):
            angle = 2.0 * np.pi / nlon * (steps % nlon)
            return np.concatenate([np.cos(angle) * valid, np.sin(angle) * valid], axis=axis)

        blocks = [
            both(points[::8, None] * waves[None, :], lanes & (points[::8, None] < half), 1),
            both(points[:8, None] * waves[None, :], True, 1),
            both(16 * np.arange(width // 8)[:, None] * points[None, :], (points < half)[None, :], 0),
            both(waves[:8, None] * points[None, :], True, 0),
        ]
        columns = max(x.shape[1] for x in blocks)
        arrays.append(
            np.concatenate([np.pad(x, ((0, 0), (0, columns - x.shape[1]))) for x in blocks]).astype(np.float32)
        )
    return arrays


def softplus(s):
    return jnp.maximum(s, 0.0) + jnp.log(1.0 + jnp.exp(-jnp.abs(s)))


def wrapped(row, nlon, full):
    base = nlon // LANES * LANES
    rest = nlon - base
    body, tail = row[:, :base], row[:, base:]
    tail = jnp.concatenate([tail, jnp.zeros((row.shape[0], full - nlon), row.dtype)], axis=1)
    lane = lax.broadcasted_iota(jnp.int32, tail.shape, 1)
    head = pltpu.roll(row[:, : full - base], rest, 1)
    end = pltpu.roll(tail, full - base - rest, 1)
    tail = jnp.where(lane < rest, tail, jnp.where(lane < full - base - 8, head, end))
    return jnp.concatenate([body, tail], axis=1)


def diagonal(shape):
    return lax.broadcasted_iota(jnp.int32, shape, 0) == lax.broadcasted_iota(jnp.int32, shape, 1)


def column(row):
    count = row.shape[1]
    same = lax.broadcasted_iota(jnp.int32, (count, count), 0) == lax.broadcasted_iota(
        jnp.int32, (count, count), 1
    )
    return jnp.sum(jnp.where(same, row, 0.0), axis=1, keepdims=True)


def dense_tiles(levels, nlon):
    rest = nlon % LANES
    shared = LANES // rest if rest else 1
    whole = levels // 8 * (nlon // LANES)
    return whole, shared, (-(-(levels // 8) // shared) if rest else 0)


def pack_row(row, out_ref, i):
    levels, nlon = row.shape
    whole, shared, extra = dense_tiles(levels, nlon)
    per = nlon // LANES
    rest = nlon % LANES
    for t in range(whole):
        g, k = divmod(t, per)
        out_ref[i, 8 * t : 8 * t + 8, :] = row[8 * g : 8 * g + 8, k * LANES : (k + 1) * LANES]
    for e in range(extra):
        parts = [
            row[8 * g : 8 * g + 8, per * LANES :]
            for g in range(e * shared, min((e + 1) * shared, levels // 8))
        ]
        parts.append(jnp.zeros((8, LANES - rest * len(parts)), row.dtype))
        t = whole + e
        out_ref[i, 8 * t : 8 * t + 8, :] = jnp.concatenate([p for p in parts if p.shape[1]], axis=1)


def packed_tile(ref, i, g, k, levels, nlon):
    whole, shared, _ = dense_tiles(levels, nlon)
    per = nlon // LANES
    rest = nlon % LANES
    if k < per:
        t = g * per + k
        return ref[i, 8 * t : 8 * t + 8, :]
    t = whole + g // shared
    last = ref[i, 8 * t : 8 * t + 8, :]
    at = g % shared * rest
    return (pltpu.roll(last, LANES - at, 1) if at else last)[:, :rest]


def edge_rows(upper, rows):
    return jnp.where(upper, rows - 2, 1), jnp.where(upper, rows - 1, 0)


def pack_kernel(
    h_ref, v_ref, cos_ref, flags_ref, cutoffs_ref, out_ref, about_ref, edge_ref, cos, flags, cutoffs, sem
):
    rows = h_ref.shape[0]
    nlat = flags_ref.shape[0]
    position = lax.axis_index("lat")
    first = position * rows
    far, near = edge_rows(position % 2 == 1, rows)
    moves = [(h_ref.at[far], edge_ref.at[0]), (h_ref.at[near], edge_ref.at[1]), (v_ref.at[near], edge_ref.at[2])]
    moves += [(cos_ref, cos), (flags_ref, flags), (cutoffs_ref, cutoffs)]
    copies = [pltpu.make_async_copy(source, target, sem.at[i]) for i, (source, target) in enumerate(moves)]
    for c in copies:
        c.start()
    for c in copies[3:]:
        c.wait()
    flat = (8, LANES)
    for j in range(rows):
        about_ref[j] = 1.0 / jnp.full(flat, cos[first + j])
        about_ref[rows + j] = jnp.full(flat, flags[first + j].astype(jnp.float32))
        about_ref[2 * rows + j] = jnp.full(flat, cutoffs[first + j].astype(jnp.float32))
        about_ref[3 * rows + j] = jnp.full(flat, cos[first + j])
    for f in range(rows + 1):
        about_ref[4 * rows + f] = jnp.full(flat, cos[nlat + first + f] * (0.5 / 12.0))
    for c in copies[:3]:
        c.wait()
    for i in range(3):
        pack_row(edge_ref[i], out_ref, i)


def source_kernel(about_ref, rates_ref, thresholds_ref, h_ref, v_ref, edge_ref, sum_ref, out_ref):
    rows, levels, nlon = h_ref.shape
    full = round_up(nlon, LANES)
    base = base_of(nlon)
    position = lax.axis_index("lat")
    rates = column(rates_ref[...])
    thresholds = column(thresholds_ref[...])
    total = jnp.zeros((levels, LANES), jnp.float32)
    for j in range(rows):
        s = softplus(h_ref[j] - thresholds) * -rates
        out_ref[j] = s
        acc = s[:, 0:LANES]
        for t in range(1, nlon // LANES):
            acc = acc + s[:, t * LANES : (t + 1) * LANES]
        if base < nlon:
            acc = acc + jnp.concatenate(
                [s[:, base:], jnp.zeros((levels, full - nlon), jnp.float32)], axis=1
            )
        weight = about_ref[3 * rows + j]
        total = total + acc * jnp.concatenate([weight] * (levels // 8), axis=0)
    total = jnp.broadcast_to(jnp.sum(total, axis=1, keepdims=True), (levels, sum_ref.shape[1]))
    sum_ref[...] = jnp.sum(jnp.where(diagonal(total.shape), total, 0.0), axis=0, keepdims=True)
    far, near = edge_rows(position % 2 == 0, rows)
    edge_ref[0] = h_ref[far]
    edge_ref[1] = h_ref[near]
    edge_ref[2] = v_ref[near]


def zonal_kernel(h_ref, u_ref, s_ref, out_ref):
    rows, _, nlon = h_ref.shape
    full = round_up(nlon, LANES)
    for j in range(rows):
        h0 = h_ref[j]
        h = wrapped(h0, nlon, full)
        u = wrapped(u_ref[j], nlon, full)
        east = pltpu.roll(h, full - 1, 1)
        far_east = pltpu.roll(h, full - 2, 1)
        west = pltpu.roll(h, 1, 1)
        face = (7.0 * (h + east) - (west + far_east)) * (0.5 / 12.0)
        flux = (u + pltpu.roll(u, full - 1, 1)) * face
        div = flux - pltpu.roll(flux, 1, 1)
        out_ref[j] = h0 - div[:, :nlon] + s_ref[j]


def table_kernel(parity, half, source_ref, high_ref, low_ref, high_t_ref, low_t_ref):
    depth, cols = high_ref.shape
    width = cols // 2

    def put(high, low, at, cols, values):
        h = values.astype(jnp.bfloat16)
        high[at, cols] = h
        low[at, cols] = (values - h.astype(jnp.float32)).astype(jnp.bfloat16)

    def fill(coarse_cos, coarse_sin, fine_cos, fine_sin, count, store):
        for k in range(0, count, 2):
            pieces = []
            for q in (k, k + 1):
                cc, cs = coarse_cos(q), coarse_sin(q)
                pieces.append((cc * fine_cos - cs * fine_sin, cs * fine_cos + cc * fine_sin))
            store(k, *[jnp.concatenate(p, axis=0) for p in zip(*pieces)])

    def store(k, c, s):
        at = slice(8 * k, 8 * k + 16)
        put(high_ref, low_ref, at, slice(0, width), c)
        put(high_ref, low_ref, at, slice(width, cols), s)

    def store_t(k, c, s):
        if 2 * (8 * k + 15) + parity > half:
            waves = 2 * (8 * k + lax.broadcasted_iota(jnp.int32, c.shape, 0)) + parity
            c, s = jnp.where(waves <= half, c, 0.0), jnp.where(waves <= half, s, 0.0)
        put(high_t_ref, low_t_ref, slice(8 * k, 8 * k + 16), slice(None), c)
        put(high_t_ref, low_t_ref, slice(width + 8 * k, width + 8 * k + 16), slice(None), s)

    fine = depth // 8
    turned = fine + 8
    fine_t = turned + 2 * (width // 8)
    fill(
        lambda q: source_ref[q : q + 1, :width],
        lambda q: source_ref[q : q + 1, width:cols],
        source_ref[fine : fine + 8, :width],
        source_ref[fine : fine + 8, width:cols],
        depth // 8,
        store,
    )
    fill(
        lambda q: source_ref[turned + q : turned + q + 1, :depth],
        lambda q: source_ref[turned + width // 8 + q : turned + width // 8 + q + 1, :depth],
        source_ref[fine_t : fine_t + 8, :depth],
        source_ref[fine_t + 8 : fine_t + 16, :depth],
        width // 8,
        store_t,
    )


class Side:
    def __init__(self, lower, about_ref, arrays):
        self.about_ref = about_ref
        self.h_ref, self.v_ref, self.part_ref = arrays
        self.rows, self.levels, self.nlon = self.h_ref.shape
        self.full = round_up(self.nlon, LANES)
        self.lower = lower
        self.outermost = lax.axis_index("lat") == jnp.where(lower, 0, lax.axis_size("lat") - 1)

    def row(self, i):
        return jnp.where(self.lower, i, self.rows - 1 - i)

    def tiles(self, g):
        for k in range(self.full // LANES):
            yield k, slice(8 * g, 8 * g + 8), slice(k * LANES, min((k + 1) * LANES, self.nlon))

    def any_marked(self):
        marked = self.about_ref[self.rows]
        for j in range(1, self.rows):
            marked = jnp.maximum(marked, self.about_ref[self.rows + j])
        return marked[0, 0] > 0

    def update(self, count, halo_tile, out_ref):
        sign = jnp.where(self.lower, 1.0, -1.0)
        scale = [self.about_ref[self.row(i)] * sign for i in range(count)]
        face_cos = [
            self.about_ref[4 * self.rows + jnp.where(self.lower, i, self.rows - i)] for i in range(count + 1)
        ]
        for g in range(self.levels // 8):
            for k, at, lanes in self.tiles(g):
                wide = lanes.stop - lanes.start
                far, near, beyond = (jnp.where(self.outermost, 0.0, halo_tile(i, g, k)) for i in range(3))
                height = [far, near, *(self.h_ref[self.row(i), at, lanes] for i in range(count + 2))]
                speed = [beyond, *(self.v_ref[self.row(i), at, lanes] for i in range(count + 1))]
                flux = []
                for f in range(count + 1):
                    p = 7.0 * (height[f + 1] + height[f + 2]) - (height[f] + height[f + 3])
                    flux.append((speed[f] + speed[f + 1]) * face_cos[f][:, :wide] * p)
                for i in range(count):
                    div = (flux[i + 1] - flux[i]) * scale[i][:, :wide]
                    out_ref[i, at, lanes] = self.part_ref[self.row(i), at, lanes] - div

    def filter(self, count, tables, y_ref, s_ref, d_ref, out_ref):
        levels, nlon, full = self.levels, self.nlon, self.full
        half = nlon // 2
        depth, cols = tables[0].shape
        width = cols // 2
        units = count * levels
        for r in range(0, units, 16):
            j, q = divmod(r, levels)
            x = out_ref[j, q : q + 16, :]
            near = x[:, :depth]
            x = jnp.concatenate([x, jnp.zeros((16, full - nlon), jnp.float32)], axis=1)
            far = pltpu.roll(x, full - half, 1)[:, :depth]
            for parity, y in ((0, near + far), (1, near - far)):
                put_parts(y_ref, parity, r, units, slice(None), y)
        lane = lax.broadcasted_iota(jnp.int32, (8, width), 1)
        chunk = 256 if cols % 256 == 0 and depth % 256 == 0 else LANES
        for parity in (0, 1):
            high_ref, low_ref = tables[4 * parity : 4 * parity + 2]
            waves = 2 * lane + parity
            weight = jnp.where((waves > 0) & (waves < half), 2.0 / nlon, 1.0 / nlon)
            inverse = 1.0 / jnp.maximum(waves, 1).astype(jnp.float32)
            factors = []
            for j in range(count):
                row = self.rows + self.row(j)
                ratio = self.about_ref[self.rows + row][:, :1] * inverse
                factor = (1.0 - jnp.minimum(1.0, ratio * ratio)) * weight
                factor = jnp.where(self.about_ref[row][:, :1] > 0, factor, 0.0)
                factors.append(jnp.concatenate([factor, factor], axis=1))
            for c in range(0, cols, chunk):
                spectrum = products(y_ref.at[parity], high_ref, low_ref, c, chunk, units)
                for r in range(0, units, 16):
                    f = factors[r // levels][:, c : c + chunk]
                    y = spectrum[r : r + 16] * jnp.concatenate([f, f], axis=0)
                    put_parts(s_ref, parity, r, units, slice(c, c + chunk), y)
        for c in range(0, depth, chunk):
            even = products(s_ref.at[0], tables[2], tables[3], c, chunk, units)
            uneven = products(s_ref.at[1], tables[6], tables[7], c, chunk, units)
            for r in range(0, units, 16):
                j, q = divmod(r, levels)
                x, y = even[r : r + 16], uneven[r : r + 16]
                out_ref[j, q : q + 16, c : c + chunk] -= x + y
                d_ref[r : r + 16, c : c + chunk] = x - y
        start = half // LANES * LANES
        for r in range(0, units, 8):
            j, q = divmod(r, levels)
            d = jnp.concatenate([d_ref[r : r + 8, :], jnp.zeros((8, full - depth), jnp.float32)], axis=1)
            out_ref[j, q : q + 8, start:] -= pltpu.roll(d, half, 1)[:, start:nlon]


def put_parts(ref, parity, r, units, lanes, y):
    high = y.astype(jnp.bfloat16)
    ref[parity, r : r + 16, lanes] = high
    ref[parity, units + r : units + r + 16, lanes] = (y - high.astype(jnp.float32)).astype(jnp.bfloat16)


def near_kernel(about_ref, h_ref, v_ref, part_ref, a_ref, *refs):
    tables, out_ref, scratch = refs[:8], refs[8], refs[9:]
    side = Side(lax.axis_index("lat") % 2 == 1, about_ref, (h_ref, v_ref, part_ref))
    count = out_ref.shape[0]

    def halo_tile(i, g, k):
        return a_ref[i, 8 * g : 8 * g + 8, k * LANES : min((k + 1) * LANES, side.nlon)]

    side.update(count, halo_tile, out_ref)
    pl.when(side.any_marked())(lambda: side.filter(count, tables, *scratch, out_ref))


def far_kernel(about_ref, h_ref, v_ref, part_ref, b_ref, *refs):
    tables, out_ref, scratch = refs[:8], refs[8], refs[9:]
    side = Side(lax.axis_index("lat") % 2 == 0, about_ref, (h_ref, v_ref, part_ref))
    count = out_ref.shape[0]
    side.update(count, lambda i, g, k: packed_tile(b_ref, i, g, k, side.levels, side.nlon), out_ref)
    pl.when(side.any_marked())(lambda: side.filter(count, tables, *scratch, out_ref))


def mean_kernel(nlat, about_ref, sums_ref, near_ref, far_ref, out_ref, row_ref, sem):
    rows, levels, nlon = row_ref.shape
    odd = lax.axis_index("lat") % 2 == 1
    area = nlon * float(np.sum(np.sin(np.pi * (np.arange(nlat) + 0.5) / nlat)))
    width = sums_ref.shape[1]
    mean = jnp.where(diagonal((levels, width)), sums_ref[...] * (1.0 / area), 0.0)
    mean = jnp.broadcast_to(jnp.sum(mean, axis=1, keepdims=True), (levels, LANES))
    done = near_ref.shape[0]
    copies = []
    for i in range(rows):
        ref, k, lower = (near_ref, i, odd) if i < done else (far_ref, i - done, odd == False)
        row = jnp.where(lower, k, rows - 1 - k)
        cut = about_ref[2 * rows + row]
        kept = jnp.where(about_ref[rows + row] > 0, jnp.minimum(1.0, cut * cut), 1.0)
        for g in range(levels // 8):
            at = slice(8 * g, 8 * g + 8)
            shift = mean[at] * kept
            for t in range(0, nlon, LANES):
                lanes = slice(t, min(t + LANES, nlon))
                row_ref[i, at, lanes] = ref[k, at, lanes] - shift[:, : lanes.stop - lanes.start]
            if g % 2 == 1 or g == levels // 8 - 1:
                at = pl.ds(8 * (g - g % 2), 8 * (g % 2) + 8)
                n = len(copies)
                copies.append(pltpu.make_async_copy(row_ref.at[i, at], out_ref.at[row, at], sem.at[n]))
                copies[-1].start()
    for c in copies:
        c.wait()


def products(y_ref, high_ref, low_ref, c, chunk, units):
    both = jnp.dot(y_ref[...], high_ref[:, c : c + chunk], preferred_element_type=jnp.float32)
    third = jnp.dot(y_ref[:units, :], low_ref[:, c : c + chunk], preferred_element_type=jnp.float32)
    return both[:units] + both[units:] + third


def base_of(nlon):
    return nlon // LANES * LANES


def call(kernel, ins, outs, megabytes, scratch=(), out_space=pltpu.VMEM):
    return pl.pallas_call(
        kernel,
        in_specs=[pl.BlockSpec(memory_space=space) for _, space in ins],
        out_specs=[pl.BlockSpec(memory_space=out_space) for _ in outs],
        out_shape=[jax.ShapeDtypeStruct(shape, dtype) for shape, dtype in outs],
        scratch_shapes=list(scratch),
        compiler_params=pltpu.CompilerParams(vmem_limit_bytes=megabytes << 20),
    )(*[x for x, _ in ins])


def permute(x, pairs, axes="lat"):
    return lax.ppermute(x, axes, pairs)


def step(height, zonal_courant, merid_courant, rates, thresholds, flags, cutoffs):
    rows, levels, nlon = height.shape
    count = lax.axis_size("lat")
    nlat = rows * count
    half = nlon // 2
    vmem, hbm = pltpu.VMEM, pltpu.HBM
    f32 = jnp.float32

    between = [(i, i + 1) for i in range(1, count - 1, 2)]
    within = [(i, i + 1) for i in range(0, count - 1, 2)]
    between = between + [(j, i) for i, j in between]
    parts = lax.axis_size("member")
    between = [(p * count + i, p * count + j) for p in range(parts) for i, j in between]
    ends = [0, count - 1] if count % 2 == 0 else [0]
    if parts % 2 == 0:
        between += [(p * count + e, (p ^ 1) * count + e) for p in range(parts) for e in ends]
    within = within + [(j, i) for i, j in within]
    whole, _, extra = dense_tiles(levels, nlon)
    faces = np.sin(np.pi * np.arange(nlat + 1) / nlat)
    faces[0] = faces[nlat] = 0.0
    cosines = np.concatenate([np.sin(np.pi * (np.arange(nlat) + 0.5) / nlat), faces])
    cosines = jnp.asarray(cosines.astype(np.float32))
    edge_b, about = call(
        pack_kernel,
        [
            (pltpu.with_memory_space_constraint(x, hbm), hbm)
            for x in (height, merid_courant, cosines, flags, cutoffs)
        ],
        [((3, 8 * (whole + extra), LANES), f32), ((5 * rows + 1, 8, LANES), f32)],
        4,
        [
            pltpu.VMEM((3, levels, nlon), f32),
            pltpu.SMEM(cosines.shape, f32),
            pltpu.SMEM(flags.shape, jnp.int32),
            pltpu.SMEM(cutoffs.shape, jnp.int32),
            pltpu.SemaphoreType.DMA((6,)),
        ],
    )
    b = permute(edge_b, between, ("member", "lat"))

    edge_a, sums, source = call(
        source_kernel,
        [(x, vmem) for x in (about, rates[None], thresholds[None], height, merid_courant)],
        [((3, levels, nlon), f32), ((1, round_up(levels, LANES)), f32), (height.shape, f32)],
        8,
    )
    a = permute(edge_a, within)
    (part,) = call(zonal_kernel, [(height, vmem), (zonal_courant, vmem), (source, vmem)], [(height.shape, f32)], 8)
    depth = round_up(half, LANES)
    cols = 2 * round_up(half // 2 + 1, LANES)
    tables = []
    for parity in (0, 1):
        tables += call(
            functools.partial(table_kernel, parity, half),
            [(jnp.asarray(phases(nlon)[parity]), vmem)],
            [((depth, cols), jnp.bfloat16)] * 2 + [((cols, depth), jnp.bfloat16)] * 2,
            8,
        )

    bits = [1 << i for i in range((count - 1).bit_length())]
    if count == 1 << len(bits):
        far = bits[2:]
        rounds = [bits[:1], *([mask | 1 for mask in (*far[i : i + 2], sum(far[i : i + 2]))] for i in range(0, len(far), 2)), [mask | 1 for mask in bits[1:2]]]
        for masks in rounds:
            sums = sums + sum(permute(sums, [(p, p ^ mask) for p in range(count)]) for mask in dict.fromkeys(masks))
    else:
        sums = lax.psum(sums, "lat")

    def rows_of(kernel, edge, rows):
        return call(
            kernel,
            [(x, vmem) for x in (about, height, merid_courant, part, edge, *tables)],
            [((rows, levels, nlon), f32)],
            16,
            [
                pltpu.VMEM((2, 2 * rows * levels, depth), jnp.bfloat16),
                pltpu.VMEM((2, 2 * rows * levels, cols), jnp.bfloat16),
                pltpu.VMEM((rows * levels, depth), f32),
            ],
        )[0]

    near = rows_of(near_kernel, a, rows - 2)
    far = rows_of(far_kernel, b, 2)
    (out,) = call(
        functools.partial(mean_kernel, nlat),
        [(x, vmem) for x in (about, sums, near, far)],
        [(height.shape, f32)],
        4,
        [pltpu.VMEM(height.shape, f32), pltpu.SemaphoreType.DMA((rows * (levels // 8),))],
        hbm,
    )
    return out


def solution(mesh):
    split_rows = P(("member", "lat"), None, None)
    return jax.shard_map(
        step,
        mesh=mesh,
        in_specs=(split_rows, split_rows, split_rows, P("member"), P("member"), P(), P()),
        out_specs=split_rows,
        check_vma=False,
    )
```
